32 devices in a mesh: rep: 4 (over y, x), cp: 8 (over z, core).
Axes of the slice: x: 2, y: 2, z: 4, core: 2. Of those that a mesh axis runs over, the one named last changes fastest.
Arguments:
- tokens: bfloat16 [4, 2048, 768], P('rep', 'cp'), may hold values from -6 to 6
- query_weight: bfloat16 [768, 768], P('cp'), may hold values from -0.3125 to 0.3125
- query_bias: bfloat16 [768], P('cp'), may hold values from -3 to 3
- key_weight: bfloat16 [768, 768], P('cp'), may hold values from -0.3125 to 0.3125
- value_weight: bfloat16 [768, 768], P('cp'), may hold values from -0.21875 to 0.21875
- value_bias: bfloat16 [768], P('cp'), may hold values from -3 to 3
- output_weight: bfloat16 [768, 768], P('cp'), may hold values from -1.5 to 1.5
- output_bias: bfloat16 [768], P('cp'), may hold values from -1.796875 to 1.796875
- first_gain: bfloat16 [768], P('cp'), may hold values from 0.099609375 to 1.8984375
- first_shift: bfloat16 [768], P('cp'), may hold values from -1.796875 to 1.796875
- up_weight: bfloat16 [768, 3072], P('cp'), may hold values from -0.21875 to 0.21875
- up_bias: bfloat16 [3072], P('cp'), may hold values from -3 to 3
- down_weight: bfloat16 [3072, 768], P('cp'), may hold values from -0.109375 to 0.109375
- down_bias: bfloat16 [768], P('cp'), may hold values from -1.796875 to 1.796875
- second_gain: bfloat16 [768], P('cp'), may hold values from 0.099609375 to 1.8984375
- second_shift: bfloat16 [768], P('cp'), may hold values from -1.796875 to 1.796875
- cotangent: float32 [4, 2048, 768], P('rep', 'cp'), may hold values from -18 to 18
Outputs:
- layer_out: float32 [4, 2048, 768], P('rep', 'cp')
- grad_tokens: float32 [4, 2048, 768], P('rep', 'cp')
- grad_query_weight: float32 [768, 768], P('cp')
- grad_query_bias: float32 [768], P('cp')
- grad_key_weight: float32 [768, 768], P('cp')
- grad_value_weight: float32 [768, 768], P('cp')
- grad_value_bias: float32 [768], P('cp')
- grad_output_weight: float32 [768, 768], P('cp')
- grad_output_bias: float32 [768], P('cp')
- grad_first_gain: float32 [768], P('cp')
- grad_first_shift: float32 [768], P('cp')
- grad_up_weight: float32 [768, 3072], P('cp')
- grad_up_bias: float32 [3072], P('cp')
- grad_down_weight: float32 [3072, 768], P('cp')
- grad_down_bias: float32 [768], P('cp')
- grad_second_gain: float32 [768], P('cp')
- grad_second_shift: float32 [768], P('cp')
- rms_values: float32 [1], replicated
The draws below stay inside these ranges and needn't reach their ends.
All inputs are finite; a program needn't handle non-finite values.
Results may differ from the reference program's by a relative error of at most 0.025.
Values may be sent and summed in bfloat16 or wider, within the bound.
A program may use at most 192 MiB of HBM per device.

```python
import math
import jax
import jax.numpy as jnp
from jax import lax

D = 768
H = 12
HD = 64
FF = 3072
TOK_DEV = 256
SEQ = 2048
SEQS = 4


def draw_cotangent(key, part):
    base = jnp.clip(jax.random.normal(key, (SEQS, SEQ, D), jnp.float32), -6.0, 6.0)
    ratio = 3.0
    position = jnp.arange(SEQ, dtype=jnp.float32) / SEQ - 0.5
    sequence_at = jnp.arange(SEQS, dtype=jnp.float32) / SEQS - 0.5
    row_scale = jnp.exp(jnp.log(ratio) * (sequence_at[:, None] + position[None, :]))
    return base * row_scale[:, :, None]


def block_levels(key, shape, pieces, low, high):
    factor_of, own = 1.0, jax.random.fold_in(key, 6)
    for axis_at, shards_of in pieces:
        heights = jnp.exp(jax.random.uniform(jax.random.fold_in(own, axis_at), (shards_of,), jnp.float32, low / len(pieces), high / len(pieces)))
        factor_of = factor_of * jnp.repeat(heights, shape[axis_at] // shards_of).reshape([-1 if axis == axis_at else 1 for axis in range(len(shape))])
    return factor_of


def noise(stream_key, dims, deviation, most, split=(), kind=jnp.bfloat16):
    values = deviation * jax.random.normal(stream_key, dims, jnp.float32)
    if split:
        values = values * block_levels(stream_key, dims, split, -0.22, 0.18)
    return jnp.clip(values, -most, most).astype(kind)


def setup_inputs(seed: int = 0) -> dict:
    key_of = jax.random.split(jax.random.key(seed), 18)
    return {
        "tokens": noise(key_of[0], (SEQS, SEQ, D), 1.0, 6.0, ((0, 4), (1, 8))),
        "query_weight": noise(key_of[1], (D, D), (D // 2) ** -0.5, 0.3125, ((0, 8),)),
        "query_bias": noise(key_of[2], (D,), 0.5, 3.0, ((0, 8),)),
        "key_weight": noise(key_of[3], (D, D), (D // 2) ** -0.5, 0.3125, ((0, 8),)),
        "value_weight": noise(key_of[4], (D, D), D ** -0.5, 0.21875, ((0, 8),)),
        "value_bias": noise(key_of[5], (D,), 0.5, 3.0, ((0, 8),)),
        "output_weight": noise(key_of[6], (D, D), 0.25, 1.5, ((0, 8),)),
        "output_bias": noise(key_of[7], (D,), 0.3, 1.796875, ((0, 8),)),
        "first_gain": jnp.clip(1.0 + 0.18 * jax.random.normal(key_of[8], (D,), jnp.float32), 0.099609375, 1.8984375).astype(jnp.bfloat16),
        "first_shift": noise(key_of[9], (D,), 0.3, 1.796875, ((0, 8),)),
        "up_weight": noise(key_of[10], (D, FF), D ** -0.5, 0.21875, ((0, 8),)),
        "up_bias": noise(key_of[11], (FF,), 0.5, 3.0, ((0, 8),)),
        "down_weight": noise(key_of[12], (FF, D), FF ** -0.5, 0.109375, ((0, 8),)),
        "down_bias": noise(key_of[13], (D,), 0.3, 1.796875, ((0, 8),)),
        "second_gain": jnp.clip(1.0 + 0.18 * jax.random.normal(key_of[14], (D,), jnp.float32), 0.099609375, 1.8984375).astype(jnp.bfloat16),
        "second_shift": noise(key_of[15], (D,), 0.3, 1.796875, ((0, 8),)),
        "cotangent": draw_cotangent(jax.random.fold_in(key_of[17], 71), 0),
    }


EPSILON = 1e-12
HIGHEST = lax.Precision.HIGHEST

@jax.custom_vjp
def low(v):
    return lax.optimization_barrier(v.astype(jnp.bfloat16)).astype(jnp.float32)

@jax.custom_vjp
def low_back(v):
    return v

def low_keep(v):
    return (low(v), None)

def low_pass(kept, grad):
    return (grad,)

def back_keep(v):
    return (v, None)

def back_low(kept, grad):
    return (low(grad),)
low.defvjp(low_keep, low_pass)
low_back.defvjp(back_keep, back_low)

def product(left, right):
    return jnp.dot(left, right, precision=HIGHEST, preferred_element_type=jnp.float32)

def normalize(values, norm_gain, norm_shift):
    center = values - lax.optimization_barrier(jnp.mean(values, axis=-1, keepdims=True))
    spread = lax.optimization_barrier(jnp.mean(center * center, axis=-1, keepdims=True))
    return center * lax.rsqrt(spread + EPSILON) * norm_gain + norm_shift

def gelu_exact(values):
    return 0.5 * values * (1.0 + lax.erf(values * (1.0 / math.sqrt(2.0))))

def attend(query_block, key_heads, value_heads):
    raw_scores = jnp.einsum('qhd,khd->hqk', query_block, key_heads, precision=HIGHEST)
    scores = low_back(raw_scores) * (1.0 / math.sqrt(HD))
    row_top = lax.optimization_barrier(jnp.max(scores, axis=-1, keepdims=True))
    exponent = jnp.exp(scores - row_top)
    probs = low(exponent / lax.optimization_barrier(jnp.sum(exponent, axis=-1, keepdims=True)))
    return jnp.einsum('hqk,khd->qhd', probs, value_heads, precision=HIGHEST)

def sequence(seq_tokens, weights):
    query_weight, query_bias, key_weight, value_weight, value_bias, output_weight, output_bias, first_gain, first_shift, up_weight, up_bias, down_weight, down_bias, second_gain, second_shift = weights
    length = seq_tokens.shape[0]
    query_rows = low(low_back(product(seq_tokens, query_weight) + query_bias))
    key_rows = low(low_back(product(seq_tokens, key_weight)))
    value_rows = low(low_back(product(seq_tokens, value_weight) + value_bias))
    query_blocks = query_rows.reshape(length // TOK_DEV, TOK_DEV, H, HD)
    key_heads = key_rows.reshape(length, H, HD)
    value_heads = value_rows.reshape(length, H, HD)
    context = lax.map(jax.checkpoint(lambda query_block: attend(query_block, key_heads, value_heads)), query_blocks)
    context_low = low(low_back(context.reshape(length, H * HD)))
    attn_out = low_back(product(context_low, output_weight) + output_bias)
    first_norm = normalize(seq_tokens + attn_out, first_gain, first_shift)
    inner_act = low_back(product(low(first_norm), up_weight) + up_bias)
    outer_out = low_back(product(low(gelu_exact(inner_act)), down_weight) + down_bias)
    return normalize(first_norm + outer_out, second_gain, second_shift)

def reference(tokens, query_weight, query_bias, key_weight, value_weight, value_bias, output_weight, output_bias, first_gain, first_shift, up_weight, up_bias, down_weight, down_bias, second_gain, second_shift, cotangent):
    weights = tuple((array.astype(jnp.float32) for array in (query_weight, query_bias, key_weight, value_weight, value_bias, output_weight, output_bias, first_gain, first_shift, up_weight, up_bias, down_weight, down_bias, second_gain, second_shift)))
    inputs = tokens.astype(jnp.float32)

    def forward(layer_in, params):
        return lax.map(lambda seq_tokens: sequence(seq_tokens, params), layer_in)
    layer_out, pullback = jax.vjp(forward, inputs, weights)
    grad_tokens, grads = pullback(cotangent.astype(jnp.float32))
    rms_values = jnp.stack([jnp.sqrt(jnp.mean(grad_tokens * grad_tokens))])
    return (layer_out, grad_tokens, grads[0], grads[1], grads[2], grads[3], grads[4], grads[5], grads[6], grads[7], grads[8], grads[9], grads[10], grads[11], grads[12], grads[13], grads[14], rms_values)
```

```python
import math

import jax
import jax.numpy as jnp
from jax import lax
from jax.experimental import pallas as pl
from jax.experimental.pallas import tpu as pltpu
from jax.sharding import PartitionSpec as P

HD = 64
PAIR = 2 * HD
CHUNKS = 3
EPSILON = 1e-12
BF16 = jnp.bfloat16
F32 = jnp.float32
BOTH = ("cp", "rep")


def normalize(values, norm_gain, norm_shift):
    center = values - jnp.mean(values, axis=-1, keepdims=True)
    spread = jnp.mean(center * center, axis=-1, keepdims=True)
    return center * lax.rsqrt(spread + EPSILON) * norm_gain + norm_shift


def gelu_exact(values):
    return 0.5 * values * (1.0 + lax.erf(values * (1.0 / math.sqrt(2.0))))


def matmul(left, right):
    return jnp.dot(left, right, preferred_element_type=F32)


def over_rows(left, right):
    return lax.dot_general(left, right, (((0,), (0,)), ((), ())), preferred_element_type=F32)


def against(left, right):
    return lax.dot_general(left, right, (((1,), (1,)), ((), ())), preferred_element_type=F32)


def column_sum(values):
    return jnp.sum(values.astype(F32), axis=0)


def head_mask(shape, head):
    lane = lax.broadcasted_iota(jnp.int32, shape, 1)
    return (lane >= head * HD) & (lane < (head + 1) * HD)


def forward_kernel(query_ref, pair_ref, context_ref):
    keys = pair_ref[:, :PAIR]
    values = pair_ref[:, PAIR:]
    query = query_ref[...]
    total = None
    for head in range(2):
        mask = head_mask(query.shape, head)
        scores = against(jnp.where(mask, query, jnp.zeros_like(query)), keys)
        top = jnp.max(scores, axis=-1, keepdims=True)
        weight = jnp.exp(scores - top)
        inverse = 1.0 / jnp.sum(weight, axis=-1, keepdims=True)
        part = matmul((weight * inverse).astype(BF16), values)
        total = part if head == 0 else jnp.where(mask, part, total)
    context_ref[...] = total.astype(BF16)


def backward_kernel(query_ref, grad_ref, pair_ref, grad_query_ref, grad_pair_ref):
    keys = pair_ref[:, :PAIR]
    values = pair_ref[:, PAIR:]
    query = query_ref[...]
    grad = grad_ref[...]
    zeros = jnp.zeros_like(query)
    key_part = value_part = query_part = None
    for head in range(2):
        mask = head_mask(query.shape, head)
        own_query = jnp.where(mask, query, zeros)
        own_grad = jnp.where(mask, grad, zeros)
        scores = against(keys, own_query)
        top = jnp.max(scores, axis=0, keepdims=True)
        weight = jnp.exp(scores - top)
        inverse = 1.0 / jnp.sum(weight, axis=0, keepdims=True)
        probs = weight * inverse
        grad_probs = against(values, own_grad)
        delta = jnp.sum(probs * grad_probs, axis=0, keepdims=True)
        grad_scores = (probs * (grad_probs - delta)).astype(BF16)
        new_value = matmul(probs.astype(BF16), own_grad)
        new_key = matmul(grad_scores, own_query)
        new_query = over_rows(keys, grad_scores)
        if head == 0:
            key_part, value_part, query_part = new_key, new_value, new_query
        else:
            key_part = key_part + new_key
            value_part = value_part + new_value
            row = lax.broadcasted_iota(jnp.int32, new_query.shape, 0)
            query_part = jnp.where(row < HD, query_part, new_query)
    grad_query_ref[...] = (query_part.T * (1.0 / math.sqrt(HD))).astype(BF16)
    grad_pair_ref[:, :PAIR] = key_part.astype(BF16)
    grad_pair_ref[:, PAIR:] = value_part.astype(BF16)


def column_block(rows, width):
    return pl.BlockSpec((rows, width), lambda i: (0, i))


def attend(query, pairs):
    rows, width = query.shape
    keys = pairs.shape[0]
    return pl.pallas_call(
        forward_kernel,
        grid=(width // PAIR,),
        in_specs=[column_block(rows, PAIR), column_block(keys, 2 * PAIR)],
        out_specs=column_block(rows, PAIR),
        out_shape=jax.ShapeDtypeStruct((rows, width), BF16),
    )(query, pairs)


def attend_back(query, grad, pairs):
    rows, width = query.shape
    keys = pairs.shape[0]
    return pl.pallas_call(
        backward_kernel,
        grid=(width // PAIR,),
        in_specs=[
            column_block(rows, PAIR),
            column_block(rows, PAIR),
            column_block(keys, 2 * PAIR),
        ],
        out_specs=(column_block(rows, PAIR), column_block(keys, 2 * PAIR)),
        out_shape=(
            jax.ShapeDtypeStruct((rows, width), BF16),
            jax.ShapeDtypeStruct((keys, 2 * width), BF16),
        ),
    )(query, grad, pairs)


def mixed(left, right):
    rows, width = left.shape
    joined = jnp.stack(
        [left.reshape(rows, width // PAIR, PAIR), right.reshape(rows, width // PAIR, PAIR)], axis=2
    )
    return joined.reshape(rows, 2 * width)


def unmixed(both):
    rows, width = both.shape
    parts = both.reshape(rows, width // (2 * PAIR), 2, PAIR)
    return parts[:, :, 0].reshape(rows, width // 2), parts[:, :, 1].reshape(rows, width // 2)


def own_rows(shard):
    share = shard.shape[0] // lax.axis_size("rep")
    return lax.dynamic_slice_in_dim(shard, lax.axis_index("rep") * share, share, 0)


def gather_all(shard):
    return lax.all_gather(own_rows(shard), BOTH, axis=0, tiled=True)


def scatter_all(values):
    return lax.psum_scatter(values.astype(BF16), BOTH, scatter_dimension=0, tiled=True)


def on_device(
    tokens,
    query_weight,
    query_bias,
    key_weight,
    value_weight,
    value_bias,
    output_weight,
    output_bias,
    first_gain,
    first_shift,
    up_weight,
    up_bias,
    down_weight,
    down_bias,
    second_gain,
    second_shift,
    cotangent,
):
    row_count = tokens.shape[1]
    width = tokens.shape[2]
    local_tokens = tokens[0]
    w_proj = gather_all(
        jnp.concatenate([query_weight, mixed(key_weight, value_weight)], axis=1)
    )
    small = (
        query_bias,
        value_bias,
        output_bias,
        first_gain,
        first_shift,
        up_bias,
        down_bias,
        second_gain,
        second_shift,
    )
    gathered = lax.all_gather(jnp.concatenate(small)[None], "cp", axis=0, tiled=True)
    vectors = []
    at = 0
    for vector in small:
        part = gathered[:, at : at + vector.shape[0]]
        vectors.append(part.reshape(-1).astype(F32))
        at += vector.shape[0]
    b_query, b_value, b_output, gain_one, shift_one, b_up, b_down, gain_two, shift_two = vectors
    w_pair = w_proj[:, width:]
    pair_bias = mixed(jnp.zeros_like(b_value)[None], b_value[None])
    pair_rows = (matmul(local_tokens, w_pair) + pair_bias).astype(BF16)
    chunk = width // CHUNKS
    pairs = [
        lax.all_gather(
            pair_rows[:, 2 * chunk * i : 2 * chunk * (i + 1)], "cp", axis=0, tiled=True
        )
        for i in range(CHUNKS)
    ]
    query_rows = (matmul(local_tokens, w_proj[:, :width]) + b_query).astype(BF16)
    query_scaled = query_rows * jnp.asarray(1.0 / math.sqrt(HD), BF16)
    queries = [query_scaled[:, chunk * i : chunk * (i + 1)] for i in range(CHUNKS)]
    w_wide = gather_all(jnp.concatenate([output_weight, up_weight], axis=1))
    w_output = w_wide[:, :width]
    w_up = w_wide[:, width:]
    w_down = gather_all(down_weight)

    context_low = jnp.concatenate(
        [attend(query, pair) for query, pair in zip(queries, pairs)], axis=1
    )
    attn_out = matmul(context_low, w_output) + b_output
    resid_first = local_tokens.astype(F32) + attn_out
    first_norm, pull_first = jax.vjp(normalize, resid_first, gain_one, shift_one)
    first_low = first_norm.astype(BF16)
    inner_act = matmul(first_low, w_up) + b_up
    hidden, pull_gelu = jax.vjp(gelu_exact, inner_act)
    hidden_low = hidden.astype(BF16)
    resid_second = first_norm + (matmul(hidden_low, w_down) + b_down)
    layer_out, pull_second = jax.vjp(normalize, resid_second, gain_two, shift_two)

    grad_resid2, grad_gain2, grad_shift2 = pull_second(cotangent[0])
    grad_outer = grad_resid2.astype(BF16)
    grad_down_bias = column_sum(grad_outer)
    part_down = scatter_all(over_rows(hidden_low, grad_outer))
    grad_inner = pull_gelu(against(grad_outer, w_down))[0].astype(BF16)
    grad_up_bias = column_sum(grad_inner)
    part_up = scatter_all(over_rows(first_low, grad_inner))
    grad_first = grad_resid2 + against(grad_inner, w_up)
    grad_resid1, grad_gain1, grad_shift1 = pull_first(grad_first)
    grad_attn = grad_resid1.astype(BF16)
    grad_output_bias = column_sum(grad_attn)
    part_output = scatter_all(over_rows(context_low, grad_attn))
    grad_context = against(grad_attn, w_output).astype(BF16)

    grad_queries = []
    grad_pairs = []
    for i in range(CHUNKS):
        grad_query, grad_terms = attend_back(
            queries[i], grad_context[:, chunk * i : chunk * (i + 1)], pairs[i]
        )
        grad_queries.append(grad_query)
        grad_pairs.append(
            lax.psum_scatter(grad_terms, "cp", scatter_dimension=0, tiled=True)
        )
    grad_query_low = jnp.concatenate(grad_queries, axis=1)
    grad_pair_low = jnp.concatenate(grad_pairs, axis=1)
    grad_proj = jnp.concatenate([grad_query_low, grad_pair_low], axis=1)
    part_proj = scatter_all(over_rows(local_tokens, grad_proj))
    grad_tokens = grad_resid1 + against(grad_proj, w_proj)
    proj_sums = column_sum(grad_proj)
    _, grad_value_bias = unmixed(proj_sums[None, width:])

    small_grads = (
        proj_sums[:width],
        grad_value_bias[0],
        grad_output_bias,
        grad_gain1,
        grad_shift1,
        grad_up_bias,
        grad_down_bias,
        grad_gain2,
        grad_shift2,
    )
    flat = jnp.concatenate(small_grads + (jnp.sum(grad_tokens * grad_tokens)[None],))
    sums = lax.psum(flat, ("rep", "cp"))
    place = lax.axis_index("cp")
    reduced = []
    at = 0
    for vector, shard in zip(small_grads, small):
        own = lax.dynamic_slice_in_dim(
            sums, at + place * shard.shape[0], shard.shape[0], 0
        )
        reduced.append(own)
        at += vector.shape[0]
    entries = lax.axis_size("rep") * lax.axis_size("cp") * row_count * width
    rms_values = jnp.sqrt(sums[at:] / entries)

    full_down = lax.all_gather(part_down, "rep", axis=0, tiled=True).astype(F32)
    full_wide = lax.all_gather(
        jnp.concatenate([part_output, part_up], axis=1), "rep", axis=0, tiled=True
    ).astype(F32)
    full_proj = lax.all_gather(part_proj, "rep", axis=0, tiled=True).astype(F32)
    grad_key_weight, grad_value_weight = unmixed(full_proj[:, width:])
    return (
        layer_out[None],
        grad_tokens[None],
        full_proj[:, :width],
        reduced[0],
        grad_key_weight,
        grad_value_weight,
        reduced[1],
        full_wide[:, :width],
        reduced[2],
        reduced[3],
        reduced[4],
        full_wide[:, width:],
        reduced[5],
        full_down,
        reduced[6],
        reduced[7],
        reduced[8],
        rms_values,
    )


def solution(mesh):
    rows = P("cp", None)
    vector = P("cp")
    whole = P("rep", "cp", None)
    params = (
        rows,
        vector,
        rows,
        rows,
        vector,
        rows,
        vector,
        vector,
        vector,
        rows,
        vector,
        rows,
        vector,
        vector,
        vector,
    )
    return jax.shard_map(
        on_device,
        mesh=mesh,
        in_specs=(whole,) + params + (whole,),
        out_specs=(whole, whole) + params + (P(),),
        check_vma=False,
    )
```

```python
import math

import jax
import jax.numpy as jnp
from jax import lax
from jax.experimental import pallas as pl
from jax.experimental.pallas import tpu as pltpu
from jax.sharding import PartitionSpec as P

HD = 64
PAIR = 2 * HD
CHUNKS = 3
EPSILON = 1e-12
BF16 = jnp.bfloat16
F32 = jnp.float32


def normalize(values, norm_gain, norm_shift):
    center = values - jnp.mean(values, axis=-1, keepdims=True)
    spread = jnp.mean(center * center, axis=-1, keepdims=True)
    return center * lax.rsqrt(spread + EPSILON) * norm_gain + norm_shift


def gelu_exact(values):
    return 0.5 * values * (1.0 + lax.erf(values * (1.0 / math.sqrt(2.0))))


def matmul(left, right):
    return jnp.dot(left, right, preferred_element_type=F32)


def over_rows(left, right):
    return lax.dot_general(left, right, (((0,), (0,)), ((), ())), preferred_element_type=F32)


def against(left, right):
    return lax.dot_general(left, right, (((1,), (1,)), ((), ())), preferred_element_type=F32)


def column_sum(values):
    return jnp.sum(values.astype(F32), axis=0)


def head_mask(shape, head):
    lane = lax.broadcasted_iota(jnp.int32, shape, 1)
    return (lane >= head * HD) & (lane < (head + 1) * HD)


def forward_kernel(query_ref, pair_ref, context_ref):
    keys = pair_ref[:, :PAIR]
    values = pair_ref[:, PAIR:]
    query = query_ref[...]
    total = None
    for head in range(2):
        mask = head_mask(query.shape, head)
        scores = against(jnp.where(mask, query, jnp.zeros_like(query)), keys)
        top = jnp.max(scores, axis=-1, keepdims=True)
        weight = jnp.exp(scores - top)
        inverse = 1.0 / jnp.sum(weight, axis=-1, keepdims=True)
        part = matmul((weight * inverse).astype(BF16), values)
        total = part if head == 0 else jnp.where(mask, part, total)
    context_ref[...] = total.astype(BF16)


def backward_kernel(query_ref, grad_ref, pair_ref, grad_query_ref, grad_pair_ref):
    keys = pair_ref[:, :PAIR]
    values = pair_ref[:, PAIR:]
    query = query_ref[...]
    grad = grad_ref[...]
    zeros = jnp.zeros_like(query)
    key_part = value_part = query_part = None
    for head in range(2):
        mask = head_mask(query.shape, head)
        own_query = jnp.where(mask, query, zeros)
        own_grad = jnp.where(mask, grad, zeros)
        scores = against(keys, own_query)
        top = jnp.max(scores, axis=0, keepdims=True)
        weight = jnp.exp(scores - top)
        inverse = 1.0 / jnp.sum(weight, axis=0, keepdims=True)
        probs = weight * inverse
        grad_probs = against(values, own_grad)
        delta = jnp.sum(probs * grad_probs, axis=0, keepdims=True)
        grad_scores = (probs * (grad_probs - delta)).astype(BF16)
        new_value = matmul(probs.astype(BF16), own_grad)
        new_key = matmul(grad_scores, own_query)
        new_query = over_rows(keys, grad_scores)
        if head == 0:
            key_part, value_part, query_part = new_key, new_value, new_query
        else:
            key_part = key_part + new_key
            value_part = value_part + new_value
            row = lax.broadcasted_iota(jnp.int32, new_query.shape, 0)
            query_part = jnp.where(row < HD, query_part, new_query)
    grad_query_ref[...] = (query_part.T * (1.0 / math.sqrt(HD))).astype(BF16)
    grad_pair_ref[:, :PAIR] = key_part.astype(BF16)
    grad_pair_ref[:, PAIR:] = value_part.astype(BF16)


def column_block(rows, width):
    return pl.BlockSpec((rows, width), lambda i: (0, i))


def attend(query, pairs):
    rows, width = query.shape
    keys = pairs.shape[0]
    return pl.pallas_call(
        forward_kernel,
        grid=(width // PAIR,),
        in_specs=[column_block(rows, PAIR), column_block(keys, 2 * PAIR)],
        out_specs=column_block(rows, PAIR),
        out_shape=jax.ShapeDtypeStruct((rows, width), BF16),
    )(query, pairs)


def attend_back(query, grad, pairs):
    rows, width = query.shape
    keys = pairs.shape[0]
    return pl.pallas_call(
        backward_kernel,
        grid=(width // PAIR,),
        in_specs=[
            column_block(rows, PAIR),
            column_block(rows, PAIR),
            column_block(keys, 2 * PAIR),
        ],
        out_specs=(column_block(rows, PAIR), column_block(keys, 2 * PAIR)),
        out_shape=(
            jax.ShapeDtypeStruct((rows, width), BF16),
            jax.ShapeDtypeStruct((keys, 2 * width), BF16),
        ),
    )(query, grad, pairs)


def mixed(left, right):
    rows, width = left.shape
    joined = jnp.stack(
        [left.reshape(rows, width // PAIR, PAIR), right.reshape(rows, width // PAIR, PAIR)], axis=2
    )
    return joined.reshape(rows, 2 * width)


def unmixed(both):
    rows, width = both.shape
    parts = both.reshape(rows, width // (2 * PAIR), 2, PAIR)
    return parts[:, :, 0].reshape(rows, width // 2), parts[:, :, 1].reshape(rows, width // 2)


def gather_all(shard):
    return lax.all_gather(shard, "cp", axis=0, tiled=True)


def scatter_all(values):
    return lax.psum_scatter(values.astype(BF16), "cp", scatter_dimension=0, tiled=True)


def on_device(
    tokens,
    query_weight,
    query_bias,
    key_weight,
    value_weight,
    value_bias,
    output_weight,
    output_bias,
    first_gain,
    first_shift,
    up_weight,
    up_bias,
    down_weight,
    down_bias,
    second_gain,
    second_shift,
    cotangent,
):
    row_count = tokens.shape[1]
    width = tokens.shape[2]
    local_tokens = tokens[0]
    w_proj = gather_all(
        jnp.concatenate([query_weight, mixed(key_weight, value_weight)], axis=1)
    )
    small = (
        query_bias,
        value_bias,
        output_bias,
        first_gain,
        first_shift,
        up_bias,
        down_bias,
        second_gain,
        second_shift,
    )
    gathered = lax.all_gather(jnp.concatenate(small)[None], "cp", axis=0, tiled=True)
    vectors = []
    at = 0
    for vector in small:
        part = gathered[:, at : at + vector.shape[0]]
        vectors.append(part.reshape(-1).astype(F32))
        at += vector.shape[0]
    b_query, b_value, b_output, gain_one, shift_one, b_up, b_down, gain_two, shift_two = vectors
    w_pair = w_proj[:, width:]
    pair_bias = mixed(jnp.zeros_like(b_value)[None], b_value[None])
    pair_rows = (matmul(local_tokens, w_pair) + pair_bias).astype(BF16)
    chunk = width // CHUNKS
    pairs = [
        lax.all_gather(
            pair_rows[:, 2 * chunk * i : 2 * chunk * (i + 1)], "cp", axis=0, tiled=True
        )
        for i in range(CHUNKS)
    ]
    query_rows = (matmul(local_tokens, w_proj[:, :width]) + b_query).astype(BF16)
    query_scaled = query_rows * jnp.asarray(1.0 / math.sqrt(HD), BF16)
    queries = [query_scaled[:, chunk * i : chunk * (i + 1)] for i in range(CHUNKS)]
    w_wide = gather_all(jnp.concatenate([output_weight, up_weight], axis=1))
    w_output = w_wide[:, :width]
    w_up = w_wide[:, width:]
    w_down = gather_all(down_weight)

    context_low = jnp.concatenate(
        [attend(query, pair) for query, pair in zip(queries, pairs)], axis=1
    )
    attn_out = matmul(context_low, w_output) + b_output
    resid_first = local_tokens.astype(F32) + attn_out
    first_norm, pull_first = jax.vjp(normalize, resid_first, gain_one, shift_one)
    first_low = first_norm.astype(BF16)
    inner_act = matmul(first_low, w_up) + b_up
    hidden, pull_gelu = jax.vjp(gelu_exact, inner_act)
    hidden_low = hidden.astype(BF16)
    resid_second = first_norm + (matmul(hidden_low, w_down) + b_down)
    layer_out, pull_second = jax.vjp(normalize, resid_second, gain_two, shift_two)

    grad_resid2, grad_gain2, grad_shift2 = pull_second(cotangent[0])
    grad_outer = grad_resid2.astype(BF16)
    grad_down_bias = column_sum(grad_outer)
    part_down = scatter_all(over_rows(hidden_low, grad_outer))
    grad_inner = pull_gelu(against(grad_outer, w_down))[0].astype(BF16)
    grad_up_bias = column_sum(grad_inner)
    part_up = scatter_all(over_rows(first_low, grad_inner))
    grad_first = grad_resid2 + against(grad_inner, w_up)
    grad_resid1, grad_gain1, grad_shift1 = pull_first(grad_first)
    grad_attn = grad_resid1.astype(BF16)
    grad_output_bias = column_sum(grad_attn)
    part_output = scatter_all(over_rows(context_low, grad_attn))
    grad_context = against(grad_attn, w_output).astype(BF16)

    grad_queries = []
    grad_pairs = []
    for i in range(CHUNKS):
        grad_query, grad_terms = attend_back(
            queries[i], grad_context[:, chunk * i : chunk * (i + 1)], pairs[i]
        )
        grad_queries.append(grad_query)
        grad_pairs.append(
            lax.psum_scatter(grad_terms, "cp", scatter_dimension=0, tiled=True)
        )
    grad_query_low = jnp.concatenate(grad_queries, axis=1)
    grad_pair_low = jnp.concatenate(grad_pairs, axis=1)
    grad_proj = jnp.concatenate([grad_query_low, grad_pair_low], axis=1)
    part_proj = scatter_all(over_rows(local_tokens, grad_proj))
    grad_tokens = grad_resid1 + against(grad_proj, w_proj)
    proj_sums = column_sum(grad_proj)
    _, grad_value_bias = unmixed(proj_sums[None, width:])

    small_grads = (
        proj_sums[:width],
        grad_value_bias[0],
        grad_output_bias,
        grad_gain1,
        grad_shift1,
        grad_up_bias,
        grad_down_bias,
        grad_gain2,
        grad_shift2,
    )
    flat = jnp.concatenate(small_grads + (jnp.sum(grad_tokens * grad_tokens)[None],))
    sums = lax.psum(flat, ("rep", "cp"))
    place = lax.axis_index("cp")
    reduced = []
    at = 0
    for vector, shard in zip(small_grads, small):
        own = lax.dynamic_slice_in_dim(
            sums, at + place * shard.shape[0], shard.shape[0], 0
        )
        reduced.append(own)
        at += vector.shape[0]
    entries = lax.axis_size("rep") * lax.axis_size("cp") * row_count * width
    rms_values = jnp.sqrt(sums[at:] / entries)

    full_down, full_up, full_output, full_proj = [
        part.astype(F32)
        for part in lax.psum((part_down, part_up, part_output, part_proj), "rep")
    ]
    grad_key_weight, grad_value_weight = unmixed(full_proj[:, width:])
    return (
        layer_out[None],
        grad_tokens[None],
        full_proj[:, :width],
        reduced[0],
        grad_key_weight,
        grad_value_weight,
        reduced[1],
        full_output,
        reduced[2],
        reduced[3],
        reduced[4],
        full_up,
        reduced[5],
        full_down,
        reduced[6],
        reduced[7],
        reduced[8],
        rms_values,
    )


def solution(mesh):
    rows = P("cp", None)
    vector = P("cp")
    whole = P("rep", "cp", None)
    params = (
        rows,
        vector,
        rows,
        rows,
        vector,
        rows,
        vector,
        vector,
        vector,
        rows,
        vector,
        rows,
        vector,
        vector,
        vector,
    )
    return jax.shard_map(
        on_device,
        mesh=mesh,
        in_specs=(whole,) + params + (whole,),
        out_specs=(whole, whole) + params + (P(),),
        check_vma=False,
    )
```

```python
import functools
import math

import jax
import jax.numpy as jnp
from jax import lax
from jax.experimental import pallas as pl
from jax.experimental.pallas import tpu as pltpu
from jax.sharding import PartitionSpec as P

HD = 64
PAIR = 2 * HD
CHUNKS = 3
EPSILON = 1e-12
BF16 = jnp.bfloat16
F32 = jnp.float32
MESH = pl.DeviceIdType.MESH


def normalize(values, norm_gain, norm_shift):
    center = values - jnp.mean(values, axis=-1, keepdims=True)
    spread = jnp.mean(center * center, axis=-1, keepdims=True)
    return center * lax.rsqrt(spread + EPSILON) * norm_gain + norm_shift


def gelu_exact(values):
    return 0.5 * values * (1.0 + lax.erf(values * (1.0 / math.sqrt(2.0))))


def matmul(left, right):
    return jnp.dot(left, right, preferred_element_type=F32)


def over_rows(left, right):
    return lax.dot_general(left, right, (((0,), (0,)), ((), ())), preferred_element_type=F32)


def against(left, right):
    return lax.dot_general(left, right, (((1,), (1,)), ((), ())), preferred_element_type=F32)


def column_sum(values):
    return jnp.sum(values.astype(F32), axis=0)


def head_mask(shape, head):
    lane = lax.broadcasted_iota(jnp.int32, shape, 1)
    return (lane >= head * HD) & (lane < (head + 1) * HD)


def forward_kernel(query_ref, pair_ref, context_ref):
    keys = pair_ref[:, :PAIR]
    values = pair_ref[:, PAIR:]
    query = query_ref[...]
    total = None
    for head in range(2):
        mask = head_mask(query.shape, head)
        scores = against(jnp.where(mask, query, jnp.zeros_like(query)), keys)
        top = jnp.max(scores, axis=-1, keepdims=True)
        weight = jnp.exp(scores - top)
        inverse = 1.0 / jnp.sum(weight, axis=-1, keepdims=True)
        part = matmul((weight * inverse).astype(BF16), values)
        total = part if head == 0 else jnp.where(mask, part, total)
    context_ref[...] = total.astype(BF16)


def backward_kernel(query_ref, grad_ref, pair_ref, grad_query_ref, grad_pair_ref):
    keys = pair_ref[:, :PAIR]
    values = pair_ref[:, PAIR:]
    query = query_ref[...]
    grad = grad_ref[...]
    zeros = jnp.zeros_like(query)
    key_part = value_part = query_part = None
    for head in range(2):
        mask = head_mask(query.shape, head)
        own_query = jnp.where(mask, query, zeros)
        own_grad = jnp.where(mask, grad, zeros)
        scores = against(keys, own_query)
        top = jnp.max(scores, axis=0, keepdims=True)
        weight = jnp.exp(scores - top)
        inverse = 1.0 / jnp.sum(weight, axis=0, keepdims=True)
        probs = weight * inverse
        grad_probs = against(values, own_grad)
        delta = jnp.sum(probs * grad_probs, axis=0, keepdims=True)
        grad_scores = (probs * (grad_probs - delta)).astype(BF16)
        new_value = matmul(probs.astype(BF16), own_grad)
        new_key = matmul(grad_scores, own_query)
        new_query = over_rows(keys, grad_scores)
        if head == 0:
            key_part, value_part, query_part = new_key, new_value, new_query
        else:
            key_part = key_part + new_key
            value_part = value_part + new_value
            row = lax.broadcasted_iota(jnp.int32, new_query.shape, 0)
            query_part = jnp.where(row < HD, query_part, new_query)
    grad_query_ref[...] = (query_part.T * (1.0 / math.sqrt(HD))).astype(BF16)
    grad_pair_ref[:, :PAIR] = key_part.astype(BF16)
    grad_pair_ref[:, PAIR:] = value_part.astype(BF16)


def column_block(rows, width):
    return pl.BlockSpec((rows, width), lambda i: (0, i))


def attend(query, pairs):
    rows, width = query.shape
    keys = pairs.shape[0]
    return pl.pallas_call(
        forward_kernel,
        grid=(width // PAIR,),
        in_specs=[column_block(rows, PAIR), column_block(keys, 2 * PAIR)],
        out_specs=column_block(rows, PAIR),
        out_shape=jax.ShapeDtypeStruct((rows, width), BF16),
    )(query, pairs)


def attend_back(query, grad, pairs):
    rows, width = query.shape
    keys = pairs.shape[0]
    return pl.pallas_call(
        backward_kernel,
        grid=(width // PAIR,),
        in_specs=[
            column_block(rows, PAIR),
            column_block(rows, PAIR),
            column_block(keys, 2 * PAIR),
        ],
        out_specs=(column_block(rows, PAIR), column_block(keys, 2 * PAIR)),
        out_shape=(
            jax.ShapeDtypeStruct((rows, width), BF16),
            jax.ShapeDtypeStruct((keys, 2 * width), BF16),
        ),
    )(query, grad, pairs)


def mixed(left, right):
    rows, width = left.shape
    joined = jnp.stack(
        [left.reshape(rows, width // PAIR, PAIR), right.reshape(rows, width // PAIR, PAIR)], axis=2
    )
    return joined.reshape(rows, 2 * width)


def unmixed(both):
    rows, width = both.shape
    parts = both.reshape(rows, width // (2 * PAIR), 2, PAIR)
    return parts[:, :, 0].reshape(rows, width // 2), parts[:, :, 1].reshape(rows, width // 2)


def gather_all(shard):
    return lax.all_gather(shard, "cp", axis=0, tiled=True)


def scatter_all(values):
    return lax.psum_scatter(values.astype(BF16), "cp", scatter_dimension=0, tiled=True)


def places():
    rep = lax.axis_index("rep")
    cp = lax.axis_index("cp")
    return rep, cp // 2, cp % 2


def enter(rep, depth, core, reps, depths):
    barrier = pltpu.get_barrier_semaphore()
    peers = [(rep, 2 * depth + 1 - core)]
    peers += [((rep + k) % reps, 2 * depth + core) for k in range(1, reps)]
    peers += [(rep, 2 * ((depth + k) % depths) + core) for k in range(1, depths)]
    for peer in peers:
        pl.semaphore_signal(barrier, inc=1, device_id=peer, device_id_type=MESH)
    pl.semaphore_wait(barrier, len(peers))


def remote(src, dst, sends, recvs, at, peer):
    return pltpu.make_async_remote_copy(
        src_ref=src,
        dst_ref=dst,
        send_sem=sends.at[at],
        recv_sem=recvs.at[at],
        device_id=peer,
        device_id_type=MESH,
    )


def gather_kernel(units, count, reps, depths, *refs):
    ins = refs[:count]
    outs = refs[count : 2 * count]
    sends_z, recvs_z, sends_r, recvs_r, sends_c, recvs_c, local = refs[2 * count :]
    rep, depth, core = places()
    cp = 2 * depth + core
    enter(rep, depth, core, reps, depths)
    sibling = (rep, 2 * depth + 1 - core)
    sent = []
    copies = []
    for at in range(count):
        copy = pltpu.make_async_copy(ins[at], outs[at].at[depth, core], local.at[at])
        copy.start()
        copies.append(copy)
    for u, (at, low, size) in enumerate(units):
        cols = pl.ds(low, size)
        for k in range(1, depths):
            copy = remote(
                ins[at].at[rep, :, cols],
                outs[at].at[depth, core, rep, :, cols],
                sends_z,
                recvs_z,
                u * (depths - 1) + k - 1,
                (rep, 2 * ((depth + k) % depths) + core),
            )
            copy.start()
            sent.append(copy)
    for u, (at, low, size) in enumerate(units):
        cols = pl.ds(low, size)
        copy = remote(
            ins[at].at[:, :, cols],
            outs[at].at[depth, core, :, :, cols],
            sends_c,
            recvs_c,
            u * depths,
            sibling,
        )
        copy.start()
        sent.append(copy)

    def spread(u):
        at, low, size = units[u]
        cols = pl.ds(low, size)
        for k in range(1, depths):
            origin = (depth + depths - k) % depths
            block = outs[at].at[origin, core, rep, :, cols]
            index = u * (depths - 1) + k - 1
            remote(block, block, sends_z, recvs_z, index, (rep, cp)).wait_recv()
            for j in range(1, reps):
                copy = remote(
                    block,
                    block,
                    sends_r,
                    recvs_r,
                    index * (reps - 1) + j - 1,
                    ((rep + j) % reps, cp),
                )
                copy.start()
                sent.append(copy)

    def pass_on(u):
        at, low, size = units[u]
        cols = pl.ds(low, size)
        for k in range(1, depths):
            origin = (depth + depths - k) % depths
            index = u * (depths - 1) + k - 1
            for j in range(1, reps):
                block = outs[at].at[origin, core, (rep + reps - j) % reps, :, cols]
                remote(
                    block, block, sends_r, recvs_r, index * (reps - 1) + j - 1, (rep, cp)
                ).wait_recv()
            whole = outs[at].at[origin, core, :, :, cols]
            copy = remote(whole, whole, sends_c, recvs_c, u * depths + k, sibling)
            copy.start()
            sent.append(copy)

    for u in range(len(units)):
        spread(u)
        if u:
            pass_on(u - 1)
    pass_on(len(units) - 1)
    for u, (at, low, size) in enumerate(units):
        cols = pl.ds(low, size)
        for k in range(depths):
            origin = (depth + depths - k) % depths
            block = outs[at].at[origin, 1 - core, :, :, cols]
            remote(block, block, sends_c, recvs_c, u * depths + k, sibling).wait_recv()
    for copy in sent:
        copy.wait_send()
    for copy in copies:
        copy.wait()


def cut(width, pieces):
    size = width // pieces
    if size % 128:
        return [(0, width)]
    return [(size * i, size) for i in range(pieces)]


def gather_many(shards, pieces, identity):
    reps = lax.axis_size("rep")
    depths = lax.axis_size("cp") // 2
    count = len(shards)
    units = [
        (at, low, size)
        for at, shard in enumerate(shards)
        for low, size in cut(shard.shape[2], pieces[at])
    ]
    hops = len(units) * (depths - 1)
    dma = pltpu.SemaphoreType.DMA
    return pl.pallas_call(
        functools.partial(gather_kernel, units, count, reps, depths),
        out_shape=[
            jax.ShapeDtypeStruct((depths, 2) + shard.shape, shard.dtype) for shard in shards
        ],
        in_specs=[pl.BlockSpec(memory_space=pl.ANY)] * count,
        out_specs=[pl.BlockSpec(memory_space=pl.ANY)] * count,
        scratch_shapes=[
            dma((hops,)),
            dma((hops,)),
            dma((hops * (reps - 1),)),
            dma((hops * (reps - 1),)),
            dma((len(units) * depths,)),
            dma((len(units) * depths,)),
            dma((count,)),
        ],
        compiler_params=pltpu.CompilerParams(collective_id=identity, has_side_effects=True),
    )(*shards)


def add_into(target, index, parts):
    total = parts[0].astype(F32)
    for part in parts[1:]:
        total = total + part.astype(F32)
    target[index] = total.astype(BF16)


def reduce_kernel(units, count, reps, depths, *refs):
    ins = refs[:count]
    outs = refs[count : 2 * count]
    at = 2 * count
    size = len(units)
    first = refs[at : at + size]
    second = refs[at + size : at + 2 * size]
    third = refs[at + 2 * size : at + 3 * size]
    own = refs[at + 3 * size : at + 4 * size]
    sends_c, recvs_c, sends_r, recvs_r, sends_z, recvs_z, sends_g, recvs_g = refs[at + 4 * size :]
    rep, depth, core = places()
    cp = 2 * depth + core
    enter(rep, depth, core, reps, depths)
    sibling = (rep, 2 * depth + 1 - core)
    sent = []
    for u, (a, low, width) in enumerate(units):
        copy = remote(
            ins[a].at[:, 1 - core, :, :, pl.ds(low, width)],
            first[u],
            sends_c,
            recvs_c,
            u,
            sibling,
        )
        copy.start()
        sent.append(copy)

    def over_core(u):
        a, low, width = units[u]
        remote(first[u], first[u], sends_c, recvs_c, u, sibling).wait_recv()

        def step(i, carry):
            z = i // reps
            q = i % reps
            add_into(
                first[u],
                (z, q),
                [first[u][z, q], ins[a][z, core, q, :, low : low + width]],
            )
            return carry

        lax.fori_loop(0, depths * reps, step, 0)
        for k in range(1, reps):
            target = (rep + k) % reps
            copy = remote(
                first[u].at[:, target],
                second[u].at[k - 1],
                sends_r,
                recvs_r,
                u * (reps - 1) + k - 1,
                (target, cp),
            )
            copy.start()
            sent.append(copy)

    def over_rep(u):
        for k in range(1, reps):
            block = second[u].at[k - 1]
            remote(
                block, block, sends_r, recvs_r, u * (reps - 1) + k - 1, (rep, cp)
            ).wait_recv()

        def step(z, carry):
            add_into(
                own[u],
                z,
                [first[u][z, rep]] + [second[u][k, z] for k in range(reps - 1)],
            )
            return carry

        lax.fori_loop(0, depths, step, 0)
        for k in range(1, depths):
            target = (depth + k) % depths
            copy = remote(
                own[u].at[target],
                third[u].at[k - 1],
                sends_z,
                recvs_z,
                u * (depths - 1) + k - 1,
                (rep, 2 * target + core),
            )
            copy.start()
            sent.append(copy)

    def over_depth(u):
        a, low, width = units[u]
        for k in range(1, depths):
            block = third[u].at[k - 1]
            remote(
                block, block, sends_z, recvs_z, u * (depths - 1) + k - 1, (rep, cp)
            ).wait_recv()
        total = own[u][depth].astype(F32)
        for k in range(depths - 1):
            total = total + third[u][k].astype(F32)
        outs[a][rep, :, low : low + width] = total.astype(BF16)
        block = outs[a].at[rep, :, pl.ds(low, width)]
        for k in range(1, reps):
            copy = remote(
                block,
                block,
                sends_g,
                recvs_g,
                u * (reps - 1) + k - 1,
                ((rep + k) % reps, cp),
            )
            copy.start()
            sent.append(copy)

    stages = (over_core, over_rep, over_depth)
    for step in range(size + len(stages) - 1):
        for lag, stage in enumerate(stages):
            if 0 <= step - lag < size:
                stage(step - lag)
    for u, (a, low, width) in enumerate(units):
        for k in range(1, reps):
            block = outs[a].at[(rep + reps - k) % reps, :, pl.ds(low, width)]
            remote(
                block, block, sends_g, recvs_g, u * (reps - 1) + k - 1, (rep, cp)
            ).wait_recv()
    for copy in sent:
        copy.wait_send()


def reduce_many(parts, pieces, identity):
    reps = lax.axis_size("rep")
    depths = lax.axis_size("cp") // 2
    count = len(parts)
    blocks = []
    for part in parts:
        rows, width = part.shape
        blocks.append(
            part.astype(BF16).reshape(depths, 2, reps, rows // (2 * depths * reps), width)
        )
    units = [
        (at, low, size)
        for at, block in enumerate(blocks)
        for low, size in cut(block.shape[4], pieces[at])
    ]
    rows = [blocks[at].shape[3] for at, _, _ in units]
    sizes = [size for _, _, size in units]
    dma = pltpu.SemaphoreType.DMA
    vmem = pl.BlockSpec(memory_space=pltpu.VMEM)

    def buffers(*lead):
        return [pltpu.VMEM(lead + (r, s), BF16) for r, s in zip(rows, sizes)]

    total = len(units)
    sums = pl.pallas_call(
        functools.partial(reduce_kernel, units, count, reps, depths),
        out_shape=[
            jax.ShapeDtypeStruct((reps,) + block.shape[3:], BF16) for block in blocks
        ],
        in_specs=[vmem] * count,
        out_specs=[vmem] * count,
        scratch_shapes=buffers(depths, reps)
        + buffers(reps - 1, depths)
        + buffers(depths - 1)
        + buffers(depths)
        + [dma((total,))] * 2
        + [dma((total * (reps - 1),))] * 2
        + [dma((total * (depths - 1),))] * 2
        + [dma((total * (reps - 1),))] * 2,
        compiler_params=pltpu.CompilerParams(
            collective_id=identity, has_side_effects=True, vmem_limit_bytes=56 * 1024 * 1024
        ),
    )(*blocks)
    return [total.reshape(-1, total.shape[2]).astype(F32) for total in sums]


def blocked(shard):
    return shard.reshape(lax.axis_size("rep"), -1, shard.shape[1])


def divides(rows):
    reps = lax.axis_size("rep")
    return lax.axis_size("cp") == 8 and reps == 4 and rows % (8 * reps) == 0


def on_device(
    tokens,
    query_weight,
    query_bias,
    key_weight,
    value_weight,
    value_bias,
    output_weight,
    output_bias,
    first_gain,
    first_shift,
    up_weight,
    up_bias,
    down_weight,
    down_bias,
    second_gain,
    second_shift,
    cotangent,
):
    row_count = tokens.shape[1]
    width = tokens.shape[2]
    local_tokens = tokens[0]
    fast = divides(query_weight.shape[0])
    reps = lax.axis_size("rep")
    proj_shard = jnp.concatenate([query_weight, mixed(key_weight, value_weight)], axis=1)
    small = (
        query_bias,
        value_bias,
        output_bias,
        first_gain,
        first_shift,
        up_bias,
        down_bias,
        second_gain,
        second_shift,
    )
    flat_small = jnp.concatenate(small)
    if fast:
        unit = 8 * 128 * reps
        padded = jnp.pad(flat_small, (0, -flat_small.shape[0] % unit))
        w_proj, gathered = gather_many(
            (blocked(proj_shard), padded.reshape(reps, -1, 128)), (3, 1), 1
        )
        w_proj = w_proj.reshape(-1, proj_shard.shape[1])
        gathered = gathered.reshape(-1, padded.shape[0])
    else:
        w_proj = gather_all(proj_shard)
        gathered = lax.all_gather(flat_small[None], "cp", axis=0, tiled=True)
    vectors = []
    at = 0
    for vector in small:
        part = gathered[:, at : at + vector.shape[0]]
        vectors.append(part.reshape(-1).astype(F32))
        at += vector.shape[0]
    b_query, b_value, b_output, gain_one, shift_one, b_up, b_down, gain_two, shift_two = vectors
    w_pair = w_proj[:, width:]
    pair_bias = mixed(jnp.zeros_like(b_value)[None], b_value[None])
    pair_rows = (matmul(local_tokens, w_pair) + pair_bias).astype(BF16)
    chunk = width // CHUNKS
    pairs = [
        lax.all_gather(
            pair_rows[:, 2 * chunk * i : 2 * chunk * (i + 1)], "cp", axis=0, tiled=True
        )
        for i in range(CHUNKS)
    ]
    query_rows = (matmul(local_tokens, w_proj[:, :width]) + b_query).astype(BF16)
    query_scaled = query_rows * jnp.asarray(1.0 / math.sqrt(HD), BF16)
    queries = [query_scaled[:, chunk * i : chunk * (i + 1)] for i in range(CHUNKS)]
    wide_shard = jnp.concatenate([output_weight, up_weight], axis=1)
    if fast:
        wide_shard, down_shard, _ = lax.optimization_barrier(
            (wide_shard, down_weight, pair_rows)
        )
        w_wide, w_down = gather_many((blocked(wide_shard), blocked(down_shard)), (2, 2), 2)
        w_wide = w_wide.reshape(-1, wide_shard.shape[1])
        w_down = w_down.reshape(-1, width)
        w_wide, queries = lax.optimization_barrier((w_wide, queries))
    else:
        w_wide = gather_all(wide_shard)
        w_down = gather_all(down_weight)
    w_output = w_wide[:, :width]
    w_up = w_wide[:, width:]

    context_low = jnp.concatenate(
        [attend(query, pair) for query, pair in zip(queries, pairs)], axis=1
    )
    attn_out = matmul(context_low, w_output) + b_output
    resid_first = local_tokens.astype(F32) + attn_out
    first_norm, pull_first = jax.vjp(normalize, resid_first, gain_one, shift_one)
    first_low = first_norm.astype(BF16)
    inner_act = matmul(first_low, w_up) + b_up
    hidden, pull_gelu = jax.vjp(gelu_exact, inner_act)
    hidden_low = hidden.astype(BF16)
    resid_second = first_norm + (matmul(hidden_low, w_down) + b_down)
    layer_out, pull_second = jax.vjp(normalize, resid_second, gain_two, shift_two)

    grad_resid2, grad_gain2, grad_shift2 = pull_second(cotangent[0])
    grad_outer = grad_resid2.astype(BF16)
    grad_down_bias = column_sum(grad_outer)
    part_down = over_rows(hidden_low, grad_outer).astype(BF16)
    grad_inner = pull_gelu(against(grad_outer, w_down))[0].astype(BF16)
    grad_up_bias = column_sum(grad_inner)
    part_up = over_rows(first_low, grad_inner).astype(BF16)
    grad_first = grad_resid2 + against(grad_inner, w_up)
    grad_resid1, grad_gain1, grad_shift1 = pull_first(grad_first)
    grad_attn = grad_resid1.astype(BF16)
    grad_output_bias = column_sum(grad_attn)
    part_output = over_rows(context_low, grad_attn).astype(BF16)
    grad_context = against(grad_attn, w_output).astype(BF16)

    grad_queries = []
    grad_pairs = []
    terms = []
    for i in range(CHUNKS):
        grad_query, grad_terms = attend_back(
            queries[i], grad_context[:, chunk * i : chunk * (i + 1)], pairs[i]
        )
        grad_queries.append(grad_query)
        terms.append(grad_terms)
        grad_pairs.append(
            lax.psum_scatter(grad_terms, "cp", scatter_dimension=0, tiled=True)
        )
    if fast:
        part_down, part_up, part_output, _ = lax.optimization_barrier(
            (part_down, part_up, part_output, terms)
        )
        full_down, full_up, full_output = reduce_many(
            (part_down, part_up, part_output), (2, 2, 1), 3
        )
    grad_query_low = jnp.concatenate(grad_queries, axis=1)
    grad_pair_low = jnp.concatenate(grad_pairs, axis=1)
    grad_proj = jnp.concatenate([grad_query_low, grad_pair_low], axis=1)
    part_proj = over_rows(local_tokens, grad_proj).astype(BF16)
    grad_tokens = grad_resid1 + against(grad_proj, w_proj)
    proj_sums = column_sum(grad_proj)
    _, grad_value_bias = unmixed(proj_sums[None, width:])

    small_grads = (
        proj_sums[:width],
        grad_value_bias[0],
        grad_output_bias,
        grad_gain1,
        grad_shift1,
        grad_up_bias,
        grad_down_bias,
        grad_gain2,
        grad_shift2,
    )
    flat = jnp.concatenate(small_grads + (jnp.sum(grad_tokens * grad_tokens)[None],))
    sums = lax.psum(flat, ("rep", "cp"))
    place = lax.axis_index("cp")
    reduced = []
    at = 0
    for vector, shard in zip(small_grads, small):
        own = lax.dynamic_slice_in_dim(
            sums, at + place * shard.shape[0], shard.shape[0], 0
        )
        reduced.append(own)
        at += vector.shape[0]
    entries = lax.axis_size("rep") * lax.axis_size("cp") * row_count * width
    rms_values = jnp.sqrt(sums[at:] / entries)

    if fast:
        (full_proj,) = reduce_many((part_proj,), (3,), 4)
    else:
        shards = [scatter_all(part) for part in (part_down, part_up, part_output, part_proj)]
        full_down, full_up, full_output, full_proj = [
            part.astype(F32) for part in lax.psum(tuple(shards), "rep")
        ]
    grad_key_weight, grad_value_weight = unmixed(full_proj[:, width:])
    return (
        layer_out[None],
        grad_tokens[None],
        full_proj[:, :width],
        reduced[0],
        grad_key_weight,
        grad_value_weight,
        reduced[1],
        full_output,
        reduced[2],
        reduced[3],
        reduced[4],
        full_up,
        reduced[5],
        full_down,
        reduced[6],
        reduced[7],
        reduced[8],
        rms_values,
    )


def solution(mesh):
    rows = P("cp", None)
    vector = P("cp")
    whole = P("rep", "cp", None)
    params = (
        rows,
        vector,
        rows,
        rows,
        vector,
        rows,
        vector,
        vector,
        vector,
        rows,
        vector,
        rows,
        vector,
        vector,
        vector,
    )
    return jax.shard_map(
        on_device,
        mesh=mesh,
        in_specs=(whole,) + params + (whole,),
        out_specs=(whole, whole) + params + (P(),),
        check_vma=False,
    )
```

```python
import functools
import math

import jax
import jax.numpy as jnp
from jax import lax
from jax.experimental import pallas as pl
from jax.experimental.pallas import tpu as pltpu
from jax.sharding import PartitionSpec as P

HD = 64
PAIR = 2 * HD
CHUNKS = 3
EPSILON = 1e-12
BF16 = jnp.bfloat16
F32 = jnp.float32
MESH = pl.DeviceIdType.MESH


def normalize(values, norm_gain, norm_shift):
    center = values - jnp.mean(values, axis=-1, keepdims=True)
    spread = jnp.mean(center * center, axis=-1, keepdims=True)
    return center * lax.rsqrt(spread + EPSILON) * norm_gain + norm_shift


def gelu_exact(values):
    return 0.5 * values * (1.0 + lax.erf(values * (1.0 / math.sqrt(2.0))))


def matmul(left, right):
    return jnp.dot(left, right, preferred_element_type=F32)


def over_rows(left, right):
    return lax.dot_general(left, right, (((0,), (0,)), ((), ())), preferred_element_type=F32)


def against(left, right):
    return lax.dot_general(left, right, (((1,), (1,)), ((), ())), preferred_element_type=F32)


def column_sum(values):
    return jnp.sum(values.astype(F32), axis=0)


def head_mask(shape, head):
    lane = lax.broadcasted_iota(jnp.int32, shape, 1)
    return (lane >= head * HD) & (lane < (head + 1) * HD)


def forward_kernel(query_ref, pair_ref, context_ref):
    keys = pair_ref[:, :PAIR]
    values = pair_ref[:, PAIR:]
    query = query_ref[...]
    total = None
    for head in range(2):
        mask = head_mask(query.shape, head)
        scores = against(jnp.where(mask, query, jnp.zeros_like(query)), keys)
        top = jnp.max(scores, axis=-1, keepdims=True)
        weight = jnp.exp(scores - top)
        inverse = 1.0 / jnp.sum(weight, axis=-1, keepdims=True)
        part = matmul((weight * inverse).astype(BF16), values)
        total = part if head == 0 else jnp.where(mask, part, total)
    context_ref[...] = total.astype(BF16)


def backward_kernel(query_ref, grad_ref, pair_ref, grad_query_ref, grad_pair_ref):
    keys = pair_ref[:, :PAIR]
    values = pair_ref[:, PAIR:]
    query = query_ref[...]
    grad = grad_ref[...]
    zeros = jnp.zeros_like(query)
    key_part = value_part = query_part = None
    for head in range(2):
        mask = head_mask(query.shape, head)
        own_query = jnp.where(mask, query, zeros)
        own_grad = jnp.where(mask, grad, zeros)
        scores = against(keys, own_query)
        top = jnp.max(scores, axis=0, keepdims=True)
        weight = jnp.exp(scores - top)
        inverse = 1.0 / jnp.sum(weight, axis=0, keepdims=True)
        probs = weight * inverse
        grad_probs = against(values, own_grad)
        delta = jnp.sum(probs * grad_probs, axis=0, keepdims=True)
        grad_scores = (probs * (grad_probs - delta)).astype(BF16)
        new_value = matmul(probs.astype(BF16), own_grad)
        new_key = matmul(grad_scores, own_query)
        new_query = over_rows(keys, grad_scores)
        if head == 0:
            key_part, value_part, query_part = new_key, new_value, new_query
        else:
            key_part = key_part + new_key
            value_part = value_part + new_value
            row = lax.broadcasted_iota(jnp.int32, new_query.shape, 0)
            query_part = jnp.where(row < HD, query_part, new_query)
    grad_query_ref[...] = (query_part.T * (1.0 / math.sqrt(HD))).astype(BF16)
    grad_pair_ref[:, :PAIR] = key_part.astype(BF16)
    grad_pair_ref[:, PAIR:] = value_part.astype(BF16)


def column_block(rows, width):
    return pl.BlockSpec((rows, width), lambda i: (0, i))


def attend(query, pairs):
    rows, width = query.shape
    keys = pairs.shape[0]
    return pl.pallas_call(
        forward_kernel,
        grid=(width // PAIR,),
        in_specs=[column_block(rows, PAIR), column_block(keys, 2 * PAIR)],
        out_specs=column_block(rows, PAIR),
        out_shape=jax.ShapeDtypeStruct((rows, width), BF16),
    )(query, pairs)


def attend_back(query, grad, pairs):
    rows, width = query.shape
    keys = pairs.shape[0]
    return pl.pallas_call(
        backward_kernel,
        grid=(width // PAIR,),
        in_specs=[
            column_block(rows, PAIR),
            column_block(rows, PAIR),
            column_block(keys, 2 * PAIR),
        ],
        out_specs=(column_block(rows, PAIR), column_block(keys, 2 * PAIR)),
        out_shape=(
            jax.ShapeDtypeStruct((rows, width), BF16),
            jax.ShapeDtypeStruct((keys, 2 * width), BF16),
        ),
    )(query, grad, pairs)


def mixed(left, right):
    parts = []
    for low in range(0, left.shape[1], PAIR):
        parts += [left[:, low : low + PAIR], right[:, low : low + PAIR]]
    return jnp.concatenate(parts, axis=1)


def unmixed(both):
    starts = range(0, both.shape[1], 2 * PAIR)
    return (
        jnp.concatenate([both[:, low : low + PAIR] for low in starts], axis=1),
        jnp.concatenate([both[:, low + PAIR : low + 2 * PAIR] for low in starts], axis=1),
    )


def gather_all(shard):
    return lax.all_gather(shard, "cp", axis=0, tiled=True)


def scatter_all(values):
    return lax.psum_scatter(values.astype(BF16), "cp", scatter_dimension=0, tiled=True)


def places():
    rep = lax.axis_index("rep")
    cp = lax.axis_index("cp")
    return rep, cp // 4, (cp // 2) % 2, cp % 2


def place_of(high, low, core):
    return 4 * high + 2 * low + core


def enter(reps):
    rep, high, low, core = places()
    barrier = pltpu.get_barrier_semaphore()
    peers = [
        (rep, place_of(high, low, 1 - core)),
        (rep, place_of(high, 1 - low, core)),
        (rep, place_of(1 - high, low, core)),
    ]
    peers += [((rep + k) % reps, place_of(high, low, core)) for k in range(1, reps)]
    for peer in peers:
        pl.semaphore_signal(barrier, inc=1, device_id=peer, device_id_type=MESH)
    pl.semaphore_wait(barrier, len(peers))


def remote(src, dst, sends, recvs, at, peer):
    return pltpu.make_async_remote_copy(
        src_ref=src,
        dst_ref=dst,
        send_sem=sends.at[at],
        recv_sem=recvs.at[at],
        device_id=peer,
        device_id_type=MESH,
    )


def gather_kernel(units, count, reps, *refs):
    ins = refs[:count]
    outs = refs[count : 2 * count]
    sends_z, recvs_z, sends_r, recvs_r, sends_c, recvs_c, local = refs[2 * count :]
    rep, high, low, core = places()
    me = (rep, place_of(high, low, core))
    sibling = (rep, place_of(high, low, 1 - core))
    far = (rep, place_of(1 - high, low, core))
    near = (rep, place_of(high, 1 - low, core))
    enter(reps)
    sent = []
    copies = []

    def send(src, dst, sends, recvs, at, peer):
        copy = remote(src, dst, sends, recvs, at, peer)
        copy.start()
        sent.append(copy)

    def arrived(block, sends, recvs, at):
        remote(block, block, sends, recvs, at, me).wait_recv()

    def group(u, which, side, quarter):
        at, start, size = units[u]
        cols = pl.ds(start, size)
        if which == 0:
            return outs[at].at[high, low, side, quarter, :, cols]
        if which == 1:
            return outs[at].at[1 - high, low, side, quarter, :, cols]
        return outs[at].at[:, 1 - low, side, quarter, :, cols]

    for u, (at, start, size) in enumerate(units):
        block = ins[at].at[rep, :, pl.ds(start, size)]
        send(block, group(u, 0, core, rep), sends_z, recvs_z, 2 * u, far)
    for at in range(count):
        copy = pltpu.make_async_copy(ins[at], outs[at].at[high, low, core], local.at[at])
        copy.start()
        copies.append(copy)
    for copy in copies:
        copy.wait()

    def double(u):
        at, start, size = units[u]
        arrived(group(u, 1, core, rep), sends_z, recvs_z, 2 * u)
        block = outs[at].at[:, low, core, rep, :, pl.ds(start, size)]
        send(block, block, sends_z, recvs_z, 2 * u + 1, near)
        whole = group(u, 0, core, slice(None))
        send(whole, whole, sends_c, recvs_c, 3 * u, sibling)

    def spread(u, which):
        if which == 2:
            arrived(group(u, 2, core, rep), sends_z, recvs_z, 2 * u + 1)
        block = group(u, which, core, rep)
        for j in range(1, reps):
            index = (2 * u + which - 1) * (reps - 1) + j - 1
            peer = ((rep + j) % reps, me[1])
            send(block, block, sends_r, recvs_r, index, peer)

    def pass_on(u, which):
        for j in range(1, reps):
            index = (2 * u + which - 1) * (reps - 1) + j - 1
            block = group(u, which, core, (rep + reps - j) % reps)
            arrived(block, sends_r, recvs_r, index)
        whole = group(u, which, core, slice(None))
        send(whole, whole, sends_c, recvs_c, 3 * u + which, sibling)

    total = len(units)
    for step in range(total + 3):
        if step < total:
            double(step)
            spread(step, 1)
        if 1 <= step < total + 1:
            spread(step - 1, 2)
        if 2 <= step < total + 2:
            pass_on(step - 2, 1)
        if 3 <= step:
            pass_on(step - 3, 2)
    for u in range(total):
        for which in range(3):
            block = group(u, which, 1 - core, slice(None))
            arrived(block, sends_c, recvs_c, 3 * u + which)
    for copy in sent:
        copy.wait_send()


def cut(width, pieces):
    size = width // pieces
    if size % 128:
        return [(0, width)]
    return [(size * i, size) for i in range(pieces)]


def gather_many(shards, pieces, identity):
    reps = lax.axis_size("rep")
    count = len(shards)
    units = [
        (at, low, size)
        for at, shard in enumerate(shards)
        for low, size in cut(shard.shape[2], pieces[at])
    ]
    total = len(units)
    hops = 2 * total * (reps - 1)
    dma = pltpu.SemaphoreType.DMA
    return pl.pallas_call(
        functools.partial(gather_kernel, units, count, reps),
        out_shape=[
            jax.ShapeDtypeStruct((2, 2, 2) + shard.shape, shard.dtype) for shard in shards
        ],
        in_specs=[pl.BlockSpec(memory_space=pl.ANY)] * count,
        out_specs=[pl.BlockSpec(memory_space=pl.ANY)] * count,
        scratch_shapes=[dma((2 * total,))] * 2
        + [dma((hops,))] * 2
        + [dma((3 * total,))] * 2
        + [dma((count,))],
        compiler_params=pltpu.CompilerParams(collective_id=identity, has_side_effects=True),
    )(*shards)


def summed(parts, kind):
    total = parts[0].astype(F32)
    for part in parts[1:]:
        total = total + part.astype(F32)
    return total.astype(kind)


def reduce_kernel(units, count, reps, *refs):
    ins = refs[:count]
    outs = refs[count : 2 * count]
    at = 2 * count
    size = len(units)
    first, second, third, fourth, own = [
        refs[at + i * size : at + (i + 1) * size] for i in range(5)
    ]
    sems = refs[at + 5 * size :]
    sends_c, recvs_c, sends_r, recvs_r, sends_z, recvs_z, sends_g, recvs_g = sems
    rep, high, low, core = places()
    me = (rep, place_of(high, low, core))
    sibling = (rep, place_of(high, low, 1 - core))
    far = (rep, place_of(1 - high, low, core))
    near = (rep, place_of(high, 1 - low, core))
    enter(reps)
    sent = []

    def send(src, dst, sends, recvs, at, peer):
        copy = remote(src, dst, sends, recvs, at, peer)
        copy.start()
        sent.append(copy)

    def arrived(block, sends, recvs, at):
        remote(block, block, sends, recvs, at, me).wait_recv()

    for u, (a, start, width) in enumerate(units):
        block = ins[a].at[:, :, 1 - core, :, :, pl.ds(start, width)]
        send(block, first[u], sends_c, recvs_c, u, sibling)

    def over_core(u):
        a, start, width = units[u]
        arrived(first[u], sends_c, recvs_c, u)

        def step(i, carry):
            h, w, q = i // (2 * reps), (i // reps) % 2, i % reps
            mine = ins[a][h, w, core, q, :, start : start + width]
            first[u][h, w, q] = summed([first[u][h, w, q], mine], first[u].dtype)
            return carry

        lax.fori_loop(0, 4 * reps, step, 0)
        for k in range(1, reps):
            target = (rep + k) % reps
            send(
                first[u].at[:, :, target],
                second[u].at[k - 1],
                sends_r,
                recvs_r,
                u * (reps - 1) + k - 1,
                (target, me[1]),
            )

    def over_rep(u):
        for k in range(1, reps):
            arrived(second[u].at[k - 1], sends_r, recvs_r, u * (reps - 1) + k - 1)

        def step(i, carry):
            h, w = i // 2, i % 2
            parts = [first[u][h, w, rep]] + [second[u][k, h, w] for k in range(reps - 1)]
            own[u][h, w] = summed(parts, own[u].dtype)
            return carry

        lax.fori_loop(0, 4, step, 0)
        send(own[u].at[:, 1 - low], third[u], sends_z, recvs_z, 2 * u, near)

    def over_near(u):
        arrived(third[u], sends_z, recvs_z, 2 * u)
        for h in range(2):
            own[u][h, low] = summed([own[u][h, low], third[u][h]], own[u].dtype)
        send(own[u].at[1 - high, low], fourth[u], sends_z, recvs_z, 2 * u + 1, far)

    def over_far(u):
        a, start, width = units[u]
        arrived(fourth[u], sends_z, recvs_z, 2 * u + 1)
        outs[a][rep, :, start : start + width] = summed(
            [own[u][high, low], fourth[u][...]], outs[a].dtype
        )
        block = outs[a].at[rep, :, pl.ds(start, width)]
        for k in range(1, reps):
            peer = ((rep + k) % reps, me[1])
            send(block, block, sends_g, recvs_g, u * (reps - 1) + k - 1, peer)

    stages = (over_core, over_rep, over_near, over_far)
    for step in range(size + len(stages) - 1):
        for lag, stage in enumerate(stages):
            if 0 <= step - lag < size:
                stage(step - lag)
    for u, (a, start, width) in enumerate(units):
        for k in range(1, reps):
            block = outs[a].at[(rep + reps - k) % reps, :, pl.ds(start, width)]
            arrived(block, sends_g, recvs_g, u * (reps - 1) + k - 1)
    for copy in sent:
        copy.wait_send()


def split_rows(part):
    reps = lax.axis_size("rep")
    rows, width = part.shape
    return part.reshape(2, 2, 2, reps, rows // (8 * reps), width)


def reduce_many(blocks, pieces, identity):
    reps = lax.axis_size("rep")
    count = len(blocks)
    units = [
        (at, low, size)
        for at, block in enumerate(blocks)
        for low, size in cut(block.shape[5], pieces[at])
    ]
    dma = pltpu.SemaphoreType.DMA
    vmem = pl.BlockSpec(memory_space=pltpu.VMEM)

    def buffers(*lead):
        return [
            pltpu.VMEM(lead + (blocks[at].shape[4], size), blocks[at].dtype)
            for at, _, size in units
        ]

    total = len(units)
    sums = pl.pallas_call(
        functools.partial(reduce_kernel, units, count, reps),
        out_shape=[
            jax.ShapeDtypeStruct((reps,) + block.shape[4:], block.dtype) for block in blocks
        ],
        in_specs=[vmem] * count,
        out_specs=[vmem] * count,
        scratch_shapes=buffers(2, 2, reps)
        + buffers(reps - 1, 2, 2)
        + buffers(2)
        + buffers()
        + buffers(2, 2)
        + [dma((total,))] * 2
        + [dma((total * (reps - 1),))] * 2
        + [dma((total * 2,))] * 2
        + [dma((total * (reps - 1),))] * 2,
        compiler_params=pltpu.CompilerParams(
            collective_id=identity, has_side_effects=True, vmem_limit_bytes=56 * 1024 * 1024
        ),
    )(*blocks)
    return [total.reshape(-1, total.shape[2]).astype(F32) for total in sums]


def blocked(shard):
    return shard.reshape(lax.axis_size("rep"), -1, shard.shape[1])


def divides(rows):
    reps = lax.axis_size("rep")
    return lax.axis_size("cp") == 8 and reps == 4 and rows % (8 * reps) == 0


def on_device(
    tokens,
    query_weight,
    query_bias,
    key_weight,
    value_weight,
    value_bias,
    output_weight,
    output_bias,
    first_gain,
    first_shift,
    up_weight,
    up_bias,
    down_weight,
    down_bias,
    second_gain,
    second_shift,
    cotangent,
):
    row_count = tokens.shape[1]
    width = tokens.shape[2]
    local_tokens = tokens[0]
    fast = divides(query_weight.shape[0])
    reps = lax.axis_size("rep")
    proj_shard = jnp.concatenate([query_weight, mixed(key_weight, value_weight)], axis=1)
    small = (
        query_bias,
        value_bias,
        output_bias,
        first_gain,
        first_shift,
        up_bias,
        down_bias,
        second_gain,
        second_shift,
    )
    flat_small = jnp.concatenate(small)
    if fast:
        unit = 8 * 128 * reps
        padded = jnp.pad(flat_small, (0, -flat_small.shape[0] % unit))
        w_proj, gathered = gather_many(
            (blocked(proj_shard), padded.reshape(reps, -1, 128)), (3, 1), 1
        )
        w_proj = w_proj.reshape(-1, proj_shard.shape[1])
        gathered = gathered.reshape(-1, padded.shape[0])
    else:
        w_proj = gather_all(proj_shard)
        gathered = lax.all_gather(flat_small[None], "cp", axis=0, tiled=True)
    vectors = []
    at = 0
    for vector in small:
        part = gathered[:, at : at + vector.shape[0]]
        vectors.append(part.reshape(-1).astype(F32))
        at += vector.shape[0]
    b_query, b_value, b_output, gain_one, shift_one, b_up, b_down, gain_two, shift_two = vectors
    w_pair = w_proj[:, width:]
    pair_bias = mixed(jnp.zeros_like(b_value)[None], b_value[None])
    pair_rows = (matmul(local_tokens, w_pair) + pair_bias).astype(BF16)
    chunk = width // CHUNKS
    pairs = [
        lax.all_gather(
            pair_rows[:, 2 * chunk * i : 2 * chunk * (i + 1)], "cp", axis=0, tiled=True
        )
        for i in range(CHUNKS)
    ]
    query_rows = (matmul(local_tokens, w_proj[:, :width]) + b_query).astype(BF16)
    query_scaled = query_rows * jnp.asarray(1.0 / math.sqrt(HD), BF16)
    queries = [query_scaled[:, chunk * i : chunk * (i + 1)] for i in range(CHUNKS)]
    wide_shard = jnp.concatenate([output_weight, up_weight], axis=1)
    if fast:
        wide_shard, down_shard, _ = lax.optimization_barrier(
            (wide_shard, down_weight, pair_rows)
        )
        w_wide, w_down = gather_many((blocked(wide_shard), blocked(down_shard)), (2, 2), 2)
        w_wide = w_wide.reshape(-1, wide_shard.shape[1])
        w_down = w_down.reshape(-1, width)
        w_wide, queries = lax.optimization_barrier((w_wide, queries))
    else:
        w_wide = gather_all(wide_shard)
        w_down = gather_all(down_weight)
    w_output = w_wide[:, :width]
    w_up = w_wide[:, width:]

    context_low = jnp.concatenate(
        [attend(query, pair) for query, pair in zip(queries, pairs)], axis=1
    )
    attn_out = matmul(context_low, w_output) + b_output
    resid_first = local_tokens.astype(F32) + attn_out
    first_norm, pull_first = jax.vjp(normalize, resid_first, gain_one, shift_one)
    first_low = first_norm.astype(BF16)
    inner_act = matmul(first_low, w_up) + b_up
    hidden, pull_gelu = jax.vjp(gelu_exact, inner_act)
    hidden_low = hidden.astype(BF16)
    resid_second = first_norm + (matmul(hidden_low, w_down) + b_down)
    layer_out, pull_second = jax.vjp(normalize, resid_second, gain_two, shift_two)

    grad_resid2, grad_gain2, grad_shift2 = pull_second(cotangent[0])
    grad_outer = grad_resid2.astype(BF16)
    grad_down_bias = column_sum(grad_outer)
    part_down = over_rows(hidden_low, grad_outer).astype(BF16)
    grad_inner = pull_gelu(against(grad_outer, w_down))[0].astype(BF16)
    grad_up_bias = column_sum(grad_inner)
    part_up = over_rows(first_low, grad_inner).astype(BF16)
    grad_first = grad_resid2 + against(grad_inner, w_up)
    grad_resid1, grad_gain1, grad_shift1 = pull_first(grad_first)
    grad_attn = grad_resid1.astype(BF16)
    grad_output_bias = column_sum(grad_attn)
    part_output = over_rows(context_low, grad_attn).astype(BF16)
    grad_context = against(grad_attn, w_output).astype(BF16)

    grad_queries = []
    grad_pairs = []
    terms = []
    for i in range(CHUNKS):
        grad_query, grad_terms = attend_back(
            queries[i], grad_context[:, chunk * i : chunk * (i + 1)], pairs[i]
        )
        grad_queries.append(grad_query)
        terms.append(grad_terms)
        grad_pairs.append(
            lax.psum_scatter(grad_terms, "cp", scatter_dimension=0, tiled=True)
        )
    grad_query_low = jnp.concatenate(grad_queries, axis=1)
    part_query = over_rows(local_tokens, grad_query_low).astype(BF16)
    if fast:
        parts = (part_down, part_up, part_output, part_query)
        parts, _ = lax.optimization_barrier((parts, terms))
        full_down, full_up, full_output, full_query = reduce_many(
            [split_rows(part) for part in parts], (2, 2, 1, 1), 3
        )
    grad_pair_low = jnp.concatenate(grad_pairs, axis=1)
    grad_proj = jnp.concatenate([grad_query_low, grad_pair_low], axis=1)
    part_pair = over_rows(local_tokens, grad_pair_low).astype(BF16)
    grad_tokens = grad_resid1 + against(grad_proj, w_proj)
    proj_sums = column_sum(grad_proj)
    _, grad_value_bias = unmixed(proj_sums[None, width:])

    small_grads = (
        proj_sums[:width],
        grad_value_bias[0],
        grad_output_bias,
        grad_gain1,
        grad_shift1,
        grad_up_bias,
        grad_down_bias,
        grad_gain2,
        grad_shift2,
    )
    owners = lax.axis_size("cp")
    total_sq = jnp.broadcast_to(jnp.sum(grad_tokens * grad_tokens), (owners, 1))
    flat = jnp.concatenate(
        [vector.reshape(owners, -1) for vector in small_grads] + [total_sq], axis=1
    )
    if fast:
        flat = jnp.pad(flat, ((0, 0), (0, -flat.shape[1] % (8 * 128 * reps))))
        full_pair, sums = reduce_many(
            (split_rows(part_pair), flat.reshape(2, 2, 2, reps, -1, 128)), (3, 1), 4
        )
        sums = sums.reshape(-1)
    else:
        shards = [
            scatter_all(part)
            for part in (part_down, part_up, part_output, part_query, part_pair)
        ]
        full_down, full_up, full_output, full_query, full_pair = [
            part.astype(F32) for part in lax.psum(tuple(shards), "rep")
        ]
        sums = lax.psum(flat, ("rep", "cp"))
        sums = lax.dynamic_slice_in_dim(sums, lax.axis_index("cp"), 1, 0)[0]
    reduced = []
    at = 0
    for shard in small:
        reduced.append(sums[at : at + shard.shape[0]])
        at += shard.shape[0]
    entries = lax.axis_size("rep") * owners * row_count * width
    rms_values = jnp.sqrt(sums[at : at + 1] / entries)

    grad_key_weight, grad_value_weight = unmixed(full_pair)
    return (
        layer_out[None],
        grad_tokens[None],
        full_query,
        reduced[0],
        grad_key_weight,
        grad_value_weight,
        reduced[1],
        full_output,
        reduced[2],
        reduced[3],
        reduced[4],
        full_up,
        reduced[5],
        full_down,
        reduced[6],
        reduced[7],
        reduced[8],
        rms_values,
    )


def solution(mesh):
    rows = P("cp", None)
    vector = P("cp")
    whole = P("rep", "cp", None)
    params = (
        rows,
        vector,
        rows,
        rows,
        vector,
        rows,
        vector,
        vector,
        vector,
        rows,
        vector,
        rows,
        vector,
        vector,
        vector,
    )
    return jax.shard_map(
        on_device,
        mesh=mesh,
        in_specs=(whole,) + params + (whole,),
        out_specs=(whole, whole) + params + (P(),),
        check_vma=False,
    )
```

```python
import functools
import math

import jax
import jax.numpy as jnp
from jax import lax
from jax.experimental import pallas as pl
from jax.experimental.pallas import tpu as pltpu
from jax.sharding import PartitionSpec as P

HD = 64
PAIR = 2 * HD
CHUNKS = 3
EPSILON = 1e-12
BF16 = jnp.bfloat16
F32 = jnp.float32
MESH = pl.DeviceIdType.MESH


def normalize(values, norm_gain, norm_shift):
    center = values - jnp.mean(values, axis=-1, keepdims=True)
    spread = jnp.mean(center * center, axis=-1, keepdims=True)
    return center * lax.rsqrt(spread + EPSILON) * norm_gain + norm_shift


def gelu_exact(values):
    return 0.5 * values * (1.0 + lax.erf(values * (1.0 / math.sqrt(2.0))))


def matmul(left, right):
    return jnp.dot(left, right, preferred_element_type=F32)


def over_rows(left, right):
    return lax.dot_general(left, right, (((0,), (0,)), ((), ())), preferred_element_type=F32)


def against(left, right):
    return lax.dot_general(left, right, (((1,), (1,)), ((), ())), preferred_element_type=F32)


def column_sum(values):
    return jnp.sum(values.astype(F32), axis=0)


def head_mask(shape, head):
    lane = lax.broadcasted_iota(jnp.int32, shape, 1)
    return (lane >= head * HD) & (lane < (head + 1) * HD)


def forward_kernel(query_ref, pair_ref, context_ref):
    keys = pair_ref[:, :PAIR]
    values = pair_ref[:, PAIR:]
    query = query_ref[...]
    total = None
    for head in range(2):
        mask = head_mask(query.shape, head)
        scores = against(jnp.where(mask, query, jnp.zeros_like(query)), keys)
        top = jnp.max(scores, axis=-1, keepdims=True)
        weight = jnp.exp(scores - top)
        inverse = 1.0 / jnp.sum(weight, axis=-1, keepdims=True)
        part = matmul((weight * inverse).astype(BF16), values)
        total = part if head == 0 else jnp.where(mask, part, total)
    context_ref[...] = total.astype(BF16)


def backward_kernel(query_ref, grad_ref, pair_ref, grad_query_ref, grad_pair_ref):
    keys = pair_ref[:, :PAIR]
    values = pair_ref[:, PAIR:]
    query = query_ref[...]
    grad = grad_ref[...]
    zeros = jnp.zeros_like(query)
    key_part = value_part = query_part = None
    for head in range(2):
        mask = head_mask(query.shape, head)
        own_query = jnp.where(mask, query, zeros)
        own_grad = jnp.where(mask, grad, zeros)
        scores = against(keys, own_query)
        top = jnp.max(scores, axis=0, keepdims=True)
        weight = jnp.exp(scores - top)
        inverse = 1.0 / jnp.sum(weight, axis=0, keepdims=True)
        probs = weight * inverse
        grad_probs = against(values, own_grad)
        delta = jnp.sum(probs * grad_probs, axis=0, keepdims=True)
        grad_scores = (probs * (grad_probs - delta)).astype(BF16)
        new_value = matmul(probs.astype(BF16), own_grad)
        new_key = matmul(grad_scores, own_query)
        new_query = over_rows(keys, grad_scores)
        if head == 0:
            key_part, value_part, query_part = new_key, new_value, new_query
        else:
            key_part = key_part + new_key
            value_part = value_part + new_value
            row = lax.broadcasted_iota(jnp.int32, new_query.shape, 0)
            query_part = jnp.where(row < HD, query_part, new_query)
    grad_query_ref[...] = (query_part.T * (1.0 / math.sqrt(HD))).astype(BF16)
    grad_pair_ref[:, :PAIR] = key_part.astype(BF16)
    grad_pair_ref[:, PAIR:] = value_part.astype(BF16)


def column_block(rows, width):
    return pl.BlockSpec((rows, width), lambda i: (0, i))


def attend(query, pairs):
    rows, width = query.shape
    keys = pairs.shape[0]
    return pl.pallas_call(
        forward_kernel,
        grid=(width // PAIR,),
        in_specs=[column_block(rows, PAIR), column_block(keys, 2 * PAIR)],
        out_specs=column_block(rows, PAIR),
        out_shape=jax.ShapeDtypeStruct((rows, width), BF16),
    )(query, pairs)


def attend_back(query, grad, pairs):
    rows, width = query.shape
    keys = pairs.shape[0]
    return pl.pallas_call(
        backward_kernel,
        grid=(width // PAIR,),
        in_specs=[
            column_block(rows, PAIR),
            column_block(rows, PAIR),
            column_block(keys, 2 * PAIR),
        ],
        out_specs=(column_block(rows, PAIR), column_block(keys, 2 * PAIR)),
        out_shape=(
            jax.ShapeDtypeStruct((rows, width), BF16),
            jax.ShapeDtypeStruct((keys, 2 * width), BF16),
        ),
    )(query, grad, pairs)


def mixed(left, right):
    parts = []
    for low in range(0, left.shape[1], PAIR):
        parts += [left[:, low : low + PAIR], right[:, low : low + PAIR]]
    return jnp.concatenate(parts, axis=1)


def unmixed(both):
    starts = range(0, both.shape[1], 2 * PAIR)
    return (
        jnp.concatenate([both[:, low : low + PAIR] for low in starts], axis=1),
        jnp.concatenate([both[:, low + PAIR : low + 2 * PAIR] for low in starts], axis=1),
    )


def gather_all(shard):
    return lax.all_gather(shard, "cp", axis=0, tiled=True)


def scatter_all(values):
    return lax.psum_scatter(values.astype(BF16), "cp", scatter_dimension=0, tiled=True)


def places():
    rep = lax.axis_index("rep")
    cp = lax.axis_index("cp")
    return rep, cp // 4, (cp // 2) % 2, cp % 2


def place_of(high, low, core):
    return 4 * high + 2 * low + core


def enter(reps):
    rep, high, low, core = places()
    barrier = pltpu.get_barrier_semaphore()
    peers = [
        (rep, place_of(high, low, 1 - core)),
        (rep, place_of(high, 1 - low, core)),
        (rep, place_of(1 - high, low, core)),
    ]
    peers += [((rep + k) % reps, place_of(high, low, core)) for k in range(1, reps)]
    for peer in peers:
        pl.semaphore_signal(barrier, inc=1, device_id=peer, device_id_type=MESH)
    pl.semaphore_wait(barrier, len(peers))


def remote(src, dst, sends, recvs, at, peer):
    return pltpu.make_async_remote_copy(
        src_ref=src,
        dst_ref=dst,
        send_sem=sends.at[at],
        recv_sem=recvs.at[at],
        device_id=peer,
        device_id_type=MESH,
    )


def gather_kernel(units, count, reps, *refs):
    ins = refs[:count]
    outs = refs[count : 2 * count]
    sends_z, recvs_z, sends_r, recvs_r, sends_c, recvs_c, local = refs[2 * count :]
    rep, high, low, core = places()
    me = (rep, place_of(high, low, core))
    sibling = (rep, place_of(high, low, 1 - core))
    far = (rep, place_of(1 - high, low, core))
    near = (rep, place_of(high, 1 - low, core))
    enter(reps)
    sent = []
    copies = []

    def send(src, dst, sends, recvs, at, peer):
        copy = remote(src, dst, sends, recvs, at, peer)
        copy.start()
        sent.append(copy)

    def arrived(block, sends, recvs, at):
        remote(block, block, sends, recvs, at, me).wait_recv()

    origins = (
        (high, low),
        (high, 1 - low),
        (1 - high, low),
        (1 - high, 1 - low),
    )

    def block_of(u, which, side, quarter):
        at, start, size = units[u]
        from_high, from_low = origins[which]
        return outs[at].at[from_high, from_low, side, quarter, :, pl.ds(start, size)]

    for u, (at, start, size) in enumerate(units):
        block = ins[at].at[rep, :, pl.ds(start, size)]
        send(block, block_of(u, 0, core, rep), sends_z, recvs_z, 3 * u + 1, far)
        send(block, block_of(u, 0, core, rep), sends_z, recvs_z, 3 * u, near)
    for u, (at, start, size) in enumerate(units):
        whole = ins[at].at[:, :, pl.ds(start, size)]
        send(whole, block_of(u, 0, core, slice(None)), sends_c, recvs_c, 4 * u, sibling)
    for at in range(count):
        copy = pltpu.make_async_copy(ins[at], outs[at].at[high, low, core], local.at[at])
        copy.start()
        copies.append(copy)

    def spread(u, which):
        block = block_of(u, which, core, rep)
        arrived(block, sends_z, recvs_z, 3 * u + which - 1)
        if which == 2:
            send(block, block, sends_z, recvs_z, 3 * u + 2, near)
        for j in range(1, reps):
            index = (3 * u + which - 1) * (reps - 1) + j - 1
            peer = ((rep + j) % reps, me[1])
            send(block, block, sends_r, recvs_r, index, peer)

    def pass_on(u, which):
        for j in range(1, reps):
            index = (3 * u + which - 1) * (reps - 1) + j - 1
            block = block_of(u, which, core, (rep + reps - j) % reps)
            arrived(block, sends_r, recvs_r, index)
        whole = block_of(u, which, core, slice(None))
        send(whole, whole, sends_c, recvs_c, 4 * u + which, sibling)

    total = len(units)
    for step in range(total + 2):
        if step < total:
            spread(step, 1)
            spread(step, 2)
        if 1 <= step < total + 1:
            spread(step - 1, 3)
        if 2 <= step:
            for which in range(1, 4):
                pass_on(step - 2, which)
    for u in range(total):
        for which in range(4):
            block = block_of(u, which, 1 - core, slice(None))
            arrived(block, sends_c, recvs_c, 4 * u + which)
    for copy in sent:
        copy.wait_send()
    for copy in copies:
        copy.wait()


def cut(width, pieces):
    size = width // pieces
    if size % 128:
        return [(0, width)]
    return [(size * i, size) for i in range(pieces)]


def gather_many(shards, pieces, identity):
    reps = lax.axis_size("rep")
    count = len(shards)
    units = [
        (at, low, size)
        for at, shard in enumerate(shards)
        for low, size in cut(shard.shape[2], pieces[at])
    ]
    total = len(units)
    hops = 3 * total * (reps - 1)
    dma = pltpu.SemaphoreType.DMA
    return pl.pallas_call(
        functools.partial(gather_kernel, units, count, reps),
        out_shape=[
            jax.ShapeDtypeStruct((2, 2, 2) + shard.shape, shard.dtype) for shard in shards
        ],
        in_specs=[pl.BlockSpec(memory_space=pl.ANY)] * count,
        out_specs=[pl.BlockSpec(memory_space=pl.ANY)] * count,
        scratch_shapes=[dma((3 * total,))] * 2
        + [dma((hops,))] * 2
        + [dma((4 * total,))] * 2
        + [dma((count,))],
        compiler_params=pltpu.CompilerParams(collective_id=identity, has_side_effects=True),
    )(*shards)


def summed(parts, kind):
    total = parts[0].astype(F32)
    for part in parts[1:]:
        total = total + part.astype(F32)
    return total.astype(kind)


def reduce_kernel(units, count, reps, *refs):
    ins = refs[:count]
    outs = refs[count : 2 * count]
    at = 2 * count
    size = len(units)
    first, second, third, fourth, own = [
        refs[at + i * size : at + (i + 1) * size] for i in range(5)
    ]
    sems = refs[at + 5 * size :]
    sends_c, recvs_c, sends_r, recvs_r, sends_z, recvs_z, sends_g, recvs_g = sems
    rep, high, low, core = places()
    me = (rep, place_of(high, low, core))
    sibling = (rep, place_of(high, low, 1 - core))
    far = (rep, place_of(1 - high, low, core))
    near = (rep, place_of(high, 1 - low, core))
    enter(reps)
    sent = []

    def send(src, dst, sends, recvs, at, peer):
        copy = remote(src, dst, sends, recvs, at, peer)
        copy.start()
        sent.append(copy)

    def arrived(block, sends, recvs, at):
        remote(block, block, sends, recvs, at, me).wait_recv()

    for u, (a, start, width) in enumerate(units):
        block = ins[a].at[:, :, 1 - core, :, :, pl.ds(start, width)]
        send(block, first[u], sends_c, recvs_c, u, sibling)

    def over_core(u):
        a, start, width = units[u]
        arrived(first[u], sends_c, recvs_c, u)

        def step(i, carry):
            h, w, q = i // (2 * reps), (i // reps) % 2, i % reps
            mine = ins[a][h, w, core, q, :, start : start + width]
            first[u][h, w, q] = summed([first[u][h, w, q], mine], first[u].dtype)
            return carry

        lax.fori_loop(0, 4 * reps, step, 0)
        for k in range(1, reps):
            target = (rep + k) % reps
            send(
                first[u].at[:, :, target],
                second[u].at[k - 1],
                sends_r,
                recvs_r,
                u * (reps - 1) + k - 1,
                (target, me[1]),
            )

    def over_rep(u):
        for k in range(1, reps):
            arrived(second[u].at[k - 1], sends_r, recvs_r, u * (reps - 1) + k - 1)

        def step(i, carry):
            h, w = i // 2, i % 2
            parts = [first[u][h, w, rep]] + [second[u][k, h, w] for k in range(reps - 1)]
            own[u][h, w] = summed(parts, own[u].dtype)
            return carry

        lax.fori_loop(0, 4, step, 0)
        send(own[u].at[:, 1 - low], third[u], sends_z, recvs_z, 2 * u, near)

    def over_near(u):
        arrived(third[u], sends_z, recvs_z, 2 * u)
        for h in range(2):
            own[u][h, low] = summed([own[u][h, low], third[u][h]], own[u].dtype)
        send(own[u].at[1 - high, low], fourth[u], sends_z, recvs_z, 2 * u + 1, far)

    def over_far(u):
        a, start, width = units[u]
        arrived(fourth[u], sends_z, recvs_z, 2 * u + 1)
        outs[a][rep, :, start : start + width] = summed(
            [own[u][high, low], fourth[u][...]], outs[a].dtype
        )
        block = outs[a].at[rep, :, pl.ds(start, width)]
        for k in range(1, reps):
            peer = ((rep + k) % reps, me[1])
            send(block, block, sends_g, recvs_g, u * (reps - 1) + k - 1, peer)

    stages = (over_core, over_rep, over_near, over_far)
    for step in range(size + len(stages) - 1):
        for lag, stage in enumerate(stages):
            if 0 <= step - lag < size:
                stage(step - lag)
    for u, (a, start, width) in enumerate(units):
        for k in range(1, reps):
            block = outs[a].at[(rep + reps - k) % reps, :, pl.ds(start, width)]
            arrived(block, sends_g, recvs_g, u * (reps - 1) + k - 1)
    for copy in sent:
        copy.wait_send()


def split_rows(part):
    reps = lax.axis_size("rep")
    rows, width = part.shape
    return part.reshape(2, 2, 2, reps, rows // (8 * reps), width)


def reduce_many(blocks, pieces, identity):
    reps = lax.axis_size("rep")
    count = len(blocks)
    units = [
        (at, low, size)
        for at, block in enumerate(blocks)
        for low, size in cut(block.shape[5], pieces[at])
    ]
    dma = pltpu.SemaphoreType.DMA
    vmem = pl.BlockSpec(memory_space=pltpu.VMEM)

    def buffers(*lead):
        return [
            pltpu.VMEM(lead + (blocks[at].shape[4], size), blocks[at].dtype)
            for at, _, size in units
        ]

    total = len(units)
    sums = pl.pallas_call(
        functools.partial(reduce_kernel, units, count, reps),
        out_shape=[
            jax.ShapeDtypeStruct((reps,) + block.shape[4:], block.dtype) for block in blocks
        ],
        in_specs=[vmem] * count,
        out_specs=[vmem] * count,
        scratch_shapes=buffers(2, 2, reps)
        + buffers(reps - 1, 2, 2)
        + buffers(2)
        + buffers()
        + buffers(2, 2)
        + [dma((total,))] * 2
        + [dma((total * (reps - 1),))] * 2
        + [dma((total * 2,))] * 2
        + [dma((total * (reps - 1),))] * 2,
        compiler_params=pltpu.CompilerParams(
            collective_id=identity, has_side_effects=True, vmem_limit_bytes=56 * 1024 * 1024
        ),
    )(*blocks)
    return [total.reshape(-1, total.shape[2]).astype(F32) for total in sums]


def blocked(shard):
    return shard.reshape(lax.axis_size("rep"), -1, shard.shape[1])


def divides(rows):
    reps = lax.axis_size("rep")
    return lax.axis_size("cp") == 8 and reps == 4 and rows % (8 * reps) == 0


def on_device(
    tokens,
    query_weight,
    query_bias,
    key_weight,
    value_weight,
    value_bias,
    output_weight,
    output_bias,
    first_gain,
    first_shift,
    up_weight,
    up_bias,
    down_weight,
    down_bias,
    second_gain,
    second_shift,
    cotangent,
):
    row_count = tokens.shape[1]
    width = tokens.shape[2]
    local_tokens = tokens[0]
    fast = divides(query_weight.shape[0])
    reps = lax.axis_size("rep")
    proj_shard = jnp.concatenate([query_weight, mixed(key_weight, value_weight)], axis=1)
    small = (
        query_bias,
        value_bias,
        output_bias,
        first_gain,
        first_shift,
        up_bias,
        down_bias,
        second_gain,
        second_shift,
    )
    if fast:
        rows = []
        for vector in small:
            lines = -(-vector.shape[0] // 128)
            rows.append(
                jnp.pad(vector.astype(F32), (0, 128 * lines - vector.shape[0])).reshape(lines, 128)
            )
        packed = jnp.concatenate(rows, axis=0)
        packed = jnp.pad(packed, ((0, -packed.shape[0] % (8 * reps)), (0, 0))).astype(BF16)
        w_proj, gathered = gather_many(
            (blocked(proj_shard), blocked(packed)), (3, 1), 1
        )
        w_proj = w_proj.reshape(-1, proj_shard.shape[1])
        gathered = gathered.reshape(-1, packed.shape[0], 128)
    else:
        w_proj = gather_all(proj_shard)
        gathered = lax.all_gather(jnp.concatenate(small)[None], "cp", axis=0, tiled=True)
    vectors = []
    at = 0
    for vector in small:
        size = vector.shape[0]
        if fast:
            lines = -(-size // 128)
            part = gathered[:, at : at + lines].reshape(-1, 128 * lines)[:, :size]
            at += lines
        else:
            part = gathered[:, at : at + size]
            at += size
        vectors.append(part.reshape(-1).astype(F32))
    b_query, b_value, b_output, gain_one, shift_one, b_up, b_down, gain_two, shift_two = vectors
    w_pair = w_proj[:, width:]
    pair_bias = mixed(jnp.zeros_like(b_value)[None], b_value[None])
    pair_rows = (matmul(local_tokens, w_pair) + pair_bias).astype(BF16)
    chunk = width // CHUNKS
    pairs = [
        lax.all_gather(
            pair_rows[:, 2 * chunk * i : 2 * chunk * (i + 1)], "cp", axis=0, tiled=True
        )
        for i in range(CHUNKS)
    ]
    query_rows = (matmul(local_tokens, w_proj[:, :width]) + b_query).astype(BF16)
    query_scaled = query_rows * jnp.asarray(1.0 / math.sqrt(HD), BF16)
    queries = [query_scaled[:, chunk * i : chunk * (i + 1)] for i in range(CHUNKS)]
    wide_shard = jnp.concatenate([output_weight, up_weight], axis=1)
    if fast:
        wide_shard, down_shard, _ = lax.optimization_barrier(
            (wide_shard, down_weight, pair_rows)
        )
        w_wide, w_down = gather_many((blocked(wide_shard), blocked(down_shard)), (2, 2), 2)
        w_wide = w_wide.reshape(-1, wide_shard.shape[1])
        w_down = w_down.reshape(-1, width)
        w_wide, queries = lax.optimization_barrier((w_wide, queries))
    else:
        w_wide = gather_all(wide_shard)
        w_down = gather_all(down_weight)
    w_output = w_wide[:, :width]
    w_up = w_wide[:, width:]

    context_low = jnp.concatenate(
        [attend(query, pair) for query, pair in zip(queries, pairs)], axis=1
    )
    attn_out = matmul(context_low, w_output) + b_output
    resid_first = local_tokens.astype(F32) + attn_out
    first_norm, pull_first = jax.vjp(normalize, resid_first, gain_one, shift_one)
    first_low = first_norm.astype(BF16)
    inner_act = matmul(first_low, w_up) + b_up
    hidden, pull_gelu = jax.vjp(gelu_exact, inner_act)
    hidden_low = hidden.astype(BF16)
    resid_second = first_norm + (matmul(hidden_low, w_down) + b_down)
    layer_out, pull_second = jax.vjp(normalize, resid_second, gain_two, shift_two)

    grad_resid2, grad_gain2, grad_shift2 = pull_second(cotangent[0])
    grad_outer = grad_resid2.astype(BF16)
    grad_down_bias = column_sum(grad_outer)
    part_down = over_rows(hidden_low, grad_outer).astype(BF16)
    grad_inner = pull_gelu(against(grad_outer, w_down))[0].astype(BF16)
    grad_up_bias = column_sum(grad_inner)
    part_up = over_rows(first_low, grad_inner).astype(BF16)
    grad_first = grad_resid2 + against(grad_inner, w_up)
    grad_resid1, grad_gain1, grad_shift1 = pull_first(grad_first)
    grad_attn = grad_resid1.astype(BF16)
    grad_output_bias = column_sum(grad_attn)
    part_output = over_rows(context_low, grad_attn).astype(BF16)
    grad_context = against(grad_attn, w_output).astype(BF16)

    grad_queries = []
    grad_pairs = []
    terms = []
    for i in range(CHUNKS):
        grad_query, grad_terms = attend_back(
            queries[i], grad_context[:, chunk * i : chunk * (i + 1)], pairs[i]
        )
        grad_queries.append(grad_query)
        terms.append(grad_terms)
        grad_pairs.append(
            lax.psum_scatter(grad_terms, "cp", scatter_dimension=0, tiled=True)
        )
    grad_query_low = jnp.concatenate(grad_queries, axis=1)
    part_query = over_rows(local_tokens, grad_query_low).astype(BF16)
    if fast:
        parts = (part_down, part_up, part_output, part_query)
        parts, _ = lax.optimization_barrier((parts, terms))
        full_down, full_up, full_output, full_query = reduce_many(
            [split_rows(part) for part in parts], (2, 2, 1, 1), 3
        )
    grad_pair_low = jnp.concatenate(grad_pairs, axis=1)
    grad_proj = jnp.concatenate([grad_query_low, grad_pair_low], axis=1)
    part_pair = over_rows(local_tokens, grad_pair_low).astype(BF16)
    grad_tokens = grad_resid1 + against(grad_proj, w_proj)
    proj_sums = column_sum(grad_proj)
    _, grad_value_bias = unmixed(proj_sums[None, width:])

    small_grads = (
        proj_sums[:width],
        grad_value_bias[0],
        grad_output_bias,
        grad_gain1,
        grad_shift1,
        grad_up_bias,
        grad_down_bias,
        grad_gain2,
        grad_shift2,
    )
    owners = lax.axis_size("cp")
    total_sq = jnp.broadcast_to(jnp.sum(grad_tokens * grad_tokens), (owners, 1))
    flat = jnp.concatenate(
        [vector.reshape(owners, -1) for vector in small_grads] + [total_sq], axis=1
    )
    if fast:
        flat = jnp.pad(flat, ((0, 0), (0, -flat.shape[1] % (8 * 128 * reps))))
        full_pair, sums = reduce_many(
            (split_rows(part_pair), flat.reshape(2, 2, 2, reps, -1, 128)), (3, 1), 4
        )
        sums = sums.reshape(-1)
    else:
        shards = [
            scatter_all(part)
            for part in (part_down, part_up, part_output, part_query, part_pair)
        ]
        full_down, full_up, full_output, full_query, full_pair = [
            part.astype(F32) for part in lax.psum(tuple(shards), "rep")
        ]
        sums = lax.psum(flat, ("rep", "cp"))
        sums = lax.dynamic_slice_in_dim(sums, lax.axis_index("cp"), 1, 0)[0]
    reduced = []
    at = 0
    for shard in small:
        reduced.append(sums[at : at + shard.shape[0]])
        at += shard.shape[0]
    entries = lax.axis_size("rep") * owners * row_count * width
    rms_values = jnp.sqrt(sums[at : at + 1] / entries)

    grad_key_weight, grad_value_weight = unmixed(full_pair)
    return (
        layer_out[None],
        grad_tokens[None],
        full_query,
        reduced[0],
        grad_key_weight,
        grad_value_weight,
        reduced[1],
        full_output,
        reduced[2],
        reduced[3],
        reduced[4],
        full_up,
        reduced[5],
        full_down,
        reduced[6],
        reduced[7],
        reduced[8],
        rms_values,
    )


def solution(mesh):
    rows = P("cp", None)
    vector = P("cp")
    whole = P("rep", "cp", None)
    params = (
        rows,
        vector,
        rows,
        rows,
        vector,
        rows,
        vector,
        vector,
        vector,
        rows,
        vector,
        rows,
        vector,
        vector,
        vector,
    )
    return jax.shard_map(
        on_device,
        mesh=mesh,
        in_specs=(whole,) + params + (whole,),
        out_specs=(whole, whole) + params + (P(),),
        check_vma=False,
    )
```

```python
import functools
import math

import jax
import jax.numpy as jnp
from jax import lax
from jax.experimental import pallas as pl
from jax.experimental.pallas import tpu as pltpu
from jax.sharding import PartitionSpec as P

HD = 64
PAIR = 2 * HD
CHUNKS = 3
EPSILON = 1e-12
BF16 = jnp.bfloat16
F32 = jnp.float32
MESH = pl.DeviceIdType.MESH


def normalize(values, norm_gain, norm_shift):
    center = values - jnp.mean(values, axis=-1, keepdims=True)
    spread = jnp.mean(center * center, axis=-1, keepdims=True)
    return center * lax.rsqrt(spread + EPSILON) * norm_gain + norm_shift


def gelu_exact(values):
    return 0.5 * values * (1.0 + lax.erf(values * (1.0 / math.sqrt(2.0))))


def matmul(left, right):
    return jnp.dot(left, right, preferred_element_type=F32)


def over_rows(left, right):
    return lax.dot_general(left, right, (((0,), (0,)), ((), ())), preferred_element_type=F32)


def against(left, right):
    return lax.dot_general(left, right, (((1,), (1,)), ((), ())), preferred_element_type=F32)


def column_sum(values):
    return jnp.sum(values.astype(F32), axis=0)


def head_mask(shape, head):
    lane = lax.broadcasted_iota(jnp.int32, shape, 1)
    return (lane >= head * HD) & (lane < (head + 1) * HD)


def forward_kernel(query_ref, pair_ref, context_ref):
    keys = pair_ref[:, :PAIR]
    values = pair_ref[:, PAIR:]
    query = query_ref[...]
    total = None
    for head in range(2):
        mask = head_mask(query.shape, head)
        scores = against(jnp.where(mask, query, jnp.zeros_like(query)), keys)
        top = jnp.max(scores, axis=-1, keepdims=True)
        weight = jnp.exp(scores - top)
        inverse = 1.0 / jnp.sum(weight, axis=-1, keepdims=True)
        part = matmul((weight * inverse).astype(BF16), values)
        total = part if head == 0 else jnp.where(mask, part, total)
    context_ref[...] = total.astype(BF16)


def pair_grads(query, grad, keys, values):
    zeros = jnp.zeros_like(query)
    key_part = value_part = query_part = None
    for head in range(2):
        mask = head_mask(query.shape, head)
        own_query = jnp.where(mask, query, zeros)
        own_grad = jnp.where(mask, grad, zeros)
        scores = against(keys, own_query)
        top = jnp.max(scores, axis=0, keepdims=True)
        weight = jnp.exp(scores - top)
        inverse = 1.0 / jnp.sum(weight, axis=0, keepdims=True)
        probs = weight * inverse
        grad_probs = against(values, own_grad)
        delta = jnp.sum(probs * grad_probs, axis=0, keepdims=True)
        grad_scores = (probs * (grad_probs - delta)).astype(BF16)
        new_value = matmul(probs.astype(BF16), own_grad)
        new_key = matmul(grad_scores, own_query)
        new_query = over_rows(keys, grad_scores)
        if head == 0:
            key_part, value_part, query_part = new_key, new_value, new_query
        else:
            key_part = key_part + new_key
            value_part = value_part + new_value
            row = lax.broadcasted_iota(jnp.int32, new_query.shape, 0)
            query_part = jnp.where(row < HD, query_part, new_query)
    query_part = (query_part.T * (1.0 / math.sqrt(HD))).astype(BF16)
    return query_part, key_part.astype(BF16), value_part.astype(BF16)


def backward_kernel(query_ref, grad_ref, pair_ref, grad_query_ref, grad_pair_ref):
    grad_query_ref[...], grad_pair_ref[:, :PAIR], grad_pair_ref[:, PAIR:] = pair_grads(
        query_ref[...], grad_ref[...], pair_ref[:, :PAIR], pair_ref[:, PAIR:]
    )


def column_block(rows, width):
    return pl.BlockSpec((rows, width), lambda i: (0, i))


def attend(query, pairs):
    rows, width = query.shape
    keys = pairs.shape[0]
    return pl.pallas_call(
        forward_kernel,
        grid=(width // PAIR,),
        in_specs=[column_block(rows, PAIR), column_block(keys, 2 * PAIR)],
        out_specs=column_block(rows, PAIR),
        out_shape=jax.ShapeDtypeStruct((rows, width), BF16),
    )(query, pairs)


def attend_back(query, grad, pairs):
    rows, width = query.shape
    keys = pairs.shape[0]
    return pl.pallas_call(
        backward_kernel,
        grid=(width // PAIR,),
        in_specs=[
            column_block(rows, PAIR),
            column_block(rows, PAIR),
            column_block(keys, 2 * PAIR),
        ],
        out_specs=(column_block(rows, PAIR), column_block(keys, 2 * PAIR)),
        out_shape=(
            jax.ShapeDtypeStruct((rows, width), BF16),
            jax.ShapeDtypeStruct((keys, 2 * width), BF16),
        ),
    )(query, grad, pairs)


def mixed(left, right):
    parts = []
    for low in range(0, left.shape[1], PAIR):
        parts += [left[:, low : low + PAIR], right[:, low : low + PAIR]]
    return jnp.concatenate(parts, axis=1)


def unmixed(both):
    starts = range(0, both.shape[1], 2 * PAIR)
    return (
        jnp.concatenate([both[:, low : low + PAIR] for low in starts], axis=1),
        jnp.concatenate([both[:, low + PAIR : low + 2 * PAIR] for low in starts], axis=1),
    )


def gather_all(shard):
    return lax.all_gather(shard, "cp", axis=0, tiled=True)


def scatter_all(values):
    return lax.psum_scatter(values.astype(BF16), "cp", scatter_dimension=0, tiled=True)


def places():
    rep = lax.axis_index("rep")
    cp = lax.axis_index("cp")
    return rep, cp // 4, (cp // 2) % 2, cp % 2


def place_of(high, low, core):
    return 4 * high + 2 * low + core


def enter(reps):
    rep, high, low, core = places()
    barrier = pltpu.get_barrier_semaphore()
    peers = [
        (rep, place_of(high, low, 1 - core)),
        (rep, place_of(high, 1 - low, core)),
        (rep, place_of(1 - high, low, core)),
    ]
    peers += [((rep + k) % reps, place_of(high, low, core)) for k in range(1, reps)]
    for peer in peers:
        pl.semaphore_signal(barrier, inc=1, device_id=peer, device_id_type=MESH)
    pl.semaphore_wait(barrier, len(peers))


def remote(src, dst, sends, recvs, at, peer):
    return pltpu.make_async_remote_copy(
        src_ref=src,
        dst_ref=dst,
        send_sem=sends.at[at],
        recv_sem=recvs.at[at],
        device_id=peer,
        device_id_type=MESH,
    )


def gather_kernel(units, count, reps, *refs):
    ins = refs[:count]
    outs = refs[count : 2 * count]
    sends_z, recvs_z, sends_r, recvs_r, sends_c, recvs_c, local = refs[2 * count :]
    rep, high, low, core = places()
    me = (rep, place_of(high, low, core))
    sibling = (rep, place_of(high, low, 1 - core))
    far = (rep, place_of(1 - high, low, core))
    near = (rep, place_of(high, 1 - low, core))
    enter(reps)
    sent = []
    copies = []

    def send(src, dst, sends, recvs, at, peer):
        copy = remote(src, dst, sends, recvs, at, peer)
        copy.start()
        sent.append(copy)

    def arrived(block, sends, recvs, at):
        remote(block, block, sends, recvs, at, me).wait_recv()

    origins = (
        (high, low),
        (high, 1 - low),
        (1 - high, low),
        (1 - high, 1 - low),
    )

    def block_of(u, which, side, quarter):
        at, start, size = units[u]
        from_high, from_low = origins[which]
        return outs[at].at[from_high, from_low, side, quarter, :, pl.ds(start, size)]

    for u, (at, start, size) in enumerate(units):
        block = ins[at].at[rep, :, pl.ds(start, size)]
        send(block, block_of(u, 0, core, rep), sends_z, recvs_z, 3 * u + 1, far)
        send(block, block_of(u, 0, core, rep), sends_z, recvs_z, 3 * u, near)
    for u, (at, start, size) in enumerate(units):
        whole = ins[at].at[:, :, pl.ds(start, size)]
        send(whole, block_of(u, 0, core, slice(None)), sends_c, recvs_c, 4 * u, sibling)
    for at in range(count):
        copy = pltpu.make_async_copy(ins[at], outs[at].at[high, low, core], local.at[at])
        copy.start()
        copies.append(copy)

    def spread(u, which):
        block = block_of(u, which, core, rep)
        arrived(block, sends_z, recvs_z, 3 * u + which - 1)
        if which == 2:
            send(block, block, sends_z, recvs_z, 3 * u + 2, near)
        for j in range(1, reps):
            index = (3 * u + which - 1) * (reps - 1) + j - 1
            peer = ((rep + j) % reps, me[1])
            send(block, block, sends_r, recvs_r, index, peer)

    def pass_on(u, which):
        for j in range(1, reps):
            index = (3 * u + which - 1) * (reps - 1) + j - 1
            block = block_of(u, which, core, (rep + reps - j) % reps)
            arrived(block, sends_r, recvs_r, index)
        whole = block_of(u, which, core, slice(None))
        send(whole, whole, sends_c, recvs_c, 4 * u + which, sibling)

    total = len(units)
    for step in range(total + 2):
        if step < total:
            spread(step, 1)
            spread(step, 2)
        if 1 <= step < total + 1:
            spread(step - 1, 3)
        if 2 <= step:
            for which in range(1, 4):
                pass_on(step - 2, which)
    for u in range(total):
        for which in range(4):
            block = block_of(u, which, 1 - core, slice(None))
            arrived(block, sends_c, recvs_c, 4 * u + which)
    for copy in sent:
        copy.wait_send()
    for copy in copies:
        copy.wait()


def cut(width, pieces):
    size = width // pieces
    if size % 128:
        return [(0, width)]
    return [(size * i, size) for i in range(pieces)]


def gather_many(shards, pieces, identity):
    reps = lax.axis_size("rep")
    count = len(shards)
    units = [
        (at, low, size)
        for at, shard in enumerate(shards)
        for low, size in cut(shard.shape[2], pieces[at])
    ]
    total = len(units)
    hops = 3 * total * (reps - 1)
    dma = pltpu.SemaphoreType.DMA
    return pl.pallas_call(
        functools.partial(gather_kernel, units, count, reps),
        out_shape=[
            jax.ShapeDtypeStruct((2, 2, 2) + shard.shape, shard.dtype) for shard in shards
        ],
        in_specs=[pl.BlockSpec(memory_space=pl.ANY)] * count,
        out_specs=[pl.BlockSpec(memory_space=pl.ANY)] * count,
        scratch_shapes=[dma((3 * total,))] * 2
        + [dma((hops,))] * 2
        + [dma((4 * total,))] * 2
        + [dma((count,))],
        compiler_params=pltpu.CompilerParams(collective_id=identity, has_side_effects=True),
    )(*shards)


def summed(parts, kind):
    total = parts[0].astype(F32)
    for part in parts[1:]:
        total = total + part.astype(F32)
    return total.astype(kind)


def reduce_kernel(units, count, reps, chunks, *refs):
    ins = refs[:count]
    at = count
    if chunks:
        query_ref, grad_ref = refs[at : at + 2]
        pair_refs = refs[at + 2 : at + 2 + chunks]
        at += 2 + chunks
    outs = refs[at : at + count]
    at += count
    if chunks:
        grad_query_ref, grad_pair_ref = refs[at : at + 2]
        at += 2
    size = len(units)
    first, second, third, fourth, own = [
        refs[at + i * size : at + (i + 1) * size] for i in range(5)
    ]
    sems = refs[at + 5 * size :]
    sends_c, recvs_c, sends_r, recvs_r, sends_z, recvs_z, sends_g, recvs_g = sems[:8]
    rep, high, low, core = places()
    me = (rep, place_of(high, low, core))
    sibling = (rep, place_of(high, low, 1 - core))
    far = (rep, place_of(1 - high, low, core))
    near = (rep, place_of(high, 1 - low, core))
    enter(reps)
    def send(src, dst, sends, recvs, at, peer):
        remote(src, dst, sends, recvs, at, peer).start()

    def left(block, sends, recvs, at):
        remote(block, block, sends, recvs, at, me).wait_send()

    def arrived(block, sends, recvs, at):
        remote(block, block, sends, recvs, at, me).wait_recv()

    for u, (a, start, width) in enumerate(units):
        block = ins[a].at[:, :, 1 - core, :, :, pl.ds(start, width)]
        send(block, first[u], sends_c, recvs_c, u, sibling)

    def over_core(u):
        a, start, width = units[u]
        arrived(first[u], sends_c, recvs_c, u)

        def step(i, carry):
            h, w, q = i // (2 * reps), (i // reps) % 2, i % reps
            mine = ins[a][h, w, core, q, :, start : start + width]
            first[u][h, w, q] = summed([first[u][h, w, q], mine], first[u].dtype)
            return carry

        lax.fori_loop(0, 4 * reps, step, 0)
        for k in range(1, reps):
            target = (rep + k) % reps
            send(
                first[u].at[:, :, target],
                second[u].at[k - 1],
                sends_r,
                recvs_r,
                u * (reps - 1) + k - 1,
                (target, me[1]),
            )

    def over_rep(u):
        for k in range(1, reps):
            arrived(second[u].at[k - 1], sends_r, recvs_r, u * (reps - 1) + k - 1)

        def step(i, carry):
            h, w = i // 2, i % 2
            parts = [first[u][h, w, rep]] + [second[u][k, h, w] for k in range(reps - 1)]
            own[u][h, w] = summed(parts, own[u].dtype)
            return carry

        lax.fori_loop(0, 4, step, 0)
        send(own[u].at[:, 1 - low], third[u], sends_z, recvs_z, 2 * u, near)

    def over_near(u):
        arrived(third[u], sends_z, recvs_z, 2 * u)
        for h in range(2):
            own[u][h, low] = summed([own[u][h, low], third[u][h]], own[u].dtype)
        send(own[u].at[1 - high, low], fourth[u], sends_z, recvs_z, 2 * u + 1, far)

    def over_far(u):
        a, start, width = units[u]
        arrived(fourth[u], sends_z, recvs_z, 2 * u + 1)
        outs[a][rep, :, start : start + width] = summed(
            [own[u][high, low], fourth[u][...]], outs[a].dtype
        )
        block = outs[a].at[rep, :, pl.ds(start, width)]
        for k in range(1, reps):
            peer = ((rep + k) % reps, me[1])
            send(block, block, sends_g, recvs_g, u * (reps - 1) + k - 1, peer)

    stages = (over_core, over_rep, over_near, over_far)

    def advance(step):
        for lag, stage in enumerate(stages):
            if 0 <= step - lag < size:
                stage(step - lag)

    steps = size + len(stages) - 1
    if not chunks:
        for step in range(steps):
            advance(step)
    else:
        terms, merged, from_near, from_far, held, sends_k, recvs_k, fetched = sems[8:]
        pairs = terms.shape[0]
        each = pairs // chunks

        def fetch(p, wait):
            for i in range(pairs):

                @pl.when(p == i)
                def _(i=i):
                    copy = pltpu.make_async_copy(
                        pair_refs[i // each].at[:, pl.ds(2 * PAIR * (i % each), 2 * PAIR)],
                        held.at[i % 2],
                        fetched.at[i % 2],
                    )
                    copy.wait() if wait else copy.start()

        def hop(p, which):
            if which == 0:
                return remote(
                    terms.at[p, :, :, 1 - core], merged.at[p], sends_k, recvs_k, 3 * p, sibling
                )
            if which == 1:
                return remote(
                    merged.at[p, :, 1 - low], from_near.at[p], sends_k, recvs_k, 3 * p + 1, near
                )
            return remote(
                merged.at[p, 1 - high, low], from_far.at[p], sends_k, recvs_k, 3 * p + 2, far
            )

        def merge_core(p):
            arrived(merged.at[p], sends_k, recvs_k, 3 * p)
            for h in range(2):
                for w in range(2):
                    both = [merged[p, h, w], terms[p, h, w, core]]
                    merged[p, h, w] = summed(both, BF16)
            hop(p, 1).start()

        def merge_near(p):
            arrived(from_near.at[p], sends_k, recvs_k, 3 * p + 1)
            for h in range(2):
                merged[p, h, low] = summed([merged[p, h, low], from_near[p, h]], BF16)
            hop(p, 2).start()

        def merge_far(p):
            arrived(from_far.at[p], sends_k, recvs_k, 3 * p + 2)
            cols = pl.ds(pl.multiple_of(p * 2 * PAIR, 2 * PAIR), 2 * PAIR)
            grad_pair_ref[:, cols] = summed([merged[p, high, low], from_far[p]], BF16)

        def compute(p):
            fetch(p, True)
            fetch(p + 1, False)
            cols = pl.ds(pl.multiple_of(p * PAIR, PAIR), PAIR)
            slot = p % 2
            query_part, key_part, value_part = pair_grads(
                query_ref[:, cols], grad_ref[:, cols], held[slot, :, :PAIR], held[slot, :, PAIR:]
            )
            grad_query_ref[:, cols] = query_part
            shape = terms.shape[1:5] + (PAIR,)
            terms[p, :, :, :, :, :PAIR] = key_part.reshape(shape)
            terms[p, :, :, :, :, PAIR:] = value_part.reshape(shape)
            hop(p, 0).start()

        fetch(0, False)

        def step_all(t, carry):
            for lag, merge in ((1, merge_core), (2, merge_near), (3, merge_far)):

                @pl.when((t >= lag) & (t < pairs + lag))
                def _(lag=lag, merge=merge):
                    merge(t - lag)

            @pl.when(t < pairs)
            def _():
                compute(t)

            for i in range(steps):

                @pl.when(t == i)
                def _(i=i):
                    advance(i)

            return carry

        lax.fori_loop(0, max(pairs + 3, steps), step_all, 0)
        for p in range(pairs):
            for which in range(3):
                hop(p, which).wait_send()
    for u, (a, start, width) in enumerate(units):
        for k in range(1, reps):
            block = outs[a].at[(rep + reps - k) % reps, :, pl.ds(start, width)]
            arrived(block, sends_g, recvs_g, u * (reps - 1) + k - 1)
    for u, (a, start, width) in enumerate(units):
        cols = pl.ds(start, width)
        left(ins[a].at[:, :, 1 - core, :, :, cols], sends_c, recvs_c, u)
        left(own[u].at[:, 1 - low], sends_z, recvs_z, 2 * u)
        left(own[u].at[1 - high, low], sends_z, recvs_z, 2 * u + 1)
        for k in range(1, reps):
            index = u * (reps - 1) + k - 1
            left(first[u].at[:, :, (rep + k) % reps], sends_r, recvs_r, index)
            left(outs[a].at[rep, :, cols], sends_g, recvs_g, index)


def split_rows(part):
    reps = lax.axis_size("rep")
    rows, width = part.shape
    return part.reshape(2, 2, 2, reps, rows // (8 * reps), width)


def reduce_many(blocks, pieces, identity, query=None, grad=None, pairs=()):
    reps = lax.axis_size("rep")
    count = len(blocks)
    units = [
        (at, low, size)
        for at, block in enumerate(blocks)
        for low, size in cut(block.shape[5], pieces[at])
    ]
    dma = pltpu.SemaphoreType.DMA
    vmem = pl.BlockSpec(memory_space=pltpu.VMEM)

    def buffers(*lead):
        return [
            pltpu.VMEM(lead + (blocks[at].shape[4], size), blocks[at].dtype)
            for at, _, size in units
        ]

    total = len(units)
    out_shape = [
        jax.ShapeDtypeStruct((reps,) + block.shape[4:], block.dtype) for block in blocks
    ]
    operands = list(blocks)
    in_specs = [vmem] * count
    more = []
    if pairs:
        tokens, width = query.shape
        number = width // PAIR
        block = (tokens, 2 * PAIR)
        operands += [query, grad] + list(pairs)
        in_specs += [vmem] * 2 + [pl.BlockSpec(memory_space=pl.ANY)] * len(pairs)
        out_shape += [
            jax.ShapeDtypeStruct((tokens, width), BF16),
            jax.ShapeDtypeStruct((tokens, 2 * width), BF16),
        ]
        more = [
            pltpu.VMEM((number, 2, 2, 2) + block, BF16),
            pltpu.VMEM((number, 2, 2) + block, BF16),
            pltpu.VMEM((number, 2) + block, BF16),
            pltpu.VMEM((number,) + block, BF16),
            pltpu.VMEM((2, pairs[0].shape[0], 2 * PAIR), BF16),
            dma((3 * number,)),
            dma((3 * number,)),
            dma((2,)),
        ]
    sums = pl.pallas_call(
        functools.partial(reduce_kernel, units, count, reps, len(pairs)),
        out_shape=out_shape,
        in_specs=in_specs,
        out_specs=[vmem] * len(out_shape),
        scratch_shapes=buffers(2, 2, reps)
        + buffers(reps - 1, 2, 2)
        + buffers(2)
        + buffers()
        + buffers(2, 2)
        + [dma((total,))] * 2
        + [dma((total * (reps - 1),))] * 2
        + [dma((total * 2,))] * 2
        + [dma((total * (reps - 1),))] * 2
        + more,
        compiler_params=pltpu.CompilerParams(
            collective_id=identity, has_side_effects=True, vmem_limit_bytes=60 * 1024 * 1024
        ),
    )(*operands)
    totals = [total.reshape(-1, total.shape[2]).astype(F32) for total in sums[:count]]
    return totals + list(sums[count:])


def blocked(shard):
    return shard.reshape(lax.axis_size("rep"), -1, shard.shape[1])


def divides(rows):
    reps = lax.axis_size("rep")
    return lax.axis_size("cp") == 8 and reps == 4 and rows % (8 * reps) == 0


def on_device(
    tokens,
    query_weight,
    query_bias,
    key_weight,
    value_weight,
    value_bias,
    output_weight,
    output_bias,
    first_gain,
    first_shift,
    up_weight,
    up_bias,
    down_weight,
    down_bias,
    second_gain,
    second_shift,
    cotangent,
):
    row_count = tokens.shape[1]
    width = tokens.shape[2]
    local_tokens = tokens[0]
    fast = divides(query_weight.shape[0])
    reps = lax.axis_size("rep")
    proj_shard = jnp.concatenate([query_weight, mixed(key_weight, value_weight)], axis=1)
    small = (
        query_bias,
        value_bias,
        output_bias,
        first_gain,
        first_shift,
        up_bias,
        down_bias,
        second_gain,
        second_shift,
    )
    if fast:
        rows = []
        for vector in small:
            lines = -(-vector.shape[0] // 128)
            rows.append(
                jnp.pad(vector.astype(F32), (0, 128 * lines - vector.shape[0])).reshape(lines, 128)
            )
        packed = jnp.concatenate(rows, axis=0)
        packed = jnp.pad(packed, ((0, -packed.shape[0] % (8 * reps)), (0, 0))).astype(BF16)
        w_proj, gathered = gather_many(
            (blocked(proj_shard), blocked(packed)), (3, 1), 1
        )
        w_proj = w_proj.reshape(-1, proj_shard.shape[1])
        gathered = gathered.reshape(-1, packed.shape[0], 128)
    else:
        w_proj = gather_all(proj_shard)
        gathered = lax.all_gather(jnp.concatenate(small)[None], "cp", axis=0, tiled=True)
    vectors = []
    at = 0
    for vector in small:
        size = vector.shape[0]
        if fast:
            lines = -(-size // 128)
            part = gathered[:, at : at + lines].reshape(-1, 128 * lines)[:, :size]
            at += lines
        else:
            part = gathered[:, at : at + size]
            at += size
        vectors.append(part.reshape(-1).astype(F32))
    b_query, b_value, b_output, gain_one, shift_one, b_up, b_down, gain_two, shift_two = vectors
    w_pair = w_proj[:, width:]
    pair_bias = mixed(jnp.zeros_like(b_value)[None], b_value[None])
    pair_rows = (matmul(local_tokens, w_pair) + pair_bias).astype(BF16)
    chunk = width // CHUNKS
    pairs = [
        lax.all_gather(
            pair_rows[:, 2 * chunk * i : 2 * chunk * (i + 1)], "cp", axis=0, tiled=True
        )
        for i in range(CHUNKS)
    ]
    query_rows = (matmul(local_tokens, w_proj[:, :width]) + b_query).astype(BF16)
    query_scaled = query_rows * jnp.asarray(1.0 / math.sqrt(HD), BF16)
    queries = [query_scaled[:, chunk * i : chunk * (i + 1)] for i in range(CHUNKS)]
    wide_shard = jnp.concatenate([output_weight, up_weight], axis=1)
    if fast:
        wide_shard, down_shard, _ = lax.optimization_barrier(
            (wide_shard, down_weight, pair_rows)
        )
        w_wide, w_down = gather_many((blocked(wide_shard), blocked(down_shard)), (2, 2), 2)
        w_wide = w_wide.reshape(-1, wide_shard.shape[1])
        w_down = w_down.reshape(-1, width)
        w_wide, queries = lax.optimization_barrier((w_wide, queries))
    else:
        w_wide = gather_all(wide_shard)
        w_down = gather_all(down_weight)
    w_output = w_wide[:, :width]
    w_up = w_wide[:, width:]

    context_low = jnp.concatenate(
        [attend(query, pair) for query, pair in zip(queries, pairs)], axis=1
    )
    attn_out = matmul(context_low, w_output) + b_output
    resid_first = local_tokens.astype(F32) + attn_out
    first_norm, pull_first = jax.vjp(normalize, resid_first, gain_one, shift_one)
    first_low = first_norm.astype(BF16)
    inner_act = matmul(first_low, w_up) + b_up
    hidden, pull_gelu = jax.vjp(gelu_exact, inner_act)
    hidden_low = hidden.astype(BF16)
    resid_second = first_norm + (matmul(hidden_low, w_down) + b_down)
    layer_out, pull_second = jax.vjp(normalize, resid_second, gain_two, shift_two)

    grad_resid2, grad_gain2, grad_shift2 = pull_second(cotangent[0])
    grad_outer = grad_resid2.astype(BF16)
    grad_down_bias = column_sum(grad_outer)
    part_down = over_rows(hidden_low, grad_outer).astype(BF16)
    grad_inner = pull_gelu(against(grad_outer, w_down))[0].astype(BF16)
    grad_up_bias = column_sum(grad_inner)
    part_up = over_rows(first_low, grad_inner).astype(BF16)
    grad_first = grad_resid2 + against(grad_inner, w_up)
    grad_resid1, grad_gain1, grad_shift1 = pull_first(grad_first)
    grad_attn = grad_resid1.astype(BF16)
    grad_output_bias = column_sum(grad_attn)
    part_output = over_rows(context_low, grad_attn).astype(BF16)
    grad_context = against(grad_attn, w_output).astype(BF16)

    if fast:
        full_down, full_up, full_output, grad_query_low, grad_pair_low = reduce_many(
            [split_rows(part) for part in (part_down, part_up, part_output)],
            (2, 2, 1),
            3,
            query_scaled,
            grad_context,
            pairs,
        )
    else:
        grad_queries = []
        grad_pairs = []
        for i in range(CHUNKS):
            grad_query, grad_terms = attend_back(
                queries[i], grad_context[:, chunk * i : chunk * (i + 1)], pairs[i]
            )
            grad_queries.append(grad_query)
            grad_pairs.append(
                lax.psum_scatter(grad_terms, "cp", scatter_dimension=0, tiled=True)
            )
        grad_query_low = jnp.concatenate(grad_queries, axis=1)
        grad_pair_low = jnp.concatenate(grad_pairs, axis=1)
    grad_proj = jnp.concatenate([grad_query_low, grad_pair_low], axis=1)
    part_proj = over_rows(local_tokens, grad_proj).astype(BF16)
    grad_tokens = grad_resid1 + against(grad_proj, w_proj)
    proj_sums = column_sum(grad_proj)
    _, grad_value_bias = unmixed(proj_sums[None, width:])

    small_grads = (
        proj_sums[:width],
        grad_value_bias[0],
        grad_output_bias,
        grad_gain1,
        grad_shift1,
        grad_up_bias,
        grad_down_bias,
        grad_gain2,
        grad_shift2,
    )
    owners = lax.axis_size("cp")
    total_sq = jnp.broadcast_to(jnp.sum(grad_tokens * grad_tokens), (owners, 1))
    flat = jnp.concatenate(
        [vector.reshape(owners, -1) for vector in small_grads] + [total_sq], axis=1
    )
    if fast:
        flat = jnp.pad(flat, ((0, 0), (0, -flat.shape[1] % (8 * 128 * reps))))
        full_proj, sums = reduce_many(
            (split_rows(part_proj), flat.reshape(2, 2, 2, reps, -1, 128)), (3, 1), 4
        )
        sums = sums.reshape(-1)
    else:
        shards = [
            scatter_all(part)
            for part in (part_down, part_up, part_output, part_proj)
        ]
        full_down, full_up, full_output, full_proj = [
            part.astype(F32) for part in lax.psum(tuple(shards), "rep")
        ]
        sums = lax.psum(flat, ("rep", "cp"))
        sums = lax.dynamic_slice_in_dim(sums, lax.axis_index("cp"), 1, 0)[0]
    reduced = []
    at = 0
    for shard in small:
        reduced.append(sums[at : at + shard.shape[0]])
        at += shard.shape[0]
    entries = lax.axis_size("rep") * owners * row_count * width
    rms_values = jnp.sqrt(sums[at : at + 1] / entries)

    grad_key_weight, grad_value_weight = unmixed(full_proj[:, width:])
    return (
        layer_out[None],
        grad_tokens[None],
        full_proj[:, :width],
        reduced[0],
        grad_key_weight,
        grad_value_weight,
        reduced[1],
        full_output,
        reduced[2],
        reduced[3],
        reduced[4],
        full_up,
        reduced[5],
        full_down,
        reduced[6],
        reduced[7],
        reduced[8],
        rms_values,
    )


def solution(mesh):
    rows = P("cp", None)
    vector = P("cp")
    whole = P("rep", "cp", None)
    params = (
        rows,
        vector,
        rows,
        rows,
        vector,
        rows,
        vector,
        vector,
        vector,
        rows,
        vector,
        rows,
        vector,
        vector,
        vector,
    )
    return jax.shard_map(
        on_device,
        mesh=mesh,
        in_specs=(whole,) + params + (whole,),
        out_specs=(whole, whole) + params + (P(),),
        check_vma=False,
    )
```

```python
import functools
import math

import jax
import jax.numpy as jnp
from jax import lax
from jax.experimental import pallas as pl
from jax.experimental.pallas import tpu as pltpu
from jax.sharding import PartitionSpec as P

HD = 64
PAIR = 2 * HD
CHUNKS = 3
EPSILON = 1e-12
BF16 = jnp.bfloat16
F32 = jnp.float32
MESH = pl.DeviceIdType.MESH


def normalize(values, norm_gain, norm_shift):
    center = values - jnp.mean(values, axis=-1, keepdims=True)
    spread = jnp.mean(center * center, axis=-1, keepdims=True)
    return center * lax.rsqrt(spread + EPSILON) * norm_gain + norm_shift


def gelu_exact(values):
    return 0.5 * values * (1.0 + lax.erf(values * (1.0 / math.sqrt(2.0))))


def matmul(left, right):
    return jnp.dot(left, right, preferred_element_type=F32)


def over_rows(left, right):
    return lax.dot_general(left, right, (((0,), (0,)), ((), ())), preferred_element_type=F32)


def against(left, right):
    return lax.dot_general(left, right, (((1,), (1,)), ((), ())), preferred_element_type=F32)


def column_sum(values):
    return jnp.sum(values.astype(F32), axis=0)


def head_mask(shape, head):
    lane = lax.broadcasted_iota(jnp.int32, shape, 1)
    return (lane >= head * HD) & (lane < (head + 1) * HD)


def pair_context(query, keys, values):
    total = None
    for head in range(2):
        mask = head_mask(query.shape, head)
        scores = against(jnp.where(mask, query, jnp.zeros_like(query)), keys)
        top = jnp.max(scores, axis=-1, keepdims=True)
        weight = jnp.exp(scores - top)
        inverse = 1.0 / jnp.sum(weight, axis=-1, keepdims=True)
        part = matmul((weight * inverse).astype(BF16), values)
        total = part if head == 0 else jnp.where(mask, part, total)
    return total.astype(BF16)


def forward_kernel(query_ref, pair_ref, context_ref):
    context_ref[...] = pair_context(query_ref[...], pair_ref[:, :PAIR], pair_ref[:, PAIR:])


def pair_grads(query, grad, keys, values):
    zeros = jnp.zeros_like(query)
    key_part = value_part = query_part = None
    for head in range(2):
        mask = head_mask(query.shape, head)
        own_query = jnp.where(mask, query, zeros)
        own_grad = jnp.where(mask, grad, zeros)
        scores = against(keys, own_query)
        top = jnp.max(scores, axis=0, keepdims=True)
        weight = jnp.exp(scores - top)
        inverse = 1.0 / jnp.sum(weight, axis=0, keepdims=True)
        probs = weight * inverse
        grad_probs = against(values, own_grad)
        delta = jnp.sum(probs * grad_probs, axis=0, keepdims=True)
        grad_scores = (probs * (grad_probs - delta)).astype(BF16)
        new_value = matmul(probs.astype(BF16), own_grad)
        new_key = matmul(grad_scores, own_query)
        new_query = over_rows(keys, grad_scores)
        if head == 0:
            key_part, value_part, query_part = new_key, new_value, new_query
        else:
            key_part = key_part + new_key
            value_part = value_part + new_value
            row = lax.broadcasted_iota(jnp.int32, new_query.shape, 0)
            query_part = jnp.where(row < HD, query_part, new_query)
    query_part = (query_part.T * (1.0 / math.sqrt(HD))).astype(BF16)
    return query_part, key_part.astype(BF16), value_part.astype(BF16)


def backward_kernel(query_ref, grad_ref, pair_ref, grad_query_ref, grad_pair_ref):
    grad_query_ref[...], grad_pair_ref[:, :PAIR], grad_pair_ref[:, PAIR:] = pair_grads(
        query_ref[...], grad_ref[...], pair_ref[:, :PAIR], pair_ref[:, PAIR:]
    )


def column_block(rows, width):
    return pl.BlockSpec((rows, width), lambda i: (0, i))


def attend(query, pairs):
    rows, width = query.shape
    keys = pairs.shape[0]
    return pl.pallas_call(
        forward_kernel,
        grid=(width // PAIR,),
        in_specs=[column_block(rows, PAIR), column_block(keys, 2 * PAIR)],
        out_specs=column_block(rows, PAIR),
        out_shape=jax.ShapeDtypeStruct((rows, width), BF16),
    )(query, pairs)


def attend_back(query, grad, pairs):
    rows, width = query.shape
    keys = pairs.shape[0]
    return pl.pallas_call(
        backward_kernel,
        grid=(width // PAIR,),
        in_specs=[
            column_block(rows, PAIR),
            column_block(rows, PAIR),
            column_block(keys, 2 * PAIR),
        ],
        out_specs=(column_block(rows, PAIR), column_block(keys, 2 * PAIR)),
        out_shape=(
            jax.ShapeDtypeStruct((rows, width), BF16),
            jax.ShapeDtypeStruct((keys, 2 * width), BF16),
        ),
    )(query, grad, pairs)


def mixed(left, right):
    parts = []
    for low in range(0, left.shape[1], PAIR):
        parts += [left[:, low : low + PAIR], right[:, low : low + PAIR]]
    return jnp.concatenate(parts, axis=1)


def unmixed(both):
    starts = range(0, both.shape[1], 2 * PAIR)
    return (
        jnp.concatenate([both[:, low : low + PAIR] for low in starts], axis=1),
        jnp.concatenate([both[:, low + PAIR : low + 2 * PAIR] for low in starts], axis=1),
    )


def gather_all(shard):
    return lax.all_gather(shard, "cp", axis=0, tiled=True)


def scatter_all(values):
    return lax.psum_scatter(values.astype(BF16), "cp", scatter_dimension=0, tiled=True)


def places():
    rep = lax.axis_index("rep")
    cp = lax.axis_index("cp")
    return rep, cp // 4, (cp // 2) % 2, cp % 2


def place_of(high, low, core):
    return 4 * high + 2 * low + core


def enter(reps):
    rep, high, low, core = places()
    barrier = pltpu.get_barrier_semaphore()
    peers = [
        (rep, place_of(high, low, 1 - core)),
        (rep, place_of(high, 1 - low, core)),
        (rep, place_of(1 - high, low, core)),
    ]
    peers += [((rep + k) % reps, place_of(high, low, core)) for k in range(1, reps)]
    for peer in peers:
        pl.semaphore_signal(barrier, inc=1, device_id=peer, device_id_type=MESH)
    pl.semaphore_wait(barrier, len(peers))


def remote(src, dst, sends, recvs, at, peer):
    return pltpu.make_async_remote_copy(
        src_ref=src,
        dst_ref=dst,
        send_sem=sends.at[at],
        recv_sem=recvs.at[at],
        device_id=peer,
        device_id_type=MESH,
    )


def gather_kernel(units, count, reps, pairs, *refs):
    ins = refs[:count]
    at = count
    if pairs:
        query_ref, rows_ref = refs[at : at + 2]
        at += 2
    outs = refs[at : at + count]
    at += count
    if pairs:
        context_ref, pair_ref = refs[at : at + 2]
        at += 2
    sends_z, recvs_z, sends_r, recvs_r, sends_c, recvs_c, local = refs[at : at + 7]
    rep, high, low, core = places()
    me = (rep, place_of(high, low, core))
    sibling = (rep, place_of(high, low, 1 - core))
    far = (rep, place_of(1 - high, low, core))
    near = (rep, place_of(high, 1 - low, core))
    enter(reps)
    copies = []

    def send(src, dst, sends, recvs, at, peer):
        remote(src, dst, sends, recvs, at, peer).start()

    def left(block, sends, recvs, at):
        remote(block, block, sends, recvs, at, me).wait_send()

    def arrived(block, sends, recvs, at):
        remote(block, block, sends, recvs, at, me).wait_recv()

    origins = (
        (high, low),
        (high, 1 - low),
        (1 - high, low),
        (1 - high, 1 - low),
    )

    def block_of(u, which, side, quarter):
        at, start, size = units[u]
        from_high, from_low = origins[which]
        return outs[at].at[from_high, from_low, side, quarter, :, pl.ds(start, size)]

    def held(p, which, side):
        from_high, from_low = origins[which]
        return pair_ref.at[p, from_high, from_low, side]

    if pairs:
        sends_k, recvs_k, sends_s, recvs_s = refs[at + 7 :]
        for p in range(pairs):
            pair_ref[p, high, low, core] = rows_ref[:, 2 * PAIR * p : 2 * PAIR * (p + 1)]
            own = held(p, 0, core)
            send(own, own, sends_k, recvs_k, 3 * p + 1, far)
            send(own, own, sends_k, recvs_k, 3 * p, near)
            send(own, own, sends_s, recvs_s, 4 * p, sibling)
    for u, (at, start, size) in enumerate(units):
        block = ins[at].at[rep, :, pl.ds(start, size)]
        send(block, block_of(u, 0, core, rep), sends_z, recvs_z, 3 * u + 1, far)
        send(block, block_of(u, 0, core, rep), sends_z, recvs_z, 3 * u, near)
    for u, (at, start, size) in enumerate(units):
        whole = ins[at].at[:, :, pl.ds(start, size)]
        send(whole, block_of(u, 0, core, slice(None)), sends_c, recvs_c, 4 * u, sibling)
    for at in range(count):
        copy = pltpu.make_async_copy(ins[at], outs[at].at[high, low, core], local.at[at])
        copy.start()
        copies.append(copy)

    def spread(u, which):
        block = block_of(u, which, core, rep)
        arrived(block, sends_z, recvs_z, 3 * u + which - 1)
        if which == 2:
            send(block, block, sends_z, recvs_z, 3 * u + 2, near)
        for j in range(1, reps):
            index = (3 * u + which - 1) * (reps - 1) + j - 1
            peer = ((rep + j) % reps, me[1])
            send(block, block, sends_r, recvs_r, index, peer)

    def pass_on(u, which):
        for j in range(1, reps):
            index = (3 * u + which - 1) * (reps - 1) + j - 1
            block = block_of(u, which, core, (rep + reps - j) % reps)
            arrived(block, sends_r, recvs_r, index)
        whole = block_of(u, which, core, slice(None))
        send(whole, whole, sends_c, recvs_c, 4 * u + which, sibling)

    total = len(units)

    def advance(step):
        if step < total:
            spread(step, 1)
            spread(step, 2)
        if 1 <= step < total + 1:
            spread(step - 1, 3)
        if 2 <= step:
            for which in range(1, 4):
                pass_on(step - 2, which)

    def take(p, which):
        block = held(p, which, core)
        arrived(block, sends_k, recvs_k, 3 * p + which - 1)
        if which == 2:
            send(block, block, sends_k, recvs_k, 3 * p + 2, near)
        send(block, block, sends_s, recvs_s, 4 * p + which, sibling)

    def compute(p):
        for which in range(4):
            arrived(held(p, which, 1 - core), sends_s, recvs_s, 4 * p + which)
        cols = pl.ds(pl.multiple_of(p * PAIR, PAIR), PAIR)
        shape = (-1, PAIR)
        context_ref[:, cols] = pair_context(
            query_ref[:, cols],
            pair_ref[p, :, :, :, :, :PAIR].reshape(shape),
            pair_ref[p, :, :, :, :, PAIR:].reshape(shape),
        )

    steps = total + 2
    if not pairs:
        for step in range(steps):
            advance(step)
    else:

        def step_all(t, carry):
            @pl.when(t < pairs)
            def _():
                take(t, 1)
                take(t, 2)

            @pl.when((t >= 1) & (t < pairs + 1))
            def _():
                take(t - 1, 3)

            for i in range(steps):

                @pl.when(t == i)
                def _(i=i):
                    advance(i)

            @pl.when((t >= 2) & (t < pairs + 2))
            def _():
                compute(t - 2)

            return carry

        lax.fori_loop(0, max(pairs + 2, steps), step_all, 0)
    for u in range(total):
        for which in range(4):
            block = block_of(u, which, 1 - core, slice(None))
            arrived(block, sends_c, recvs_c, 4 * u + which)
    for u, (at, start, size) in enumerate(units):
        cols = pl.ds(start, size)
        left(ins[at].at[rep, :, cols], sends_z, recvs_z, 3 * u)
        left(ins[at].at[rep, :, cols], sends_z, recvs_z, 3 * u + 1)
        left(block_of(u, 2, core, rep), sends_z, recvs_z, 3 * u + 2)
        left(ins[at].at[:, :, cols], sends_c, recvs_c, 4 * u)
        for which in range(1, 4):
            left(block_of(u, which, core, slice(None)), sends_c, recvs_c, 4 * u + which)
            for j in range(1, reps):
                index = (3 * u + which - 1) * (reps - 1) + j - 1
                left(block_of(u, which, core, rep), sends_r, recvs_r, index)
    for p in range(pairs):
        for at, which in enumerate((0, 0, 2)):
            left(held(p, which, core), sends_k, recvs_k, 3 * p + at)
        for which in range(4):
            left(held(p, which, core), sends_s, recvs_s, 4 * p + which)
    for copy in copies:
        copy.wait()


def cut(width, pieces):
    size = width // pieces
    if size % 128:
        return [(0, width)]
    return [(size * i, size) for i in range(pieces)]


def gather_many(shards, pieces, identity, query=None, rows=None):
    reps = lax.axis_size("rep")
    count = len(shards)
    units = [
        (at, low, size)
        for at, shard in enumerate(shards)
        for low, size in cut(shard.shape[2], pieces[at])
    ]
    total = len(units)
    hops = 3 * total * (reps - 1)
    dma = pltpu.SemaphoreType.DMA
    vmem = pl.BlockSpec(memory_space=pltpu.VMEM)
    out_shape = [
        jax.ShapeDtypeStruct((2, 2, 2) + shard.shape, shard.dtype) for shard in shards
    ]
    operands = list(shards)
    spaces = []
    more = []
    pairs = 0
    if query is not None:
        pairs = query.shape[1] // PAIR
        operands += [query, rows]
        spaces = [vmem] * 2
        out_shape += [
            jax.ShapeDtypeStruct(query.shape, BF16),
            jax.ShapeDtypeStruct((pairs, 2, 2, 2, rows.shape[0], 2 * PAIR), BF16),
        ]
        more = [dma((3 * pairs,))] * 2 + [dma((4 * pairs,))] * 2
    return pl.pallas_call(
        functools.partial(gather_kernel, units, count, reps, pairs),
        out_shape=out_shape,
        in_specs=[pl.BlockSpec(memory_space=pl.ANY)] * count + spaces,
        out_specs=[pl.BlockSpec(memory_space=pl.ANY)] * count + spaces,
        scratch_shapes=[dma((3 * total,))] * 2
        + [dma((hops,))] * 2
        + [dma((4 * total,))] * 2
        + [dma((count,))]
        + more,
        compiler_params=pltpu.CompilerParams(
            collective_id=identity, has_side_effects=True, vmem_limit_bytes=60 * 1024 * 1024
        ),
    )(*operands)


def summed(parts, kind):
    total = parts[0].astype(F32)
    for part in parts[1:]:
        total = total + part.astype(F32)
    return total.astype(kind)


def reduce_kernel(units, count, reps, fused, *refs):
    ins = refs[:count]
    at = count
    if fused:
        query_ref, grad_ref, pair_ref = refs[at : at + 3]
        at += 3
    outs = refs[at : at + count]
    at += count
    if fused:
        grad_query_ref, grad_pair_ref = refs[at : at + 2]
        at += 2
    size = len(units)
    first, second, third, fourth, own = [
        refs[at + i * size : at + (i + 1) * size] for i in range(5)
    ]
    sems = refs[at + 5 * size :]
    sends_c, recvs_c, sends_r, recvs_r, sends_z, recvs_z, sends_g, recvs_g = sems[:8]
    rep, high, low, core = places()
    me = (rep, place_of(high, low, core))
    sibling = (rep, place_of(high, low, 1 - core))
    far = (rep, place_of(1 - high, low, core))
    near = (rep, place_of(high, 1 - low, core))
    enter(reps)
    def send(src, dst, sends, recvs, at, peer):
        remote(src, dst, sends, recvs, at, peer).start()

    def left(block, sends, recvs, at):
        remote(block, block, sends, recvs, at, me).wait_send()

    def arrived(block, sends, recvs, at):
        remote(block, block, sends, recvs, at, me).wait_recv()

    for u, (a, start, width) in enumerate(units):
        block = ins[a].at[:, :, 1 - core, :, :, pl.ds(start, width)]
        send(block, first[u], sends_c, recvs_c, u, sibling)

    def over_core(u):
        a, start, width = units[u]
        arrived(first[u], sends_c, recvs_c, u)

        def step(i, carry):
            h, w, q = i // (2 * reps), (i // reps) % 2, i % reps
            mine = ins[a][h, w, core, q, :, start : start + width]
            first[u][h, w, q] = summed([first[u][h, w, q], mine], first[u].dtype)
            return carry

        lax.fori_loop(0, 4 * reps, step, 0)
        for k in range(1, reps):
            target = (rep + k) % reps
            send(
                first[u].at[:, :, target],
                second[u].at[k - 1],
                sends_r,
                recvs_r,
                u * (reps - 1) + k - 1,
                (target, me[1]),
            )

    def over_rep(u):
        for k in range(1, reps):
            arrived(second[u].at[k - 1], sends_r, recvs_r, u * (reps - 1) + k - 1)

        def step(i, carry):
            h, w = i // 2, i % 2
            parts = [first[u][h, w, rep]] + [second[u][k, h, w] for k in range(reps - 1)]
            own[u][h, w] = summed(parts, own[u].dtype)
            return carry

        lax.fori_loop(0, 4, step, 0)
        send(own[u].at[:, 1 - low], third[u], sends_z, recvs_z, 2 * u, near)

    def over_near(u):
        arrived(third[u], sends_z, recvs_z, 2 * u)
        for h in range(2):
            own[u][h, low] = summed([own[u][h, low], third[u][h]], own[u].dtype)
        send(own[u].at[1 - high, low], fourth[u], sends_z, recvs_z, 2 * u + 1, far)

    def over_far(u):
        a, start, width = units[u]
        arrived(fourth[u], sends_z, recvs_z, 2 * u + 1)
        outs[a][rep, :, start : start + width] = summed(
            [own[u][high, low], fourth[u][...]], outs[a].dtype
        )
        block = outs[a].at[rep, :, pl.ds(start, width)]
        for k in range(1, reps):
            peer = ((rep + k) % reps, me[1])
            send(block, block, sends_g, recvs_g, u * (reps - 1) + k - 1, peer)

    stages = (over_core, over_rep, over_near, over_far)

    def advance(step):
        for lag, stage in enumerate(stages):
            if 0 <= step - lag < size:
                stage(step - lag)

    steps = size + len(stages) - 1
    if not fused:
        for step in range(steps):
            advance(step)
    else:
        terms, merged, from_near, from_far, held, sends_k, recvs_k, fetched = sems[8:]
        pairs = terms.shape[0]

        def fetch(p):
            return pltpu.make_async_copy(pair_ref.at[p], held.at[p % 2], fetched.at[p % 2])

        def hop(p, which):
            if which == 0:
                return remote(
                    terms.at[p, :, :, 1 - core], merged.at[p], sends_k, recvs_k, 3 * p, sibling
                )
            if which == 1:
                return remote(
                    merged.at[p, :, 1 - low], from_near.at[p], sends_k, recvs_k, 3 * p + 1, near
                )
            return remote(
                merged.at[p, 1 - high, low], from_far.at[p], sends_k, recvs_k, 3 * p + 2, far
            )

        def merge_core(p):
            arrived(merged.at[p], sends_k, recvs_k, 3 * p)
            for h in range(2):
                for w in range(2):
                    both = [merged[p, h, w], terms[p, h, w, core]]
                    merged[p, h, w] = summed(both, BF16)
            hop(p, 1).start()

        def merge_near(p):
            arrived(from_near.at[p], sends_k, recvs_k, 3 * p + 1)
            for h in range(2):
                merged[p, h, low] = summed([merged[p, h, low], from_near[p, h]], BF16)
            hop(p, 2).start()

        def merge_far(p):
            arrived(from_far.at[p], sends_k, recvs_k, 3 * p + 2)
            cols = pl.ds(pl.multiple_of(p * 2 * PAIR, 2 * PAIR), 2 * PAIR)
            grad_pair_ref[:, cols] = summed([merged[p, high, low], from_far[p]], BF16)

        def compute(p):
            fetch(p).wait()

            @pl.when(p < pairs - 1)
            def _():
                fetch(p + 1).start()

            cols = pl.ds(pl.multiple_of(p * PAIR, PAIR), PAIR)
            slot = p % 2
            query_part, key_part, value_part = pair_grads(
                query_ref[:, cols], grad_ref[:, cols], held[slot, :, :PAIR], held[slot, :, PAIR:]
            )
            grad_query_ref[:, cols] = query_part
            shape = terms.shape[1:5] + (PAIR,)
            terms[p, :, :, :, :, :PAIR] = key_part.reshape(shape)
            terms[p, :, :, :, :, PAIR:] = value_part.reshape(shape)
            hop(p, 0).start()

        fetch(0).start()

        def step_all(t, carry):
            for lag, merge in ((1, merge_core), (2, merge_near), (3, merge_far)):

                @pl.when((t >= lag) & (t < pairs + lag))
                def _(lag=lag, merge=merge):
                    merge(t - lag)

            @pl.when(t < pairs)
            def _():
                compute(t)

            for i in range(steps):

                @pl.when(t == i)
                def _(i=i):
                    advance(i)

            return carry

        lax.fori_loop(0, max(pairs + 3, steps), step_all, 0)
        for p in range(pairs):
            for which in range(3):
                hop(p, which).wait_send()
    for u, (a, start, width) in enumerate(units):
        for k in range(1, reps):
            block = outs[a].at[(rep + reps - k) % reps, :, pl.ds(start, width)]
            arrived(block, sends_g, recvs_g, u * (reps - 1) + k - 1)
    for u, (a, start, width) in enumerate(units):
        cols = pl.ds(start, width)
        left(ins[a].at[:, :, 1 - core, :, :, cols], sends_c, recvs_c, u)
        left(own[u].at[:, 1 - low], sends_z, recvs_z, 2 * u)
        left(own[u].at[1 - high, low], sends_z, recvs_z, 2 * u + 1)
        for k in range(1, reps):
            index = u * (reps - 1) + k - 1
            left(first[u].at[:, :, (rep + k) % reps], sends_r, recvs_r, index)
            left(outs[a].at[rep, :, cols], sends_g, recvs_g, index)


def split_rows(part):
    reps = lax.axis_size("rep")
    rows, width = part.shape
    return part.reshape(2, 2, 2, reps, rows // (8 * reps), width)


def reduce_many(blocks, pieces, identity, query=None, grad=None, pairs=None):
    reps = lax.axis_size("rep")
    count = len(blocks)
    units = [
        (at, low, size)
        for at, block in enumerate(blocks)
        for low, size in cut(block.shape[5], pieces[at])
    ]
    dma = pltpu.SemaphoreType.DMA
    vmem = pl.BlockSpec(memory_space=pltpu.VMEM)

    def buffers(*lead):
        return [
            pltpu.VMEM(lead + (blocks[at].shape[4], size), blocks[at].dtype)
            for at, _, size in units
        ]

    total = len(units)
    out_shape = [
        jax.ShapeDtypeStruct((reps,) + block.shape[4:], block.dtype) for block in blocks
    ]
    operands = list(blocks)
    in_specs = [vmem] * count
    more = []
    if pairs is not None:
        tokens, width = query.shape
        number = width // PAIR
        block = (tokens, 2 * PAIR)
        operands += [query, grad, pairs]
        in_specs += [vmem] * 2 + [pl.BlockSpec(memory_space=pl.ANY)]
        out_shape += [
            jax.ShapeDtypeStruct((tokens, width), BF16),
            jax.ShapeDtypeStruct((tokens, 2 * width), BF16),
        ]
        more = [
            pltpu.VMEM((number, 2, 2, 2) + block, BF16),
            pltpu.VMEM((number, 2, 2) + block, BF16),
            pltpu.VMEM((number, 2) + block, BF16),
            pltpu.VMEM((number,) + block, BF16),
            pltpu.VMEM((2,) + pairs.shape[1:], BF16),
            dma((3 * number,)),
            dma((3 * number,)),
            dma((2,)),
        ]
    sums = pl.pallas_call(
        functools.partial(reduce_kernel, units, count, reps, pairs is not None),
        out_shape=out_shape,
        in_specs=in_specs,
        out_specs=[vmem] * len(out_shape),
        scratch_shapes=buffers(2, 2, reps)
        + buffers(reps - 1, 2, 2)
        + buffers(2)
        + buffers()
        + buffers(2, 2)
        + [dma((total,))] * 2
        + [dma((total * (reps - 1),))] * 2
        + [dma((total * 2,))] * 2
        + [dma((total * (reps - 1),))] * 2
        + more,
        compiler_params=pltpu.CompilerParams(
            collective_id=identity, has_side_effects=True, vmem_limit_bytes=60 * 1024 * 1024
        ),
    )(*operands)
    totals = [total.reshape(-1, total.shape[2]).astype(F32) for total in sums[:count]]
    return totals + list(sums[count:])


def blocked(shard):
    return shard.reshape(lax.axis_size("rep"), -1, shard.shape[1])


def divides(rows):
    reps = lax.axis_size("rep")
    return lax.axis_size("cp") == 8 and reps == 4 and rows % (8 * reps) == 0


def on_device(
    tokens,
    query_weight,
    query_bias,
    key_weight,
    value_weight,
    value_bias,
    output_weight,
    output_bias,
    first_gain,
    first_shift,
    up_weight,
    up_bias,
    down_weight,
    down_bias,
    second_gain,
    second_shift,
    cotangent,
):
    row_count = tokens.shape[1]
    width = tokens.shape[2]
    local_tokens = tokens[0]
    fast = divides(query_weight.shape[0])
    reps = lax.axis_size("rep")
    proj_shard = jnp.concatenate([query_weight, mixed(key_weight, value_weight)], axis=1)
    small = (
        query_bias,
        value_bias,
        output_bias,
        first_gain,
        first_shift,
        up_bias,
        down_bias,
        second_gain,
        second_shift,
    )
    if fast:
        rows = []
        for vector in small:
            lines = -(-vector.shape[0] // 128)
            rows.append(
                jnp.pad(vector.astype(F32), (0, 128 * lines - vector.shape[0])).reshape(lines, 128)
            )
        packed = jnp.concatenate(rows, axis=0)
        packed = jnp.pad(packed, ((0, -packed.shape[0] % (8 * reps)), (0, 0))).astype(BF16)
        w_proj, gathered = gather_many(
            (blocked(proj_shard), blocked(packed)), (3, 1), 1
        )
        w_proj = w_proj.reshape(-1, proj_shard.shape[1])
        gathered = gathered.reshape(-1, packed.shape[0], 128)
    else:
        w_proj = gather_all(proj_shard)
        gathered = lax.all_gather(jnp.concatenate(small)[None], "cp", axis=0, tiled=True)
    vectors = []
    at = 0
    for vector in small:
        size = vector.shape[0]
        if fast:
            lines = -(-size // 128)
            part = gathered[:, at : at + lines].reshape(-1, 128 * lines)[:, :size]
            at += lines
        else:
            part = gathered[:, at : at + size]
            at += size
        vectors.append(part.reshape(-1).astype(F32))
    b_query, b_value, b_output, gain_one, shift_one, b_up, b_down, gain_two, shift_two = vectors
    w_pair = w_proj[:, width:]
    pair_bias = mixed(jnp.zeros_like(b_value)[None], b_value[None])
    pair_rows = (matmul(local_tokens, w_pair) + pair_bias).astype(BF16)
    chunk = width // CHUNKS
    query_rows = (matmul(local_tokens, w_proj[:, :width]) + b_query).astype(BF16)
    query_scaled = query_rows * jnp.asarray(1.0 / math.sqrt(HD), BF16)
    wide_shard = jnp.concatenate([output_weight, up_weight], axis=1)
    if fast:
        w_wide, w_down, context_low, pairs = gather_many(
            (blocked(wide_shard), blocked(down_weight)), (2, 2), 2, query_scaled, pair_rows
        )
        w_wide = w_wide.reshape(-1, wide_shard.shape[1])
        w_down = w_down.reshape(-1, width)
        pairs = pairs.reshape(pairs.shape[0], -1, 2 * PAIR)
    else:
        w_wide = gather_all(wide_shard)
        w_down = gather_all(down_weight)
        queries = [query_scaled[:, chunk * i : chunk * (i + 1)] for i in range(CHUNKS)]
        pairs = [
            lax.all_gather(
                pair_rows[:, 2 * chunk * i : 2 * chunk * (i + 1)], "cp", axis=0, tiled=True
            )
            for i in range(CHUNKS)
        ]
        context_low = jnp.concatenate(
            [attend(query, pair) for query, pair in zip(queries, pairs)], axis=1
        )
    w_output = w_wide[:, :width]
    w_up = w_wide[:, width:]
    attn_out = matmul(context_low, w_output) + b_output
    resid_first = local_tokens.astype(F32) + attn_out
    first_norm, pull_first = jax.vjp(normalize, resid_first, gain_one, shift_one)
    first_low = first_norm.astype(BF16)
    inner_act = matmul(first_low, w_up) + b_up
    hidden, pull_gelu = jax.vjp(gelu_exact, inner_act)
    hidden_low = hidden.astype(BF16)
    resid_second = first_norm + (matmul(hidden_low, w_down) + b_down)
    layer_out, pull_second = jax.vjp(normalize, resid_second, gain_two, shift_two)

    grad_resid2, grad_gain2, grad_shift2 = pull_second(cotangent[0])
    grad_outer = grad_resid2.astype(BF16)
    grad_down_bias = column_sum(grad_outer)
    part_down = over_rows(hidden_low, grad_outer).astype(BF16)
    grad_inner = pull_gelu(against(grad_outer, w_down))[0].astype(BF16)
    grad_up_bias = column_sum(grad_inner)
    part_up = over_rows(first_low, grad_inner).astype(BF16)
    grad_first = grad_resid2 + against(grad_inner, w_up)
    grad_resid1, grad_gain1, grad_shift1 = pull_first(grad_first)
    grad_attn = grad_resid1.astype(BF16)
    grad_output_bias = column_sum(grad_attn)
    part_output = over_rows(context_low, grad_attn).astype(BF16)
    grad_context = against(grad_attn, w_output).astype(BF16)

    if fast:
        full_down, full_up, full_output, grad_query_low, grad_pair_low = reduce_many(
            [split_rows(part) for part in (part_down, part_up, part_output)],
            (2, 2, 1),
            3,
            query_scaled,
            grad_context,
            pairs,
        )
    else:
        grad_queries = []
        grad_pairs = []
        for i in range(CHUNKS):
            grad_query, grad_terms = attend_back(
                queries[i], grad_context[:, chunk * i : chunk * (i + 1)], pairs[i]
            )
            grad_queries.append(grad_query)
            grad_pairs.append(
                lax.psum_scatter(grad_terms, "cp", scatter_dimension=0, tiled=True)
            )
        grad_query_low = jnp.concatenate(grad_queries, axis=1)
        grad_pair_low = jnp.concatenate(grad_pairs, axis=1)
    grad_proj = jnp.concatenate([grad_query_low, grad_pair_low], axis=1)
    part_proj = over_rows(local_tokens, grad_proj).astype(BF16)
    grad_tokens = grad_resid1 + against(grad_proj, w_proj)
    proj_sums = column_sum(grad_proj)
    _, grad_value_bias = unmixed(proj_sums[None, width:])

    small_grads = (
        proj_sums[:width],
        grad_value_bias[0],
        grad_output_bias,
        grad_gain1,
        grad_shift1,
        grad_up_bias,
        grad_down_bias,
        grad_gain2,
        grad_shift2,
    )
    owners = lax.axis_size("cp")
    total_sq = jnp.broadcast_to(jnp.sum(grad_tokens * grad_tokens), (owners, 1))
    flat = jnp.concatenate(
        [vector.reshape(owners, -1) for vector in small_grads] + [total_sq], axis=1
    )
    if fast:
        flat = jnp.pad(flat, ((0, 0), (0, -flat.shape[1] % (8 * 128 * reps))))
        full_proj, sums = reduce_many(
            (split_rows(part_proj), flat.reshape(2, 2, 2, reps, -1, 128)), (3, 1), 4
        )
        sums = sums.reshape(-1)
    else:
        shards = [
            scatter_all(part)
            for part in (part_down, part_up, part_output, part_proj)
        ]
        full_down, full_up, full_output, full_proj = [
            part.astype(F32) for part in lax.psum(tuple(shards), "rep")
        ]
        sums = lax.psum(flat, ("rep", "cp"))
        sums = lax.dynamic_slice_in_dim(sums, lax.axis_index("cp"), 1, 0)[0]
    reduced = []
    at = 0
    for shard in small:
        reduced.append(sums[at : at + shard.shape[0]])
        at += shard.shape[0]
    entries = lax.axis_size("rep") * owners * row_count * width
    rms_values = jnp.sqrt(sums[at : at + 1] / entries)

    grad_key_weight, grad_value_weight = unmixed(full_proj[:, width:])
    return (
        layer_out[None],
        grad_tokens[None],
        full_proj[:, :width],
        reduced[0],
        grad_key_weight,
        grad_value_weight,
        reduced[1],
        full_output,
        reduced[2],
        reduced[3],
        reduced[4],
        full_up,
        reduced[5],
        full_down,
        reduced[6],
        reduced[7],
        reduced[8],
        rms_values,
    )


def solution(mesh):
    rows = P("cp", None)
    vector = P("cp")
    whole = P("rep", "cp", None)
    params = (
        rows,
        vector,
        rows,
        rows,
        vector,
        rows,
        vector,
        vector,
        vector,
        rows,
        vector,
        rows,
        vector,
        vector,
        vector,
    )
    return jax.shard_map(
        on_device,
        mesh=mesh,
        in_specs=(whole,) + params + (whole,),
        out_specs=(whole, whole) + params + (P(),),
        check_vma=False,
    )
```

```python
import functools
import math

import jax
import jax.numpy as jnp
from jax import lax
from jax.experimental import pallas as pl
from jax.experimental.pallas import tpu as pltpu
from jax.sharding import PartitionSpec as P

HD = 64
PAIR = 2 * HD
CHUNKS = 3
AHEAD = 2
EPSILON = 1e-12
BF16 = jnp.bfloat16
F32 = jnp.float32
MESH = pl.DeviceIdType.MESH


def normalize(values, norm_gain, norm_shift):
    center = values - jnp.mean(values, axis=-1, keepdims=True)
    spread = jnp.mean(center * center, axis=-1, keepdims=True)
    return center * lax.rsqrt(spread + EPSILON) * norm_gain + norm_shift


def gelu_exact(values):
    return 0.5 * values * (1.0 + lax.erf(values * (1.0 / math.sqrt(2.0))))


def matmul(left, right):
    return jnp.dot(left, right, preferred_element_type=F32)


def over_rows(left, right):
    return lax.dot_general(left, right, (((0,), (0,)), ((), ())), preferred_element_type=F32)


def against(left, right):
    return lax.dot_general(left, right, (((1,), (1,)), ((), ())), preferred_element_type=F32)


def column_sum(values):
    return jnp.sum(values.astype(F32), axis=0)


def head_mask(shape, head):
    lane = lax.broadcasted_iota(jnp.int32, shape, 1)
    return (lane >= head * HD) & (lane < (head + 1) * HD)


def pair_context(query, keys, values):
    total = None
    for head in range(2):
        mask = head_mask(query.shape, head)
        scores = against(jnp.where(mask, query, jnp.zeros_like(query)), keys)
        top = jnp.max(scores, axis=-1, keepdims=True)
        weight = jnp.exp(scores - top)
        inverse = 1.0 / jnp.sum(weight, axis=-1, keepdims=True)
        part = matmul((weight * inverse).astype(BF16), values)
        total = part if head == 0 else jnp.where(mask, part, total)
    return total.astype(BF16)


def forward_kernel(query_ref, pair_ref, context_ref):
    context_ref[...] = pair_context(query_ref[...], pair_ref[:, :PAIR], pair_ref[:, PAIR:])


def pair_grads(query, grad, keys, values):
    zeros = jnp.zeros_like(query)
    key_part = value_part = query_part = None
    for head in range(2):
        mask = head_mask(query.shape, head)
        own_query = jnp.where(mask, query, zeros)
        own_grad = jnp.where(mask, grad, zeros)
        scores = against(keys, own_query)
        top = jnp.max(scores, axis=0, keepdims=True)
        weight = jnp.exp(scores - top)
        inverse = 1.0 / jnp.sum(weight, axis=0, keepdims=True)
        probs = weight * inverse
        grad_probs = against(values, own_grad)
        delta = jnp.sum(probs * grad_probs, axis=0, keepdims=True)
        grad_scores = (probs * (grad_probs - delta)).astype(BF16)
        new_value = matmul(probs.astype(BF16), own_grad)
        new_key = matmul(grad_scores, own_query)
        new_query = over_rows(keys, grad_scores)
        if head == 0:
            key_part, value_part, query_part = new_key, new_value, new_query
        else:
            key_part = key_part + new_key
            value_part = value_part + new_value
            row = lax.broadcasted_iota(jnp.int32, new_query.shape, 0)
            query_part = jnp.where(row < HD, query_part, new_query)
    query_part = (query_part.T * (1.0 / math.sqrt(HD))).astype(BF16)
    return query_part, key_part.astype(BF16), value_part.astype(BF16)


def backward_kernel(query_ref, grad_ref, pair_ref, grad_query_ref, grad_pair_ref):
    grad_query_ref[...], grad_pair_ref[:, :PAIR], grad_pair_ref[:, PAIR:] = pair_grads(
        query_ref[...], grad_ref[...], pair_ref[:, :PAIR], pair_ref[:, PAIR:]
    )


def column_block(rows, width):
    return pl.BlockSpec((rows, width), lambda i: (0, i))


def attend(query, pairs):
    rows, width = query.shape
    keys = pairs.shape[0]
    return pl.pallas_call(
        forward_kernel,
        grid=(width // PAIR,),
        in_specs=[column_block(rows, PAIR), column_block(keys, 2 * PAIR)],
        out_specs=column_block(rows, PAIR),
        out_shape=jax.ShapeDtypeStruct((rows, width), BF16),
    )(query, pairs)


def attend_back(query, grad, pairs):
    rows, width = query.shape
    keys = pairs.shape[0]
    return pl.pallas_call(
        backward_kernel,
        grid=(width // PAIR,),
        in_specs=[
            column_block(rows, PAIR),
            column_block(rows, PAIR),
            column_block(keys, 2 * PAIR),
        ],
        out_specs=(column_block(rows, PAIR), column_block(keys, 2 * PAIR)),
        out_shape=(
            jax.ShapeDtypeStruct((rows, width), BF16),
            jax.ShapeDtypeStruct((keys, 2 * width), BF16),
        ),
    )(query, grad, pairs)


def mixed(left, right):
    parts = []
    for low in range(0, left.shape[1], PAIR):
        parts += [left[:, low : low + PAIR], right[:, low : low + PAIR]]
    return jnp.concatenate(parts, axis=1)


def unmixed(both):
    starts = range(0, both.shape[1], 2 * PAIR)
    return (
        jnp.concatenate([both[:, low : low + PAIR] for low in starts], axis=1),
        jnp.concatenate([both[:, low + PAIR : low + 2 * PAIR] for low in starts], axis=1),
    )


def gather_all(shard):
    return lax.all_gather(shard, "cp", axis=0, tiled=True)


def scatter_all(values):
    return lax.psum_scatter(values.astype(BF16), "cp", scatter_dimension=0, tiled=True)


def places():
    rep = lax.axis_index("rep")
    cp = lax.axis_index("cp")
    return rep, cp // 4, (cp // 2) % 2, cp % 2


def place_of(high, low, core):
    return 4 * high + 2 * low + core


def enter(reps):
    rep, high, low, core = places()
    barrier = pltpu.get_barrier_semaphore()
    peers = [
        (rep, place_of(high, low, 1 - core)),
        (rep, place_of(high, 1 - low, core)),
        (rep, place_of(1 - high, low, core)),
    ]
    peers += [((rep + k) % reps, place_of(high, low, core)) for k in range(1, reps)]
    for peer in peers:
        pl.semaphore_signal(barrier, inc=1, device_id=peer, device_id_type=MESH)
    pl.semaphore_wait(barrier, len(peers))


def remote(src, dst, sends, recvs, at, peer):
    return pltpu.make_async_remote_copy(
        src_ref=src,
        dst_ref=dst,
        send_sem=sends.at[at],
        recv_sem=recvs.at[at],
        device_id=peer,
        device_id_type=MESH,
    )


def gather_kernel(units, count, reps, pairs, *refs):
    ins = refs[:count]
    at = count
    if pairs:
        query_ref, key_ref, value_ref = refs[at : at + 3]
        at += 3
    outs = refs[at : at + count]
    at += count
    if pairs:
        context_ref, pair_ref = refs[at : at + 2]
        at += 2
    sends_z, recvs_z, sends_r, recvs_r, sends_c, recvs_c, local = refs[at : at + 7]
    rep, high, low, core = places()
    me = (rep, place_of(high, low, core))
    sibling = (rep, place_of(high, low, 1 - core))
    far = (rep, place_of(1 - high, low, core))
    near = (rep, place_of(high, 1 - low, core))
    enter(reps)
    copies = []

    def send(src, dst, sends, recvs, at, peer):
        remote(src, dst, sends, recvs, at, peer).start()

    def left(block, sends, recvs, at):
        remote(block, block, sends, recvs, at, me).wait_send()

    def arrived(block, sends, recvs, at):
        remote(block, block, sends, recvs, at, me).wait_recv()

    origins = (
        (high, low),
        (high, 1 - low),
        (1 - high, low),
        (1 - high, 1 - low),
    )

    def block_of(u, which, side, quarter):
        at, start, size = units[u]
        from_high, from_low = origins[which]
        return outs[at].at[from_high, from_low, side, quarter, :, pl.ds(start, size)]

    def held(p, which, side):
        from_high, from_low = origins[which]
        return pair_ref.at[p, from_high, from_low, side]

    if pairs:
        sends_k, recvs_k, sends_s, recvs_s = refs[at + 7 :]

    def offer(p):
        own = held(p, 0, core)
        send(own, own, sends_k, recvs_k, 3 * p + 1, far)
        send(own, own, sends_k, recvs_k, 3 * p, near)
        send(own, own, sends_s, recvs_s, 4 * p, sibling)

    for u, (at, start, size) in enumerate(units):
        block = ins[at].at[rep, :, pl.ds(start, size)]
        send(block, block_of(u, 0, core, rep), sends_z, recvs_z, 3 * u + 1, far)
        send(block, block_of(u, 0, core, rep), sends_z, recvs_z, 3 * u, near)
    for u, (at, start, size) in enumerate(units):
        whole = ins[at].at[:, :, pl.ds(start, size)]
        send(whole, block_of(u, 0, core, slice(None)), sends_c, recvs_c, 4 * u, sibling)
    for at in range(count):
        copy = pltpu.make_async_copy(ins[at], outs[at].at[high, low, core], local.at[at])
        copy.start()
        copies.append(copy)

    for p in range(pairs):
        cols = pl.ds(PAIR * p, PAIR)
        pair_ref[p, high, low, core, :, :PAIR] = key_ref[:, cols]
        pair_ref[p, high, low, core, :, PAIR:] = value_ref[:, cols]
        if p < AHEAD:
            offer(p)

    def spread(u, which):
        block = block_of(u, which, core, rep)
        arrived(block, sends_z, recvs_z, 3 * u + which - 1)
        if which == 2:
            send(block, block, sends_z, recvs_z, 3 * u + 2, near)
        for j in range(1, reps):
            index = (3 * u + which - 1) * (reps - 1) + j - 1
            peer = ((rep + j) % reps, me[1])
            send(block, block, sends_r, recvs_r, index, peer)

    def pass_on(u, which):
        for j in range(1, reps):
            index = (3 * u + which - 1) * (reps - 1) + j - 1
            block = block_of(u, which, core, (rep + reps - j) % reps)
            arrived(block, sends_r, recvs_r, index)
        whole = block_of(u, which, core, slice(None))
        send(whole, whole, sends_c, recvs_c, 4 * u + which, sibling)

    total = len(units)

    def advance(step):
        if step < total:
            spread(step, 1)
            spread(step, 2)
        if 1 <= step < total + 1:
            spread(step - 1, 3)
        if 2 <= step:
            for which in range(1, 4):
                pass_on(step - 2, which)

    def take(p, which):
        block = held(p, which, core)
        arrived(block, sends_k, recvs_k, 3 * p + which - 1)
        if which == 2:
            send(block, block, sends_k, recvs_k, 3 * p + 2, near)
        send(block, block, sends_s, recvs_s, 4 * p + which, sibling)

    def compute(p):
        for which in range(4):
            arrived(held(p, which, 1 - core), sends_s, recvs_s, 4 * p + which)
        cols = pl.ds(pl.multiple_of(p * PAIR, PAIR), PAIR)
        shape = (-1, PAIR)
        context_ref[:, cols] = pair_context(
            query_ref[:, cols],
            pair_ref[p, :, :, :, :, :PAIR].reshape(shape),
            pair_ref[p, :, :, :, :, PAIR:].reshape(shape),
        )

    steps = total + 2
    if not pairs:
        for step in range(steps):
            advance(step)
    else:

        def step_all(t, carry):
            @pl.when(t < pairs)
            def _():
                take(t, 1)
                take(t, 2)

            @pl.when(t < pairs - AHEAD)
            def _():
                offer(t + AHEAD)

            @pl.when((t >= 1) & (t < pairs + 1))
            def _():
                take(t - 1, 3)

            for i in range(steps):

                @pl.when(t == i)
                def _(i=i):
                    advance(i)

            @pl.when((t >= 2) & (t < pairs + 2))
            def _():
                compute(t - 2)

            return carry

        lax.fori_loop(0, max(pairs + 2, steps), step_all, 0)
    for u in range(total):
        for which in range(4):
            block = block_of(u, which, 1 - core, slice(None))
            arrived(block, sends_c, recvs_c, 4 * u + which)
    for u, (at, start, size) in enumerate(units):
        cols = pl.ds(start, size)
        left(ins[at].at[rep, :, cols], sends_z, recvs_z, 3 * u)
        left(ins[at].at[rep, :, cols], sends_z, recvs_z, 3 * u + 1)
        left(block_of(u, 2, core, rep), sends_z, recvs_z, 3 * u + 2)
        left(ins[at].at[:, :, cols], sends_c, recvs_c, 4 * u)
        for which in range(1, 4):
            left(block_of(u, which, core, slice(None)), sends_c, recvs_c, 4 * u + which)
            for j in range(1, reps):
                index = (3 * u + which - 1) * (reps - 1) + j - 1
                left(block_of(u, which, core, rep), sends_r, recvs_r, index)
    for p in range(pairs):
        for at, which in enumerate((0, 0, 2)):
            left(held(p, which, core), sends_k, recvs_k, 3 * p + at)
        for which in range(4):
            left(held(p, which, core), sends_s, recvs_s, 4 * p + which)
    for copy in copies:
        copy.wait()


def cut(width, pieces):
    size = width // pieces
    if size % 128:
        return [(0, width)]
    return [(size * i, size) for i in range(pieces)]


def gather_many(shards, pieces, identity, query=None, keys=None, values=None):
    reps = lax.axis_size("rep")
    count = len(shards)
    units = [
        (at, low, size)
        for at, shard in enumerate(shards)
        for low, size in cut(shard.shape[2], pieces[at])
    ]
    total = len(units)
    hops = 3 * total * (reps - 1)
    dma = pltpu.SemaphoreType.DMA
    vmem = pl.BlockSpec(memory_space=pltpu.VMEM)
    out_shape = [
        jax.ShapeDtypeStruct((2, 2, 2) + shard.shape, shard.dtype) for shard in shards
    ]
    operands = list(shards)
    spaces = []
    more = []
    pairs = 0
    if query is not None:
        pairs = query.shape[1] // PAIR
        operands += [query, keys, values]
        spaces = [vmem] * 3
        out_shape += [
            jax.ShapeDtypeStruct(query.shape, BF16),
            jax.ShapeDtypeStruct((pairs, 2, 2, 2, keys.shape[0], 2 * PAIR), BF16),
        ]
        more = [dma((3 * pairs,))] * 2 + [dma((4 * pairs,))] * 2
    return pl.pallas_call(
        functools.partial(gather_kernel, units, count, reps, pairs),
        out_shape=out_shape,
        in_specs=[pl.BlockSpec(memory_space=pl.ANY)] * count + spaces,
        out_specs=[pl.BlockSpec(memory_space=pl.ANY)] * count + spaces[:2],
        scratch_shapes=[dma((3 * total,))] * 2
        + [dma((hops,))] * 2
        + [dma((4 * total,))] * 2
        + [dma((count,))]
        + more,
        compiler_params=pltpu.CompilerParams(
            collective_id=identity, has_side_effects=True, vmem_limit_bytes=60 * 1024 * 1024
        ),
    )(*operands)


def summed(parts, kind):
    total = parts[0].astype(F32)
    for part in parts[1:]:
        total = total + part.astype(F32)
    return total.astype(kind)


def reduce_kernel(units, count, reps, fused, *refs):
    ins = refs[:count]
    at = count
    if fused:
        query_ref, grad_ref, pair_ref = refs[at : at + 3]
        at += 3
    outs = refs[at : at + count]
    at += count
    if fused:
        grad_query_ref, grad_key_ref, grad_value_ref = refs[at : at + 3]
        at += 3
    size = len(units)
    first, second, third, fourth, own = [
        refs[at + i * size : at + (i + 1) * size] for i in range(5)
    ]
    sems = refs[at + 5 * size :]
    sends_c, recvs_c, sends_r, recvs_r, sends_z, recvs_z, sends_g, recvs_g = sems[:8]
    rep, high, low, core = places()
    me = (rep, place_of(high, low, core))
    sibling = (rep, place_of(high, low, 1 - core))
    far = (rep, place_of(1 - high, low, core))
    near = (rep, place_of(high, 1 - low, core))
    enter(reps)
    def send(src, dst, sends, recvs, at, peer):
        remote(src, dst, sends, recvs, at, peer).start()

    def left(block, sends, recvs, at):
        remote(block, block, sends, recvs, at, me).wait_send()

    def arrived(block, sends, recvs, at):
        remote(block, block, sends, recvs, at, me).wait_recv()

    for u, (a, start, width) in enumerate(units):
        block = ins[a].at[:, :, 1 - core, :, :, pl.ds(start, width)]
        send(block, first[u], sends_c, recvs_c, u, sibling)

    def over_core(u):
        a, start, width = units[u]
        arrived(first[u], sends_c, recvs_c, u)

        def step(i, carry):
            h, w, q = i // (2 * reps), (i // reps) % 2, i % reps
            mine = ins[a][h, w, core, q, :, start : start + width]
            first[u][h, w, q] = summed([first[u][h, w, q], mine], first[u].dtype)
            return carry

        lax.fori_loop(0, 4 * reps, step, 0)
        for k in range(1, reps):
            target = (rep + k) % reps
            send(
                first[u].at[:, :, target],
                second[u].at[k - 1],
                sends_r,
                recvs_r,
                u * (reps - 1) + k - 1,
                (target, me[1]),
            )

    def over_rep(u):
        for k in range(1, reps):
            arrived(second[u].at[k - 1], sends_r, recvs_r, u * (reps - 1) + k - 1)

        def step(i, carry):
            h, w = i // 2, i % 2
            parts = [first[u][h, w, rep]] + [second[u][k, h, w] for k in range(reps - 1)]
            own[u][h, w] = summed(parts, own[u].dtype)
            return carry

        lax.fori_loop(0, 4, step, 0)
        send(own[u].at[:, 1 - low], third[u], sends_z, recvs_z, 2 * u, near)

    def over_near(u):
        arrived(third[u], sends_z, recvs_z, 2 * u)
        for h in range(2):
            own[u][h, low] = summed([own[u][h, low], third[u][h]], own[u].dtype)
        send(own[u].at[1 - high, low], fourth[u], sends_z, recvs_z, 2 * u + 1, far)

    def over_far(u):
        a, start, width = units[u]
        arrived(fourth[u], sends_z, recvs_z, 2 * u + 1)
        outs[a][rep, :, start : start + width] = summed(
            [own[u][high, low], fourth[u][...]], outs[a].dtype
        )
        block = outs[a].at[rep, :, pl.ds(start, width)]
        for k in range(1, reps):
            peer = ((rep + k) % reps, me[1])
            send(block, block, sends_g, recvs_g, u * (reps - 1) + k - 1, peer)

    stages = (over_core, over_rep, over_near, over_far)

    def advance(step):
        for lag, stage in enumerate(stages):
            if 0 <= step - lag < size:
                stage(step - lag)

    steps = size + len(stages) - 1
    if not fused:
        for stage in stages:
            for u in range(size):
                stage(u)
    else:
        terms, merged, from_near, from_far, held, sends_k, recvs_k, fetched = sems[8:]
        pairs = terms.shape[0]

        def fetch(p):
            return pltpu.make_async_copy(pair_ref.at[p], held.at[p % 2], fetched.at[p % 2])

        def hop(p, which):
            if which == 0:
                return remote(
                    terms.at[p, :, :, 1 - core], merged.at[p], sends_k, recvs_k, 3 * p, sibling
                )
            if which == 1:
                return remote(
                    merged.at[p, :, 1 - low], from_near.at[p], sends_k, recvs_k, 3 * p + 1, near
                )
            return remote(
                merged.at[p, 1 - high, low], from_far.at[p], sends_k, recvs_k, 3 * p + 2, far
            )

        def merge_core(p):
            arrived(merged.at[p], sends_k, recvs_k, 3 * p)
            for h in range(2):
                for w in range(2):
                    both = [merged[p, h, w], terms[p, h, w, core]]
                    merged[p, h, w] = summed(both, BF16)
            hop(p, 1).start()

        def merge_near(p):
            arrived(from_near.at[p], sends_k, recvs_k, 3 * p + 1)
            for h in range(2):
                merged[p, h, low] = summed([merged[p, h, low], from_near[p, h]], BF16)
            hop(p, 2).start()

        def merge_far(p):
            arrived(from_far.at[p], sends_k, recvs_k, 3 * p + 2)
            cols = pl.ds(pl.multiple_of(p * PAIR, PAIR), PAIR)
            both = summed([merged[p, high, low], from_far[p]], BF16)
            grad_key_ref[:, cols] = both[:, :PAIR]
            grad_value_ref[:, cols] = both[:, PAIR:]

        def compute(p):
            fetch(p).wait()

            @pl.when(p < pairs - 1)
            def _():
                fetch(p + 1).start()

            cols = pl.ds(pl.multiple_of(p * PAIR, PAIR), PAIR)
            slot = p % 2
            query_part, key_part, value_part = pair_grads(
                query_ref[:, cols], grad_ref[:, cols], held[slot, :, :PAIR], held[slot, :, PAIR:]
            )
            grad_query_ref[:, cols] = query_part
            shape = terms.shape[1:5] + (PAIR,)
            terms[p, :, :, :, :, :PAIR] = key_part.reshape(shape)
            terms[p, :, :, :, :, PAIR:] = value_part.reshape(shape)
            hop(p, 0).start()

        fetch(0).start()

        def step_all(t, carry):
            for lag, merge in ((1, merge_core), (2, merge_near), (3, merge_far)):

                @pl.when((t >= lag) & (t < pairs + lag))
                def _(lag=lag, merge=merge):
                    merge(t - lag)

            @pl.when(t < pairs)
            def _():
                compute(t)

            for i in range(steps):

                @pl.when(t == i)
                def _(i=i):
                    advance(i)

            return carry

        lax.fori_loop(0, max(pairs + 3, steps), step_all, 0)
        for p in range(pairs):
            for which in range(3):
                hop(p, which).wait_send()
    for u, (a, start, width) in enumerate(units):
        for k in range(1, reps):
            block = outs[a].at[(rep + reps - k) % reps, :, pl.ds(start, width)]
            arrived(block, sends_g, recvs_g, u * (reps - 1) + k - 1)
    for u, (a, start, width) in enumerate(units):
        cols = pl.ds(start, width)
        left(ins[a].at[:, :, 1 - core, :, :, cols], sends_c, recvs_c, u)
        left(own[u].at[:, 1 - low], sends_z, recvs_z, 2 * u)
        left(own[u].at[1 - high, low], sends_z, recvs_z, 2 * u + 1)
        for k in range(1, reps):
            index = u * (reps - 1) + k - 1
            left(first[u].at[:, :, (rep + k) % reps], sends_r, recvs_r, index)
            left(outs[a].at[rep, :, cols], sends_g, recvs_g, index)


def split_rows(part):
    reps = lax.axis_size("rep")
    rows, width = part.shape
    return part.reshape(2, 2, 2, reps, rows // (8 * reps), width)


def reduce_many(blocks, pieces, identity, query=None, grad=None, pairs=None):
    reps = lax.axis_size("rep")
    count = len(blocks)
    units = [
        (at, low, size)
        for at, block in enumerate(blocks)
        for low, size in cut(block.shape[5], pieces[at])
    ]
    dma = pltpu.SemaphoreType.DMA
    vmem = pl.BlockSpec(memory_space=pltpu.VMEM)

    def buffers(*lead):
        return [
            pltpu.VMEM(lead + (blocks[at].shape[4], size), blocks[at].dtype)
            for at, _, size in units
        ]

    total = len(units)
    out_shape = [
        jax.ShapeDtypeStruct((reps,) + block.shape[4:], block.dtype) for block in blocks
    ]
    operands = list(blocks)
    in_specs = [vmem] * count
    more = []
    if pairs is not None:
        tokens, width = query.shape
        number = width // PAIR
        block = (tokens, 2 * PAIR)
        operands += [query, grad, pairs]
        in_specs += [vmem] * 2 + [pl.BlockSpec(memory_space=pl.ANY)]
        out_shape += [jax.ShapeDtypeStruct((tokens, width), BF16)] * 3
        more = [
            pltpu.VMEM((number, 2, 2, 2) + block, BF16),
            pltpu.VMEM((number, 2, 2) + block, BF16),
            pltpu.VMEM((number, 2) + block, BF16),
            pltpu.VMEM((number,) + block, BF16),
            pltpu.VMEM((2,) + pairs.shape[1:], BF16),
            dma((3 * number,)),
            dma((3 * number,)),
            dma((2,)),
        ]
    sums = pl.pallas_call(
        functools.partial(reduce_kernel, units, count, reps, pairs is not None),
        out_shape=out_shape,
        in_specs=in_specs,
        out_specs=[vmem] * len(out_shape),
        scratch_shapes=buffers(2, 2, reps)
        + buffers(reps - 1, 2, 2)
        + buffers(2)
        + buffers()
        + buffers(2, 2)
        + [dma((total,))] * 2
        + [dma((total * (reps - 1),))] * 2
        + [dma((total * 2,))] * 2
        + [dma((total * (reps - 1),))] * 2
        + more,
        compiler_params=pltpu.CompilerParams(
            collective_id=identity, has_side_effects=True, vmem_limit_bytes=60 * 1024 * 1024
        ),
    )(*operands)
    totals = [total.reshape(-1, total.shape[2]).astype(F32) for total in sums[:count]]
    return totals + list(sums[count:])


def blocked(shard):
    return shard.reshape(lax.axis_size("rep"), -1, shard.shape[1])


def divides(rows):
    reps = lax.axis_size("rep")
    return lax.axis_size("cp") == 8 and reps == 4 and rows % (8 * reps) == 0


def on_device(
    tokens,
    query_weight,
    query_bias,
    key_weight,
    value_weight,
    value_bias,
    output_weight,
    output_bias,
    first_gain,
    first_shift,
    up_weight,
    up_bias,
    down_weight,
    down_bias,
    second_gain,
    second_shift,
    cotangent,
):
    row_count = tokens.shape[1]
    width = tokens.shape[2]
    local_tokens = tokens[0]
    fast = divides(query_weight.shape[0])
    reps = lax.axis_size("rep")
    small = (
        query_bias,
        value_bias,
        output_bias,
        first_gain,
        first_shift,
        up_bias,
        down_bias,
        second_gain,
        second_shift,
    )
    if fast:
        rows = []
        for vector in small:
            lines = -(-vector.shape[0] // 128)
            rows.append(
                jnp.pad(vector.astype(F32), (0, 128 * lines - vector.shape[0])).reshape(lines, 128)
            )
        packed = jnp.concatenate(rows, axis=0)
        packed = jnp.pad(packed, ((0, -packed.shape[0] % (8 * reps)), (0, 0))).astype(BF16)
        shards = (key_weight, value_weight, query_weight, packed)
        w_key, w_value, w_query, gathered = gather_many(
            [blocked(shard) for shard in shards], (1, 1, 1, 1), 1
        )
        w_key, w_value, w_query = [w.reshape(-1, width) for w in (w_key, w_value, w_query)]
        gathered = gathered.reshape(-1, packed.shape[0], 128)
    else:
        w_query, w_key, w_value = [
            gather_all(shard) for shard in (query_weight, key_weight, value_weight)
        ]
        gathered = lax.all_gather(jnp.concatenate(small)[None], "cp", axis=0, tiled=True)
    vectors = []
    at = 0
    for vector in small:
        size = vector.shape[0]
        if fast:
            lines = -(-size // 128)
            part = gathered[:, at : at + lines].reshape(-1, 128 * lines)[:, :size]
            at += lines
        else:
            part = gathered[:, at : at + size]
            at += size
        vectors.append(part.reshape(-1).astype(F32))
    b_query, b_value, b_output, gain_one, shift_one, b_up, b_down, gain_two, shift_two = vectors
    key_rows = matmul(local_tokens, w_key).astype(BF16)
    value_rows = (matmul(local_tokens, w_value) + b_value).astype(BF16)
    chunk = width // CHUNKS
    query_rows = (matmul(local_tokens, w_query) + b_query).astype(BF16)
    query_scaled = query_rows * jnp.asarray(1.0 / math.sqrt(HD), BF16)
    if fast:
        shards = (output_weight, up_weight, down_weight)
        w_output, w_up, w_down, context_low, pairs = gather_many(
            [blocked(shard) for shard in shards],
            (1, 2, 2),
            2,
            query_scaled,
            key_rows,
            value_rows,
        )
        w_output, w_down = w_output.reshape(-1, width), w_down.reshape(-1, width)
        w_up = w_up.reshape(-1, up_weight.shape[1])
        pairs = pairs.reshape(pairs.shape[0], -1, 2 * PAIR)
    else:
        w_output, w_up, w_down = [
            gather_all(shard) for shard in (output_weight, up_weight, down_weight)
        ]
        pair_rows = mixed(key_rows, value_rows)
        queries = [query_scaled[:, chunk * i : chunk * (i + 1)] for i in range(CHUNKS)]
        pairs = [
            lax.all_gather(
                pair_rows[:, 2 * chunk * i : 2 * chunk * (i + 1)], "cp", axis=0, tiled=True
            )
            for i in range(CHUNKS)
        ]
        context_low = jnp.concatenate(
            [attend(query, pair) for query, pair in zip(queries, pairs)], axis=1
        )
    attn_out = matmul(context_low, w_output) + b_output
    resid_first = local_tokens.astype(F32) + attn_out
    first_norm, pull_first = jax.vjp(normalize, resid_first, gain_one, shift_one)
    first_low = first_norm.astype(BF16)
    inner_act = matmul(first_low, w_up) + b_up
    hidden, pull_gelu = jax.vjp(gelu_exact, inner_act)
    hidden_low = hidden.astype(BF16)
    resid_second = first_norm + (matmul(hidden_low, w_down) + b_down)
    layer_out, pull_second = jax.vjp(normalize, resid_second, gain_two, shift_two)

    grad_resid2, grad_gain2, grad_shift2 = pull_second(cotangent[0])
    grad_outer = grad_resid2.astype(BF16)
    grad_down_bias = column_sum(grad_outer)
    part_down = over_rows(hidden_low, grad_outer).astype(BF16)
    grad_inner = pull_gelu(against(grad_outer, w_down))[0].astype(BF16)
    grad_up_bias = column_sum(grad_inner)
    part_up = over_rows(first_low, grad_inner).astype(BF16)
    grad_first = grad_resid2 + against(grad_inner, w_up)
    grad_resid1, grad_gain1, grad_shift1 = pull_first(grad_first)
    grad_attn = grad_resid1.astype(BF16)
    grad_output_bias = column_sum(grad_attn)
    part_output = over_rows(context_low, grad_attn).astype(BF16)
    grad_context = against(grad_attn, w_output).astype(BF16)

    if fast:
        (
            full_down,
            full_up,
            full_output,
            grad_query_low,
            grad_key_low,
            grad_value_low,
        ) = reduce_many(
            [split_rows(part) for part in (part_down, part_up, part_output)],
            (2, 2, 1),
            3,
            query_scaled,
            grad_context,
            pairs,
        )
    else:
        grad_queries = []
        grad_pairs = []
        for i in range(CHUNKS):
            grad_query, grad_terms = attend_back(
                queries[i], grad_context[:, chunk * i : chunk * (i + 1)], pairs[i]
            )
            grad_queries.append(grad_query)
            grad_pairs.append(
                lax.psum_scatter(grad_terms, "cp", scatter_dimension=0, tiled=True)
            )
        grad_query_low = jnp.concatenate(grad_queries, axis=1)
        grad_key_low, grad_value_low = unmixed(jnp.concatenate(grad_pairs, axis=1))
    part_query = over_rows(local_tokens, grad_query_low).astype(BF16)
    part_key = over_rows(local_tokens, grad_key_low).astype(BF16)
    part_value = over_rows(local_tokens, grad_value_low).astype(BF16)
    grad_tokens = (
        grad_resid1
        + against(grad_query_low, w_query)
        + against(grad_key_low, w_key)
        + against(grad_value_low, w_value)
    )

    small_grads = (
        column_sum(grad_query_low),
        column_sum(grad_value_low),
        grad_output_bias,
        grad_gain1,
        grad_shift1,
        grad_up_bias,
        grad_down_bias,
        grad_gain2,
        grad_shift2,
    )
    owners = lax.axis_size("cp")
    total_sq = jnp.broadcast_to(jnp.sum(grad_tokens * grad_tokens), (owners, 1))
    flat = jnp.concatenate(
        [vector.reshape(owners, -1) for vector in small_grads] + [total_sq], axis=1
    )
    if fast:
        flat = jnp.pad(flat, ((0, 0), (0, -flat.shape[1] % (8 * 128 * reps))))
        blocks = [split_rows(part) for part in (part_query, part_key, part_value)]
        full_query, full_key, full_value, sums = reduce_many(
            blocks + [flat.reshape(2, 2, 2, reps, -1, 128)], (1, 1, 1, 1), 4
        )
        sums = sums.reshape(-1)
    else:
        parts = (part_down, part_up, part_output, part_query, part_key, part_value)
        shards = [scatter_all(part) for part in parts]
        full_down, full_up, full_output, full_query, full_key, full_value = [
            part.astype(F32) for part in lax.psum(tuple(shards), "rep")
        ]
        sums = lax.psum(flat, ("rep", "cp"))
        sums = lax.dynamic_slice_in_dim(sums, lax.axis_index("cp"), 1, 0)[0]
    reduced = []
    at = 0
    for shard in small:
        reduced.append(sums[at : at + shard.shape[0]])
        at += shard.shape[0]
    entries = lax.axis_size("rep") * owners * row_count * width
    rms_values = jnp.sqrt(sums[at : at + 1] / entries)

    return (
        layer_out[None],
        grad_tokens[None],
        full_query,
        reduced[0],
        full_key,
        full_value,
        reduced[1],
        full_output,
        reduced[2],
        reduced[3],
        reduced[4],
        full_up,
        reduced[5],
        full_down,
        reduced[6],
        reduced[7],
        reduced[8],
        rms_values,
    )


def solution(mesh):
    rows = P("cp", None)
    vector = P("cp")
    whole = P("rep", "cp", None)
    params = (
        rows,
        vector,
        rows,
        rows,
        vector,
        rows,
        vector,
        vector,
        vector,
        rows,
        vector,
        rows,
        vector,
        vector,
        vector,
    )
    return jax.shard_map(
        on_device,
        mesh=mesh,
        in_specs=(whole,) + params + (whole,),
        out_specs=(whole, whole) + params + (P(),),
        check_vma=False,
    )
```

```python
import functools
import math

import jax
import jax.numpy as jnp
from jax import lax
from jax.experimental import pallas as pl
from jax.experimental.pallas import tpu as pltpu
from jax.sharding import PartitionSpec as P

HD = 64
PAIR = 2 * HD
CHUNKS = 3
AHEAD = 2
FULL, DEPTH, REST = range(3)
EPSILON = 1e-12
BF16 = jnp.bfloat16
F32 = jnp.float32
MESH = pl.DeviceIdType.MESH


def normalize(values, norm_gain, norm_shift):
    center = values - jnp.mean(values, axis=-1, keepdims=True)
    spread = jnp.mean(center * center, axis=-1, keepdims=True)
    return center * lax.rsqrt(spread + EPSILON) * norm_gain + norm_shift


def gelu_exact(values):
    return 0.5 * values * (1.0 + lax.erf(values * (1.0 / math.sqrt(2.0))))


def matmul(left, right):
    return jnp.dot(left, right, preferred_element_type=F32)


def over_rows(left, right):
    return lax.dot_general(left, right, (((0,), (0,)), ((), ())), preferred_element_type=F32)


def against(left, right):
    return lax.dot_general(left, right, (((1,), (1,)), ((), ())), preferred_element_type=F32)


def column_sum(values):
    return jnp.sum(values.astype(F32), axis=0)


def head_mask(shape, head):
    lane = lax.broadcasted_iota(jnp.int32, shape, 1)
    return (lane >= head * HD) & (lane < (head + 1) * HD)


def pair_context(query, keys, values):
    total = None
    for head in range(2):
        mask = head_mask(query.shape, head)
        scores = against(jnp.where(mask, query, jnp.zeros_like(query)), keys)
        top = jnp.max(scores, axis=-1, keepdims=True)
        weight = jnp.exp(scores - top)
        inverse = 1.0 / jnp.sum(weight, axis=-1, keepdims=True)
        part = matmul((weight * inverse).astype(BF16), values)
        total = part if head == 0 else jnp.where(mask, part, total)
    return total.astype(BF16)


def forward_kernel(query_ref, pair_ref, context_ref):
    context_ref[...] = pair_context(query_ref[...], pair_ref[:, :PAIR], pair_ref[:, PAIR:])


def pair_grads(query, grad, keys, values):
    zeros = jnp.zeros_like(query)
    key_part = value_part = query_part = None
    for head in range(2):
        mask = head_mask(query.shape, head)
        own_query = jnp.where(mask, query, zeros)
        own_grad = jnp.where(mask, grad, zeros)
        scores = against(keys, own_query)
        top = jnp.max(scores, axis=0, keepdims=True)
        weight = jnp.exp(scores - top)
        inverse = 1.0 / jnp.sum(weight, axis=0, keepdims=True)
        probs = weight * inverse
        grad_probs = against(values, own_grad)
        delta = jnp.sum(probs * grad_probs, axis=0, keepdims=True)
        grad_scores = (probs * (grad_probs - delta)).astype(BF16)
        new_value = matmul(probs.astype(BF16), own_grad)
        new_key = matmul(grad_scores, own_query)
        new_query = over_rows(keys, grad_scores)
        if head == 0:
            key_part, value_part, query_part = new_key, new_value, new_query
        else:
            key_part = key_part + new_key
            value_part = value_part + new_value
            row = lax.broadcasted_iota(jnp.int32, new_query.shape, 0)
            query_part = jnp.where(row < HD, query_part, new_query)
    query_part = (query_part.T * (1.0 / math.sqrt(HD))).astype(BF16)
    return query_part, key_part.astype(BF16), value_part.astype(BF16)


def backward_kernel(query_ref, grad_ref, pair_ref, grad_query_ref, grad_pair_ref):
    grad_query_ref[...], grad_pair_ref[:, :PAIR], grad_pair_ref[:, PAIR:] = pair_grads(
        query_ref[...], grad_ref[...], pair_ref[:, :PAIR], pair_ref[:, PAIR:]
    )


def column_block(rows, width):
    return pl.BlockSpec((rows, width), lambda i: (0, i))


def attend(query, pairs):
    rows, width = query.shape
    keys = pairs.shape[0]
    return pl.pallas_call(
        forward_kernel,
        grid=(width // PAIR,),
        in_specs=[column_block(rows, PAIR), column_block(keys, 2 * PAIR)],
        out_specs=column_block(rows, PAIR),
        out_shape=jax.ShapeDtypeStruct((rows, width), BF16),
    )(query, pairs)


def attend_back(query, grad, pairs):
    rows, width = query.shape
    keys = pairs.shape[0]
    return pl.pallas_call(
        backward_kernel,
        grid=(width // PAIR,),
        in_specs=[
            column_block(rows, PAIR),
            column_block(rows, PAIR),
            column_block(keys, 2 * PAIR),
        ],
        out_specs=(column_block(rows, PAIR), column_block(keys, 2 * PAIR)),
        out_shape=(
            jax.ShapeDtypeStruct((rows, width), BF16),
            jax.ShapeDtypeStruct((keys, 2 * width), BF16),
        ),
    )(query, grad, pairs)


def mixed(left, right):
    parts = []
    for low in range(0, left.shape[1], PAIR):
        parts += [left[:, low : low + PAIR], right[:, low : low + PAIR]]
    return jnp.concatenate(parts, axis=1)


def unmixed(both):
    starts = range(0, both.shape[1], 2 * PAIR)
    return (
        jnp.concatenate([both[:, low : low + PAIR] for low in starts], axis=1),
        jnp.concatenate([both[:, low + PAIR : low + 2 * PAIR] for low in starts], axis=1),
    )


def gather_all(shard):
    return lax.all_gather(shard, "cp", axis=0, tiled=True)


def scatter_all(values):
    return lax.psum_scatter(values.astype(BF16), "cp", scatter_dimension=0, tiled=True)


def places():
    rep = lax.axis_index("rep")
    cp = lax.axis_index("cp")
    return rep, cp // 4, (cp // 2) % 2, cp % 2


def place_of(high, low, core):
    return 4 * high + 2 * low + core


def enter(reps):
    rep, high, low, core = places()
    barrier = pltpu.get_barrier_semaphore()
    peers = [
        (rep, place_of(high, low, 1 - core)),
        (rep, place_of(high, 1 - low, core)),
        (rep, place_of(1 - high, low, core)),
    ]
    peers += [((rep + k) % reps, place_of(high, low, core)) for k in range(1, reps)]
    for peer in peers:
        pl.semaphore_signal(barrier, inc=1, device_id=peer, device_id_type=MESH)
    pl.semaphore_wait(barrier, len(peers))


def remote(src, dst, sends, recvs, at, peer):
    return pltpu.make_async_remote_copy(
        src_ref=src,
        dst_ref=dst,
        send_sem=sends.at[at],
        recv_sem=recvs.at[at],
        device_id=peer,
        device_id_type=MESH,
    )


def gather_kernel(units, kinds, reps, pairs, *refs):
    count = len(kinds)
    ins = refs[:count]
    at = count
    if pairs:
        query_ref, key_ref, value_ref = refs[at : at + 3]
        at += 3
    outs = refs[at : at + count]
    at += count
    if pairs:
        context_ref, pair_ref = refs[at : at + 2]
        at += 2
    sends_z, recvs_z, sends_r, recvs_r, sends_c, recvs_c, local = refs[at : at + 7]
    rep, high, low, core = places()
    me = (rep, place_of(high, low, core))
    sibling = (rep, place_of(high, low, 1 - core))
    far = (rep, place_of(1 - high, low, core))
    near = (rep, place_of(high, 1 - low, core))
    enter(reps)
    copies = []

    def send(src, dst, sends, recvs, at, peer):
        remote(src, dst, sends, recvs, at, peer).start()

    def left(block, sends, recvs, at):
        remote(block, block, sends, recvs, at, me).wait_send()

    def arrived(block, sends, recvs, at):
        remote(block, block, sends, recvs, at, me).wait_recv()

    origins = (
        (high, low),
        (high, 1 - low),
        (1 - high, low),
        (1 - high, 1 - low),
    )

    def block_of(u, which, side, quarter):
        at, start, size = units[u]
        from_high, from_low = origins[which]
        return outs[at].at[from_high, from_low, side, quarter, :, pl.ds(start, size)]

    def held(p, which, side):
        from_high, from_low = origins[which]
        return pair_ref.at[p, from_high, from_low, side]

    if pairs:
        sends_k, recvs_k, sends_s, recvs_s = refs[at + 7 :]

    def offer(p):
        own = held(p, 0, core)
        send(own, own, sends_k, recvs_k, 3 * p + 1, far)
        send(own, own, sends_k, recvs_k, 3 * p, near)
        send(own, own, sends_s, recvs_s, 4 * p, sibling)

    total = len(units)
    kind_of = [kinds[at] for at, _, _ in units]

    def begin(u):
        at, start, size = units[u]
        block = ins[at].at[rep, :, pl.ds(start, size)]
        send(block, block_of(u, 0, core, rep), sends_z, recvs_z, 3 * u + 1, far)
        send(block, block_of(u, 0, core, rep), sends_z, recvs_z, 3 * u, near)

    def own_whole(u):
        at, start, size = units[u]
        if kind_of[u] == REST:
            return block_of(u, 0, core, slice(None))
        return ins[at].at[:, :, pl.ds(start, size)]

    for u in range(total):
        if kind_of[u] == FULL:
            begin(u)
    for u in range(total):
        if kind_of[u] != DEPTH:
            send(
                own_whole(u), block_of(u, 0, core, slice(None)), sends_c, recvs_c, 4 * u, sibling
            )
    for at in range(count):
        if kinds[at] != REST:
            copy = pltpu.make_async_copy(ins[at], outs[at].at[high, low, core], local.at[at])
            copy.start()
            copies.append(copy)

    for p in range(pairs):
        cols = pl.ds(PAIR * p, PAIR)
        pair_ref[p, high, low, core, :, :PAIR] = key_ref[:, cols]
        pair_ref[p, high, low, core, :, PAIR:] = value_ref[:, cols]
        if p < AHEAD:
            offer(p)

    def spread(u, which):
        block = block_of(u, which, core, rep)
        if kind_of[u] != REST:
            arrived(block, sends_z, recvs_z, 3 * u + which - 1)
            if which == 2:
                send(block, block, sends_z, recvs_z, 3 * u + 2, near)
        if kind_of[u] == DEPTH:
            return
        for j in range(1, reps):
            index = (3 * u + which - 1) * (reps - 1) + j - 1
            peer = ((rep + j) % reps, me[1])
            send(block, block, sends_r, recvs_r, index, peer)

    def pass_on(u, which):
        if kind_of[u] == DEPTH:
            return
        for j in range(1, reps):
            index = (3 * u + which - 1) * (reps - 1) + j - 1
            block = block_of(u, which, core, (rep + reps - j) % reps)
            arrived(block, sends_r, recvs_r, index)
        whole = block_of(u, which, core, slice(None))
        send(whole, whole, sends_c, recvs_c, 4 * u + which, sibling)

    lead = kind_of.count(FULL)

    def advance(step):
        if step < total:
            spread(step, 1)
            spread(step, 2)
            if step < lead:
                for u in range(lead, total):
                    if (u - lead) * lead // (total - lead) == step:
                        begin(u)
        if 1 <= step < total + 1:
            spread(step - 1, 3)
        if 2 <= step:
            for which in range(1, 4):
                pass_on(step - 2, which)

    def take(p, which):
        block = held(p, which, core)
        arrived(block, sends_k, recvs_k, 3 * p + which - 1)
        if which == 2:
            send(block, block, sends_k, recvs_k, 3 * p + 2, near)
        send(block, block, sends_s, recvs_s, 4 * p + which, sibling)

    def compute(p):
        for which in range(4):
            arrived(held(p, which, 1 - core), sends_s, recvs_s, 4 * p + which)
        cols = pl.ds(pl.multiple_of(p * PAIR, PAIR), PAIR)
        shape = (-1, PAIR)
        context_ref[:, cols] = pair_context(
            query_ref[:, cols],
            pair_ref[p, :, :, :, :, :PAIR].reshape(shape),
            pair_ref[p, :, :, :, :, PAIR:].reshape(shape),
        )

    steps = total + 2
    if pairs:
        for u in range(total):
            for which in range(1, 4):
                spread(u, which)

    def finish(step):
        if 0 < step <= total:
            for which in range(1, 4):
                pass_on(step - 1, which)

    if not pairs:
        for step in range(steps):
            advance(step)
    else:

        def step_all(t, carry):
            @pl.when(t < pairs)
            def _():
                take(t, 1)
                take(t, 2)

            @pl.when(t < pairs - AHEAD)
            def _():
                offer(t + AHEAD)

            @pl.when((t >= 1) & (t < pairs + 1))
            def _():
                take(t - 1, 3)

            for i in range(steps):

                @pl.when(t == i)
                def _(i=i):
                    finish(i)

            @pl.when((t >= 2) & (t < pairs + 2))
            def _():
                compute(t - 2)

            return carry

        lax.fori_loop(0, max(pairs + 2, steps), step_all, 0)
    for u in range(total):
        if kind_of[u] != DEPTH:
            for which in range(4):
                block = block_of(u, which, 1 - core, slice(None))
                arrived(block, sends_c, recvs_c, 4 * u + which)
    for copy in copies:
        copy.wait()
    for u, (at, start, size) in enumerate(units):
        if kind_of[u] != REST:
            block = ins[at].at[rep, :, pl.ds(start, size)]
            left(block, sends_z, recvs_z, 3 * u)
            left(block, sends_z, recvs_z, 3 * u + 1)
            left(block_of(u, 2, core, rep), sends_z, recvs_z, 3 * u + 2)
        if kind_of[u] != DEPTH:
            left(own_whole(u), sends_c, recvs_c, 4 * u)
            for which in range(1, 4):
                left(block_of(u, which, core, slice(None)), sends_c, recvs_c, 4 * u + which)
                for j in range(1, reps):
                    index = (3 * u + which - 1) * (reps - 1) + j - 1
                    left(block_of(u, which, core, rep), sends_r, recvs_r, index)
    for p in range(pairs):
        for at, which in enumerate((0, 0, 2)):
            left(held(p, which, core), sends_k, recvs_k, 3 * p + at)
        for which in range(4):
            left(held(p, which, core), sends_s, recvs_s, 4 * p + which)


def cut(width, pieces):
    size = width // pieces
    if size % 128:
        return [(0, width)]
    return [(size * i, size) for i in range(pieces)]


def gather_many(shards, pieces, kinds, identity, query=None, keys=None, values=None):
    reps = lax.axis_size("rep")
    count = len(shards)
    units = [
        (at, low, size)
        for at, shard in enumerate(shards)
        for low, size in cut(shard.shape[-1], pieces[at])
    ]
    total = len(units)
    hops = 3 * total * (reps - 1)
    dma = pltpu.SemaphoreType.DMA
    vmem = pl.BlockSpec(memory_space=pltpu.VMEM)
    out_shape = [
        jax.ShapeDtypeStruct(
            shard.shape if kind == REST else (2, 2, 2) + shard.shape, shard.dtype
        )
        for shard, kind in zip(shards, kinds)
    ]
    operands = list(shards)
    spaces = []
    more = []
    pairs = 0
    if query is not None:
        pairs = query.shape[1] // PAIR
        operands += [query, keys, values]
        spaces = [vmem] * 3
        out_shape += [
            jax.ShapeDtypeStruct(query.shape, BF16),
            jax.ShapeDtypeStruct((pairs, 2, 2, 2, keys.shape[0], 2 * PAIR), BF16),
        ]
        more = [dma((3 * pairs,))] * 2 + [dma((4 * pairs,))] * 2
    return pl.pallas_call(
        functools.partial(gather_kernel, units, tuple(kinds), reps, pairs),
        input_output_aliases={at: at for at in range(count) if kinds[at] == REST},
        out_shape=out_shape,
        in_specs=[pl.BlockSpec(memory_space=pl.ANY)] * count + spaces,
        out_specs=[pl.BlockSpec(memory_space=pl.ANY)] * count + spaces[:2],
        scratch_shapes=[dma((3 * total,))] * 2
        + [dma((hops,))] * 2
        + [dma((4 * total,))] * 2
        + [dma((count,))]
        + more,
        compiler_params=pltpu.CompilerParams(
            collective_id=identity, has_side_effects=True, vmem_limit_bytes=60 * 1024 * 1024
        ),
    )(*operands)


def summed(parts, kind):
    total = parts[0].astype(F32)
    for part in parts[1:]:
        total = total + part.astype(F32)
    return total.astype(kind)


def reduce_kernel(units, kinds, reps, fused, *refs):
    count = len(kinds)
    ins = refs[:count]
    at = count
    if fused:
        query_ref, grad_ref, pair_ref = refs[at : at + 3]
        at += 3
    outs = refs[at : at + count]
    at += count
    if fused:
        grad_query_ref, grad_key_ref, grad_value_ref = refs[at : at + 3]
        at += 3
    size = len(units)
    first, second, third, fourth, own, mid = [
        refs[at + i * size : at + (i + 1) * size] for i in range(6)
    ]
    sems = refs[at + 6 * size :]
    kind_of = [kinds[a] for a, _, _ in units]
    sends_c, recvs_c, sends_r, recvs_r, sends_z, recvs_z, sends_g, recvs_g = sems[:8]
    rep, high, low, core = places()
    me = (rep, place_of(high, low, core))
    sibling = (rep, place_of(high, low, 1 - core))
    far = (rep, place_of(1 - high, low, core))
    near = (rep, place_of(high, 1 - low, core))
    enter(reps)
    def send(src, dst, sends, recvs, at, peer):
        remote(src, dst, sends, recvs, at, peer).start()

    def left(block, sends, recvs, at):
        remote(block, block, sends, recvs, at, me).wait_send()

    def arrived(block, sends, recvs, at):
        remote(block, block, sends, recvs, at, me).wait_recv()

    for u, (a, start, width) in enumerate(units):
        if kind_of[u] == DEPTH:
            own[u][...] = ins[a][:, :, :, start : start + width]
            send(own[u].at[:, 1 - low], third[u], sends_z, recvs_z, 2 * u, near)
            continue
        block = ins[a].at[:, :, 1 - core, :, :, pl.ds(start, width)]
        send(block, first[u], sends_c, recvs_c, u, sibling)

    def over_core(u):
        a, start, width = units[u]
        if kind_of[u] == DEPTH:
            return
        arrived(first[u], sends_c, recvs_c, u)

        def step(i, carry):
            h, w, q = i // (2 * reps), (i // reps) % 2, i % reps
            mine = ins[a][h, w, core, q, :, start : start + width]
            first[u][h, w, q] = summed([first[u][h, w, q], mine], first[u].dtype)
            return carry

        lax.fori_loop(0, 4 * reps, step, 0)
        for k in range(1, reps):
            target = (rep + k) % reps
            send(
                first[u].at[:, :, target],
                second[u].at[k - 1],
                sends_r,
                recvs_r,
                u * (reps - 1) + k - 1,
                (target, me[1]),
            )

    def over_rep(u):
        a, start, width = units[u]
        if kind_of[u] == DEPTH:
            return
        for k in range(1, reps):
            arrived(second[u].at[k - 1], sends_r, recvs_r, u * (reps - 1) + k - 1)

        def step(i, carry):
            h, w = i // 2, i % 2
            parts = [first[u][h, w, rep]] + [second[u][k, h, w] for k in range(reps - 1)]
            total = summed(parts, first[u].dtype)
            if kind_of[u] == REST:
                outs[a][h, w, :, start : start + width] = total
            else:
                own[u][h, w] = total
            return carry

        lax.fori_loop(0, 4, step, 0)
        if kind_of[u] == FULL:
            send(own[u].at[:, 1 - low], third[u], sends_z, recvs_z, 2 * u, near)

    def over_near(u):
        if kind_of[u] == REST:
            return
        arrived(third[u], sends_z, recvs_z, 2 * u)
        for h in range(2):
            own[u][h, low] = summed([own[u][h, low], third[u][h]], own[u].dtype)
        send(own[u].at[1 - high, low], fourth[u], sends_z, recvs_z, 2 * u + 1, far)

    def over_far(u):
        if kind_of[u] == REST:
            return
        arrived(fourth[u], sends_z, recvs_z, 2 * u + 1)
        mid[u][rep] = summed([own[u][high, low], fourth[u][...]], mid[u].dtype)
        block = mid[u].at[rep]
        for k in range(1, reps):
            peer = ((rep + k) % reps, me[1])
            send(block, block, sends_g, recvs_g, u * (reps - 1) + k - 1, peer)

    stages = (over_core, over_rep, over_near, over_far)

    def advance(step):
        for lag, stage in enumerate(stages):
            if 0 <= step - lag < size:
                stage(step - lag)

    steps = size + len(stages) - 1
    if not fused:
        for stage in stages:
            for u in range(size):
                stage(u)
    else:
        terms, merged, from_near, from_far, held, sends_k, recvs_k, fetched = sems[8:]
        pairs = terms.shape[0]

        def fetch(p):
            return pltpu.make_async_copy(pair_ref.at[p], held.at[p % 2], fetched.at[p % 2])

        def hop(p, which):
            if which == 0:
                return remote(
                    terms.at[p, :, :, 1 - core], merged.at[p], sends_k, recvs_k, 3 * p, sibling
                )
            if which == 1:
                return remote(
                    merged.at[p, :, 1 - low], from_near.at[p], sends_k, recvs_k, 3 * p + 1, near
                )
            return remote(
                merged.at[p, 1 - high, low], from_far.at[p], sends_k, recvs_k, 3 * p + 2, far
            )

        def merge_core(p):
            arrived(merged.at[p], sends_k, recvs_k, 3 * p)
            for h in range(2):
                for w in range(2):
                    both = [merged[p, h, w], terms[p, h, w, core]]
                    merged[p, h, w] = summed(both, BF16)
            hop(p, 1).start()

        def merge_near(p):
            arrived(from_near.at[p], sends_k, recvs_k, 3 * p + 1)
            for h in range(2):
                merged[p, h, low] = summed([merged[p, h, low], from_near[p, h]], BF16)
            hop(p, 2).start()

        def merge_far(p):
            arrived(from_far.at[p], sends_k, recvs_k, 3 * p + 2)
            cols = pl.ds(pl.multiple_of(p * PAIR, PAIR), PAIR)
            both = summed([merged[p, high, low], from_far[p]], BF16)
            grad_key_ref[:, cols] = both[:, :PAIR]
            grad_value_ref[:, cols] = both[:, PAIR:]

        def compute(p):
            fetch(p).wait()

            @pl.when(p < pairs - 1)
            def _():
                fetch(p + 1).start()

            cols = pl.ds(pl.multiple_of(p * PAIR, PAIR), PAIR)
            slot = p % 2
            query_part, key_part, value_part = pair_grads(
                query_ref[:, cols], grad_ref[:, cols], held[slot, :, :PAIR], held[slot, :, PAIR:]
            )
            grad_query_ref[:, cols] = query_part
            shape = terms.shape[1:5] + (PAIR,)
            terms[p, :, :, :, :, :PAIR] = key_part.reshape(shape)
            terms[p, :, :, :, :, PAIR:] = value_part.reshape(shape)
            hop(p, 0).start()

        fetch(0).start()

        def step_all(t, carry):
            for lag, merge in ((1, merge_core), (2, merge_near), (3, merge_far)):

                @pl.when((t >= lag) & (t < pairs + lag))
                def _(lag=lag, merge=merge):
                    merge(t - lag)

            @pl.when(t < pairs)
            def _():
                compute(t)

            for i in range(steps):

                @pl.when(t == i)
                def _(i=i):
                    advance(i)

            return carry

        lax.fori_loop(0, max(pairs + 3, steps), step_all, 0)
        for p in range(pairs):
            for which in range(3):
                hop(p, which).wait_send()
    for u, (a, start, width) in enumerate(units):
        if kind_of[u] != REST:
            for k in range(1, reps):
                block = mid[u].at[(rep + reps - k) % reps]
                arrived(block, sends_g, recvs_g, u * (reps - 1) + k - 1)
            outs[a][:, :, start : start + width] = mid[u][...].astype(F32)
    for u, (a, start, width) in enumerate(units):
        cols = pl.ds(start, width)
        if kind_of[u] != DEPTH:
            left(ins[a].at[:, :, 1 - core, :, :, cols], sends_c, recvs_c, u)
        if kind_of[u] != REST:
            left(own[u].at[:, 1 - low], sends_z, recvs_z, 2 * u)
            left(own[u].at[1 - high, low], sends_z, recvs_z, 2 * u + 1)
        for k in range(1, reps):
            index = u * (reps - 1) + k - 1
            if kind_of[u] != DEPTH:
                left(first[u].at[:, :, (rep + k) % reps], sends_r, recvs_r, index)
            if kind_of[u] != REST:
                left(mid[u].at[rep], sends_g, recvs_g, index)


def split_rows(part):
    reps = lax.axis_size("rep")
    rows, width = part.shape
    return part.reshape(2, 2, 2, reps, rows // (8 * reps), width)


def reduce_many(blocks, pieces, kinds, identity, query=None, grad=None, pairs=None):
    reps = lax.axis_size("rep")
    count = len(blocks)
    units = [
        (at, low, size)
        for at, block in enumerate(blocks)
        for low, size in cut(block.shape[-1], pieces[at])
    ]
    dma = pltpu.SemaphoreType.DMA
    vmem = pl.BlockSpec(memory_space=pltpu.VMEM)

    def buffers(without, *lead):
        shapes = []
        for at, _, size in units:
            tile = (blocks[at].shape[-2], size)
            if kinds[at] == without:
                shapes.append(pltpu.VMEM((8, 128), BF16))
            else:
                shapes.append(pltpu.VMEM(lead + tile, blocks[at].dtype))
        return shapes

    total = len(units)
    out_shape = [
        jax.ShapeDtypeStruct((2, 2) + block.shape[4:], block.dtype)
        if kind == REST
        else jax.ShapeDtypeStruct((reps,) + block.shape[-2:], F32)
        for block, kind in zip(blocks, kinds)
    ]
    operands = list(blocks)
    in_specs = [vmem] * count
    more = []
    if pairs is not None:
        tokens, width = query.shape
        number = width // PAIR
        block = (tokens, 2 * PAIR)
        operands += [query, grad, pairs]
        in_specs += [vmem] * 2 + [pl.BlockSpec(memory_space=pl.ANY)]
        out_shape += [jax.ShapeDtypeStruct((tokens, width), BF16)] * 3
        more = [
            pltpu.VMEM((number, 2, 2, 2) + block, BF16),
            pltpu.VMEM((number, 2, 2) + block, BF16),
            pltpu.VMEM((number, 2) + block, BF16),
            pltpu.VMEM((number,) + block, BF16),
            pltpu.VMEM((2,) + pairs.shape[1:], BF16),
            dma((3 * number,)),
            dma((3 * number,)),
            dma((2,)),
        ]
    sums = pl.pallas_call(
        functools.partial(reduce_kernel, units, tuple(kinds), reps, pairs is not None),
        out_shape=out_shape,
        in_specs=in_specs,
        out_specs=[vmem] * len(out_shape),
        scratch_shapes=buffers(DEPTH, 2, 2, reps)
        + buffers(DEPTH, reps - 1, 2, 2)
        + buffers(REST, 2)
        + buffers(REST)
        + buffers(REST, 2, 2)
        + buffers(REST, reps)
        + [dma((total,))] * 2
        + [dma((total * (reps - 1),))] * 2
        + [dma((total * 2,))] * 2
        + [dma((total * (reps - 1),))] * 2
        + more,
        compiler_params=pltpu.CompilerParams(
            collective_id=identity, has_side_effects=True, vmem_limit_bytes=60 * 1024 * 1024
        ),
    )(*operands)
    totals = [
        total if kind == REST else total.reshape(-1, total.shape[2])
        for total, kind in zip(sums, kinds)
    ]
    return totals + list(sums[count:])


def blocked(shard):
    return shard.reshape(lax.axis_size("rep"), -1, shard.shape[1])


def divides(rows):
    reps = lax.axis_size("rep")
    return lax.axis_size("cp") == 8 and reps == 4 and rows % (8 * reps) == 0


def on_device(
    tokens,
    query_weight,
    query_bias,
    key_weight,
    value_weight,
    value_bias,
    output_weight,
    output_bias,
    first_gain,
    first_shift,
    up_weight,
    up_bias,
    down_weight,
    down_bias,
    second_gain,
    second_shift,
    cotangent,
):
    row_count = tokens.shape[1]
    width = tokens.shape[2]
    local_tokens = tokens[0]
    fast = divides(query_weight.shape[0])
    reps = lax.axis_size("rep")
    small = (
        query_bias,
        value_bias,
        output_bias,
        first_gain,
        first_shift,
        up_bias,
        down_bias,
        second_gain,
        second_shift,
    )
    if fast:
        rows = []
        for vector in small:
            lines = -(-vector.shape[0] // 128)
            rows.append(
                jnp.pad(vector.astype(F32), (0, 128 * lines - vector.shape[0])).reshape(lines, 128)
            )
        packed = jnp.concatenate(rows, axis=0)
        packed = jnp.pad(packed, ((0, -packed.shape[0] % (8 * reps)), (0, 0))).astype(BF16)
        shards = (key_weight, value_weight, query_weight, packed)
        shards += (output_weight, up_weight, down_weight)
        w_key, w_value, w_query, gathered, *begun = gather_many(
            [blocked(shard) for shard in shards],
            (1, 1, 1, 1, 1, 2, 2),
            (FULL,) * 4 + (DEPTH,) * 3,
            1,
        )
        w_key, w_value, w_query = [w.reshape(-1, width) for w in (w_key, w_value, w_query)]
        gathered = gathered.reshape(-1, packed.shape[0], 128)
    else:
        w_query, w_key, w_value = [
            gather_all(shard) for shard in (query_weight, key_weight, value_weight)
        ]
        gathered = lax.all_gather(jnp.concatenate(small)[None], "cp", axis=0, tiled=True)
    vectors = []
    at = 0
    for vector in small:
        size = vector.shape[0]
        if fast:
            lines = -(-size // 128)
            part = gathered[:, at : at + lines].reshape(-1, 128 * lines)[:, :size]
            at += lines
        else:
            part = gathered[:, at : at + size]
            at += size
        vectors.append(part.reshape(-1).astype(F32))
    b_query, b_value, b_output, gain_one, shift_one, b_up, b_down, gain_two, shift_two = vectors
    key_rows = matmul(local_tokens, w_key).astype(BF16)
    value_rows = (matmul(local_tokens, w_value) + b_value).astype(BF16)
    chunk = width // CHUNKS
    query_rows = (matmul(local_tokens, w_query) + b_query).astype(BF16)
    query_scaled = query_rows * jnp.asarray(1.0 / math.sqrt(HD), BF16)
    if fast:
        w_output, w_up, w_down, context_low, pairs = gather_many(
            begun,
            (1, 2, 2),
            (REST,) * 3,
            2,
            query_scaled,
            key_rows,
            value_rows,
        )
        w_output, w_down = w_output.reshape(-1, width), w_down.reshape(-1, width)
        w_up = w_up.reshape(-1, up_weight.shape[1])
        pairs = pairs.reshape(pairs.shape[0], -1, 2 * PAIR)
    else:
        w_output, w_up, w_down = [
            gather_all(shard) for shard in (output_weight, up_weight, down_weight)
        ]
        pair_rows = mixed(key_rows, value_rows)
        queries = [query_scaled[:, chunk * i : chunk * (i + 1)] for i in range(CHUNKS)]
        pairs = [
            lax.all_gather(
                pair_rows[:, 2 * chunk * i : 2 * chunk * (i + 1)], "cp", axis=0, tiled=True
            )
            for i in range(CHUNKS)
        ]
        context_low = jnp.concatenate(
            [attend(query, pair) for query, pair in zip(queries, pairs)], axis=1
        )
    attn_out = matmul(context_low, w_output) + b_output
    resid_first = local_tokens.astype(F32) + attn_out
    first_norm, pull_first = jax.vjp(normalize, resid_first, gain_one, shift_one)
    first_low = first_norm.astype(BF16)
    inner_act = matmul(first_low, w_up) + b_up
    hidden, pull_gelu = jax.vjp(gelu_exact, inner_act)
    hidden_low = hidden.astype(BF16)
    resid_second = first_norm + (matmul(hidden_low, w_down) + b_down)
    layer_out, pull_second = jax.vjp(normalize, resid_second, gain_two, shift_two)

    grad_resid2, grad_gain2, grad_shift2 = pull_second(cotangent[0])
    grad_outer = grad_resid2.astype(BF16)
    grad_down_bias = column_sum(grad_outer)
    part_down = over_rows(hidden_low, grad_outer).astype(BF16)
    grad_inner = pull_gelu(against(grad_outer, w_down))[0].astype(BF16)
    grad_up_bias = column_sum(grad_inner)
    part_up = over_rows(first_low, grad_inner).astype(BF16)
    grad_first = grad_resid2 + against(grad_inner, w_up)
    grad_resid1, grad_gain1, grad_shift1 = pull_first(grad_first)
    grad_attn = grad_resid1.astype(BF16)
    grad_output_bias = column_sum(grad_attn)
    part_output = over_rows(context_low, grad_attn).astype(BF16)
    grad_context = against(grad_attn, w_output).astype(BF16)

    if fast:
        (
            *begun,
            grad_query_low,
            grad_key_low,
            grad_value_low,
        ) = reduce_many(
            [split_rows(part) for part in (part_down, part_up, part_output)],
            (2, 2, 1),
            (REST,) * 3,
            3,
            query_scaled,
            grad_context,
            pairs,
        )
    else:
        grad_queries = []
        grad_pairs = []
        for i in range(CHUNKS):
            grad_query, grad_terms = attend_back(
                queries[i], grad_context[:, chunk * i : chunk * (i + 1)], pairs[i]
            )
            grad_queries.append(grad_query)
            grad_pairs.append(
                lax.psum_scatter(grad_terms, "cp", scatter_dimension=0, tiled=True)
            )
        grad_query_low = jnp.concatenate(grad_queries, axis=1)
        grad_key_low, grad_value_low = unmixed(jnp.concatenate(grad_pairs, axis=1))
    part_query = over_rows(local_tokens, grad_query_low).astype(BF16)
    part_key = over_rows(local_tokens, grad_key_low).astype(BF16)
    part_value = over_rows(local_tokens, grad_value_low).astype(BF16)
    grad_tokens = (
        grad_resid1
        + against(grad_query_low, w_query)
        + against(grad_key_low, w_key)
        + against(grad_value_low, w_value)
    )

    small_grads = (
        column_sum(grad_query_low),
        column_sum(grad_value_low),
        grad_output_bias,
        grad_gain1,
        grad_shift1,
        grad_up_bias,
        grad_down_bias,
        grad_gain2,
        grad_shift2,
    )
    owners = lax.axis_size("cp")
    total_sq = jnp.broadcast_to(jnp.sum(grad_tokens * grad_tokens), (owners, 1))
    flat = jnp.concatenate(
        [vector.reshape(owners, -1) for vector in small_grads] + [total_sq], axis=1
    )
    if fast:
        flat = jnp.pad(flat, ((0, 0), (0, -flat.shape[1] % (8 * 128 * reps))))
        blocks = [split_rows(part) for part in (part_query, part_key, part_value)]
        full_query, full_key, full_value, sums, full_down, full_up, full_output = reduce_many(
            blocks + [flat.reshape(2, 2, 2, reps, -1, 128)] + begun,
            (1,) * 7,
            (FULL,) * 4 + (DEPTH,) * 3,
            4,
        )
        sums = sums.reshape(-1)
    else:
        parts = (part_down, part_up, part_output, part_query, part_key, part_value)
        shards = [scatter_all(part) for part in parts]
        full_down, full_up, full_output, full_query, full_key, full_value = [
            part.astype(F32) for part in lax.psum(tuple(shards), "rep")
        ]
        sums = lax.psum(flat, ("rep", "cp"))
        sums = lax.dynamic_slice_in_dim(sums, lax.axis_index("cp"), 1, 0)[0]
    reduced = []
    at = 0
    for shard in small:
        reduced.append(sums[at : at + shard.shape[0]])
        at += shard.shape[0]
    entries = lax.axis_size("rep") * owners * row_count * width
    rms_values = jnp.sqrt(sums[at : at + 1] / entries)

    return (
        layer_out[None],
        grad_tokens[None],
        full_query,
        reduced[0],
        full_key,
        full_value,
        reduced[1],
        full_output,
        reduced[2],
        reduced[3],
        reduced[4],
        full_up,
        reduced[5],
        full_down,
        reduced[6],
        reduced[7],
        reduced[8],
        rms_values,
    )


def solution(mesh):
    rows = P("cp", None)
    vector = P("cp")
    whole = P("rep", "cp", None)
    params = (
        rows,
        vector,
        rows,
        rows,
        vector,
        rows,
        vector,
        vector,
        vector,
        rows,
        vector,
        rows,
        vector,
        vector,
        vector,
    )
    return jax.shard_map(
        on_device,
        mesh=mesh,
        in_specs=(whole,) + params + (whole,),
        out_specs=(whole, whole) + params + (P(),),
        check_vma=False,
    )
```

```python
import functools
import math

import jax
import jax.numpy as jnp
from jax import lax
from jax.experimental import pallas as pl
from jax.experimental.pallas import tpu as pltpu
from jax.sharding import PartitionSpec as P

HD = 64
PAIR = 2 * HD
CHUNKS = 3
AHEAD = 2
FULL, DEPTH, REST = range(3)
EPSILON = 1e-12
BF16 = jnp.bfloat16
F32 = jnp.float32
MESH = pl.DeviceIdType.MESH


def normalize(values, norm_gain, norm_shift):
    center = values - jnp.mean(values, axis=-1, keepdims=True)
    spread = jnp.mean(center * center, axis=-1, keepdims=True)
    return center * lax.rsqrt(spread + EPSILON) * norm_gain + norm_shift


def gelu_exact(values):
    return 0.5 * values * (1.0 + lax.erf(values * (1.0 / math.sqrt(2.0))))


def matmul(left, right):
    return jnp.dot(left, right, preferred_element_type=F32)


def over_rows(left, right):
    return lax.dot_general(left, right, (((0,), (0,)), ((), ())), preferred_element_type=F32)


def against(left, right):
    return lax.dot_general(left, right, (((1,), (1,)), ((), ())), preferred_element_type=F32)


def column_sum(values):
    return jnp.sum(values.astype(F32), axis=0)


def head_mask(shape, head):
    lane = lax.broadcasted_iota(jnp.int32, shape, 1)
    return (lane >= head * HD) & (lane < (head + 1) * HD)


def pair_context(query, keys, values):
    total = None
    for head in range(2):
        mask = head_mask(query.shape, head)
        scores = against(jnp.where(mask, query, jnp.zeros_like(query)), keys)
        top = jnp.max(scores, axis=-1, keepdims=True)
        weight = jnp.exp(scores - top)
        inverse = 1.0 / jnp.sum(weight, axis=-1, keepdims=True)
        part = matmul((weight * inverse).astype(BF16), values)
        total = part if head == 0 else jnp.where(mask, part, total)
    return total.astype(BF16)


def forward_kernel(query_ref, pair_ref, context_ref):
    context_ref[...] = pair_context(query_ref[...], pair_ref[:, :PAIR], pair_ref[:, PAIR:])


def pair_grads(query, grad, keys, values):
    zeros = jnp.zeros_like(query)
    key_part = value_part = query_part = None
    for head in range(2):
        mask = head_mask(query.shape, head)
        own_query = jnp.where(mask, query, zeros)
        own_grad = jnp.where(mask, grad, zeros)
        scores = against(keys, own_query)
        top = jnp.max(scores, axis=0, keepdims=True)
        weight = jnp.exp(scores - top)
        inverse = 1.0 / jnp.sum(weight, axis=0, keepdims=True)
        probs = weight * inverse
        grad_probs = against(values, own_grad)
        delta = jnp.sum(probs * grad_probs, axis=0, keepdims=True)
        grad_scores = (probs * (grad_probs - delta)).astype(BF16)
        new_value = matmul(probs.astype(BF16), own_grad)
        new_key = matmul(grad_scores, own_query)
        new_query = over_rows(keys, grad_scores)
        if head == 0:
            key_part, value_part, query_part = new_key, new_value, new_query
        else:
            key_part = key_part + new_key
            value_part = value_part + new_value
            row = lax.broadcasted_iota(jnp.int32, new_query.shape, 0)
            query_part = jnp.where(row < HD, query_part, new_query)
    query_part = (query_part.T * (1.0 / math.sqrt(HD))).astype(BF16)
    return query_part, key_part.astype(BF16), value_part.astype(BF16)


def backward_kernel(query_ref, grad_ref, pair_ref, grad_query_ref, grad_pair_ref):
    grad_query_ref[...], grad_pair_ref[:, :PAIR], grad_pair_ref[:, PAIR:] = pair_grads(
        query_ref[...], grad_ref[...], pair_ref[:, :PAIR], pair_ref[:, PAIR:]
    )


def column_block(rows, width):
    return pl.BlockSpec((rows, width), lambda i: (0, i))


def attend(query, pairs):
    rows, width = query.shape
    keys = pairs.shape[0]
    return pl.pallas_call(
        forward_kernel,
        grid=(width // PAIR,),
        in_specs=[column_block(rows, PAIR), column_block(keys, 2 * PAIR)],
        out_specs=column_block(rows, PAIR),
        out_shape=jax.ShapeDtypeStruct((rows, width), BF16),
    )(query, pairs)


def attend_back(query, grad, pairs):
    rows, width = query.shape
    keys = pairs.shape[0]
    return pl.pallas_call(
        backward_kernel,
        grid=(width // PAIR,),
        in_specs=[
            column_block(rows, PAIR),
            column_block(rows, PAIR),
            column_block(keys, 2 * PAIR),
        ],
        out_specs=(column_block(rows, PAIR), column_block(keys, 2 * PAIR)),
        out_shape=(
            jax.ShapeDtypeStruct((rows, width), BF16),
            jax.ShapeDtypeStruct((keys, 2 * width), BF16),
        ),
    )(query, grad, pairs)


def mixed(left, right):
    parts = []
    for low in range(0, left.shape[1], PAIR):
        parts += [left[:, low : low + PAIR], right[:, low : low + PAIR]]
    return jnp.concatenate(parts, axis=1)


def unmixed(both):
    starts = range(0, both.shape[1], 2 * PAIR)
    return (
        jnp.concatenate([both[:, low : low + PAIR] for low in starts], axis=1),
        jnp.concatenate([both[:, low + PAIR : low + 2 * PAIR] for low in starts], axis=1),
    )


def gather_all(shard):
    return lax.all_gather(shard, "cp", axis=0, tiled=True)


def scatter_all(values):
    return lax.psum_scatter(values.astype(BF16), "cp", scatter_dimension=0, tiled=True)


def places():
    rep = lax.axis_index("rep")
    cp = lax.axis_index("cp")
    return rep, cp // 4, (cp // 2) % 2, cp % 2


def place_of(high, low, core):
    return 4 * high + 2 * low + core


def enter(reps):
    rep, high, low, core = places()
    barrier = pltpu.get_barrier_semaphore()
    peers = [
        (rep, place_of(high, low, 1 - core)),
        (rep, place_of(high, 1 - low, core)),
        (rep, place_of(1 - high, low, core)),
    ]
    peers += [((rep + k) % reps, place_of(high, low, core)) for k in range(1, reps)]
    for peer in peers:
        pl.semaphore_signal(barrier, inc=1, device_id=peer, device_id_type=MESH)
    pl.semaphore_wait(barrier, len(peers))


def remote(src, dst, sends, recvs, at, peer):
    return pltpu.make_async_remote_copy(
        src_ref=src,
        dst_ref=dst,
        send_sem=sends.at[at],
        recv_sem=recvs.at[at],
        device_id=peer,
        device_id_type=MESH,
    )


def gather_kernel(units, kinds, reps, pairs, *refs):
    count = len(kinds)
    ins = refs[:count]
    at = count
    if pairs:
        query_ref, key_ref, value_ref = refs[at : at + 3]
        at += 3
    outs = refs[at : at + count]
    at += count
    if pairs:
        context_ref, pair_ref = refs[at : at + 2]
        at += 2
    sends_z, recvs_z, sends_r, recvs_r, sends_c, recvs_c, local = refs[at : at + 7]
    rep, high, low, core = places()
    me = (rep, place_of(high, low, core))
    sibling = (rep, place_of(high, low, 1 - core))
    far = (rep, place_of(1 - high, low, core))
    near = (rep, place_of(high, 1 - low, core))
    enter(reps)
    copies = []

    def send(src, dst, sends, recvs, at, peer):
        remote(src, dst, sends, recvs, at, peer).start()

    def left(block, sends, recvs, at):
        remote(block, block, sends, recvs, at, me).wait_send()

    def arrived(block, sends, recvs, at):
        remote(block, block, sends, recvs, at, me).wait_recv()

    origins = (
        (high, low),
        (high, 1 - low),
        (1 - high, low),
        (1 - high, 1 - low),
    )

    def block_of(u, which, side, quarter):
        at, start, size = units[u]
        from_high, from_low = origins[which]
        return outs[at].at[from_high, from_low, side, quarter, :, pl.ds(start, size)]

    def held(p, which, side):
        from_high, from_low = origins[which]
        return pair_ref.at[p, from_high, from_low, side]

    if pairs:
        sends_k, recvs_k, sends_s, recvs_s = refs[at + 7 :]

    def offer(p):
        own = held(p, 0, core)
        send(own, own, sends_k, recvs_k, 3 * p + 1, far)
        send(own, own, sends_k, recvs_k, 3 * p, near)
        send(own, own, sends_s, recvs_s, 4 * p, sibling)

    total = len(units)
    kind_of = [kinds[at] for at, _, _ in units]

    def begin(u):
        at, start, size = units[u]
        block = ins[at].at[rep, :, pl.ds(start, size)]
        send(block, block_of(u, 0, core, rep), sends_z, recvs_z, 3 * u + 1, far)
        send(block, block_of(u, 0, core, rep), sends_z, recvs_z, 3 * u, near)

    def own_whole(u):
        at, start, size = units[u]
        if kind_of[u] == REST:
            return block_of(u, 0, core, slice(None))
        return ins[at].at[:, :, pl.ds(start, size)]

    for u in range(total):
        if kind_of[u] == FULL:
            begin(u)
    for u in range(total):
        if kind_of[u] != DEPTH:
            send(
                own_whole(u), block_of(u, 0, core, slice(None)), sends_c, recvs_c, 4 * u, sibling
            )
    for at in range(count):
        if kinds[at] != REST:
            copy = pltpu.make_async_copy(ins[at], outs[at].at[high, low, core], local.at[at])
            copy.start()
            copies.append(copy)

    for p in range(pairs):
        cols = pl.ds(PAIR * p, PAIR)
        pair_ref[p, high, low, core, :, :PAIR] = key_ref[:, cols]
        pair_ref[p, high, low, core, :, PAIR:] = value_ref[:, cols]
        if p < AHEAD:
            offer(p)

    def spread(u, which):
        block = block_of(u, which, core, rep)
        if kind_of[u] != REST:
            arrived(block, sends_z, recvs_z, 3 * u + which - 1)
            if which == 2:
                send(block, block, sends_z, recvs_z, 3 * u + 2, near)
        if kind_of[u] == DEPTH:
            return
        for j in range(1, reps):
            index = (3 * u + which - 1) * (reps - 1) + j - 1
            peer = ((rep + j) % reps, me[1])
            send(block, block, sends_r, recvs_r, index, peer)

    def pass_on(u, which):
        if kind_of[u] == DEPTH:
            return
        for j in range(1, reps):
            index = (3 * u + which - 1) * (reps - 1) + j - 1
            block = block_of(u, which, core, (rep + reps - j) % reps)
            arrived(block, sends_r, recvs_r, index)
        whole = block_of(u, which, core, slice(None))
        send(whole, whole, sends_c, recvs_c, 4 * u + which, sibling)

    lead = kind_of.count(FULL)

    def advance(step):
        if step < total:
            spread(step, 1)
            spread(step, 2)
            if step < lead:
                for u in range(lead, total):
                    if (u - lead) * lead // (total - lead) == step:
                        begin(u)
        if 1 <= step < total + 1:
            spread(step - 1, 3)
        if 2 <= step:
            for which in range(1, 4):
                pass_on(step - 2, which)

    def take(p, which):
        block = held(p, which, core)
        arrived(block, sends_k, recvs_k, 3 * p + which - 1)
        if which == 2:
            send(block, block, sends_k, recvs_k, 3 * p + 2, near)
        send(block, block, sends_s, recvs_s, 4 * p + which, sibling)

    def compute(p):
        for which in range(4):
            arrived(held(p, which, 1 - core), sends_s, recvs_s, 4 * p + which)
        cols = pl.ds(pl.multiple_of(p * PAIR, PAIR), PAIR)
        shape = (-1, PAIR)
        context_ref[:, cols] = pair_context(
            query_ref[:, cols],
            pair_ref[p, :, :, :, :, :PAIR].reshape(shape),
            pair_ref[p, :, :, :, :, PAIR:].reshape(shape),
        )

    steps = total + 2
    if pairs:
        for u in range(total):
            for which in range(1, 4):
                spread(u, which)

    def finish(step):
        if 0 < step <= total:
            for which in range(1, 4):
                pass_on(step - 1, which)

    if not pairs:
        for step in range(steps):
            advance(step)
    else:

        def step_all(t, carry):
            @pl.when(t < pairs)
            def _():
                take(t, 1)
                take(t, 2)

            @pl.when(t < pairs - AHEAD)
            def _():
                offer(t + AHEAD)

            @pl.when((t >= 1) & (t < pairs + 1))
            def _():
                take(t - 1, 3)

            for i in range(steps):

                @pl.when(t == i)
                def _(i=i):
                    finish(i)

            @pl.when((t >= 2) & (t < pairs + 2))
            def _():
                compute(t - 2)

            return carry

        lax.fori_loop(0, max(pairs + 2, steps), step_all, 0)
    for u in range(total):
        if kind_of[u] != DEPTH:
            for which in range(4):
                block = block_of(u, which, 1 - core, slice(None))
                arrived(block, sends_c, recvs_c, 4 * u + which)
    for copy in copies:
        copy.wait()
    for u, (at, start, size) in enumerate(units):
        if kind_of[u] != REST:
            block = ins[at].at[rep, :, pl.ds(start, size)]
            left(block, sends_z, recvs_z, 3 * u)
            left(block, sends_z, recvs_z, 3 * u + 1)
            left(block_of(u, 2, core, rep), sends_z, recvs_z, 3 * u + 2)
        if kind_of[u] != DEPTH:
            left(own_whole(u), sends_c, recvs_c, 4 * u)
            for which in range(1, 4):
                left(block_of(u, which, core, slice(None)), sends_c, recvs_c, 4 * u + which)
                for j in range(1, reps):
                    index = (3 * u + which - 1) * (reps - 1) + j - 1
                    left(block_of(u, which, core, rep), sends_r, recvs_r, index)
    for p in range(pairs):
        for at, which in enumerate((0, 0, 2)):
            left(held(p, which, core), sends_k, recvs_k, 3 * p + at)
        for which in range(4):
            left(held(p, which, core), sends_s, recvs_s, 4 * p + which)


def cut(width, pieces):
    size = width // pieces
    if size % 128:
        return [(0, width)]
    return [(size * i, size) for i in range(pieces)]


def gather_many(shards, pieces, kinds, identity, query=None, keys=None, values=None):
    reps = lax.axis_size("rep")
    count = len(shards)
    units = [
        (at, low, size)
        for at, shard in enumerate(shards)
        for low, size in cut(shard.shape[-1], pieces[at])
    ]
    total = len(units)
    hops = 3 * total * (reps - 1)
    dma = pltpu.SemaphoreType.DMA
    vmem = pl.BlockSpec(memory_space=pltpu.VMEM)
    out_shape = [
        jax.ShapeDtypeStruct(
            shard.shape if kind == REST else (2, 2, 2) + shard.shape, shard.dtype
        )
        for shard, kind in zip(shards, kinds)
    ]
    operands = list(shards)
    spaces = []
    more = []
    pairs = 0
    if query is not None:
        pairs = query.shape[1] // PAIR
        operands += [query, keys, values]
        spaces = [vmem] * 3
        out_shape += [
            jax.ShapeDtypeStruct(query.shape, BF16),
            jax.ShapeDtypeStruct((pairs, 2, 2, 2, keys.shape[0], 2 * PAIR), BF16),
        ]
        more = [dma((3 * pairs,))] * 2 + [dma((4 * pairs,))] * 2
    return pl.pallas_call(
        functools.partial(gather_kernel, units, tuple(kinds), reps, pairs),
        input_output_aliases={at: at for at in range(count) if kinds[at] == REST},
        out_shape=out_shape,
        in_specs=[
            pl.BlockSpec(memory_space=pl.ANY if kind == REST else pltpu.VMEM) for kind in kinds
        ]
        + spaces,
        out_specs=[pl.BlockSpec(memory_space=pl.ANY)] * count + spaces[:2],
        scratch_shapes=[dma((3 * total,))] * 2
        + [dma((hops,))] * 2
        + [dma((4 * total,))] * 2
        + [dma((count,))]
        + more,
        compiler_params=pltpu.CompilerParams(
            collective_id=identity, has_side_effects=True, vmem_limit_bytes=60 * 1024 * 1024
        ),
    )(*operands)


def summed(parts, kind):
    total = parts[0].astype(F32)
    for part in parts[1:]:
        total = total + part.astype(F32)
    return total.astype(kind)


def reduce_kernel(units, kinds, reps, fused, *refs):
    count = len(kinds)
    ins = refs[:count]
    at = count
    if fused:
        query_ref, grad_ref, pair_ref = refs[at : at + 3]
        at += 3
    outs = refs[at : at + count]
    at += count
    if fused:
        grad_query_ref, grad_key_ref, grad_value_ref = refs[at : at + 3]
        at += 3
    size = len(units)
    first, second, third, fourth, own, mid = [
        refs[at + i * size : at + (i + 1) * size] for i in range(6)
    ]
    sems = refs[at + 6 * size :]
    kind_of = [kinds[a] for a, _, _ in units]
    sends_c, recvs_c, sends_r, recvs_r, sends_z, recvs_z, sends_g, recvs_g = sems[:8]
    rep, high, low, core = places()
    me = (rep, place_of(high, low, core))
    sibling = (rep, place_of(high, low, 1 - core))
    far = (rep, place_of(1 - high, low, core))
    near = (rep, place_of(high, 1 - low, core))
    enter(reps)
    def send(src, dst, sends, recvs, at, peer):
        remote(src, dst, sends, recvs, at, peer).start()

    def left(block, sends, recvs, at):
        remote(block, block, sends, recvs, at, me).wait_send()

    def arrived(block, sends, recvs, at):
        remote(block, block, sends, recvs, at, me).wait_recv()

    for u, (a, start, width) in enumerate(units):
        if kind_of[u] == DEPTH:
            own[u][...] = ins[a][:, :, :, start : start + width]
            send(own[u].at[:, 1 - low], third[u], sends_z, recvs_z, 2 * u, near)
            continue
        block = ins[a].at[:, :, 1 - core, :, :, pl.ds(start, width)]
        send(block, first[u], sends_c, recvs_c, u, sibling)

    def over_core(u):
        a, start, width = units[u]
        if kind_of[u] == DEPTH:
            return
        arrived(first[u], sends_c, recvs_c, u)

        def step(i, carry):
            h, w, q = i // (2 * reps), (i // reps) % 2, i % reps
            mine = ins[a][h, w, core, q, :, start : start + width]
            first[u][h, w, q] = summed([first[u][h, w, q], mine], first[u].dtype)
            return carry

        lax.fori_loop(0, 4 * reps, step, 0)
        for k in range(1, reps):
            target = (rep + k) % reps
            send(
                first[u].at[:, :, target],
                second[u].at[k - 1],
                sends_r,
                recvs_r,
                u * (reps - 1) + k - 1,
                (target, me[1]),
            )

    def over_rep(u):
        a, start, width = units[u]
        if kind_of[u] == DEPTH:
            return
        for k in range(1, reps):
            arrived(second[u].at[k - 1], sends_r, recvs_r, u * (reps - 1) + k - 1)

        def step(i, carry):
            h, w = i // 2, i % 2
            parts = [first[u][h, w, rep]] + [second[u][k, h, w] for k in range(reps - 1)]
            total = summed(parts, first[u].dtype)
            if kind_of[u] == REST:
                outs[a][h, w, :, start : start + width] = total
            else:
                own[u][h, w] = total
            return carry

        lax.fori_loop(0, 4, step, 0)
        if kind_of[u] == FULL:
            send(own[u].at[:, 1 - low], third[u], sends_z, recvs_z, 2 * u, near)

    def over_near(u):
        if kind_of[u] == REST:
            return
        arrived(third[u], sends_z, recvs_z, 2 * u)
        for h in range(2):
            own[u][h, low] = summed([own[u][h, low], third[u][h]], own[u].dtype)
        send(own[u].at[1 - high, low], fourth[u], sends_z, recvs_z, 2 * u + 1, far)

    def over_far(u):
        if kind_of[u] == REST:
            return
        arrived(fourth[u], sends_z, recvs_z, 2 * u + 1)
        mid[u][rep] = summed([own[u][high, low], fourth[u][...]], mid[u].dtype)
        block = mid[u].at[rep]
        for k in range(1, reps):
            peer = ((rep + k) % reps, me[1])
            send(block, block, sends_g, recvs_g, u * (reps - 1) + k - 1, peer)

    stages = (over_core, over_rep, over_near, over_far)

    def advance(step):
        for lag, stage in enumerate(stages):
            if 0 <= step - lag < size:
                stage(step - lag)

    steps = size + len(stages) - 1
    if not fused:
        whole = [u for u in range(size) if kind_of[u] != DEPTH]
        rest = [u for u in range(size) if kind_of[u] == DEPTH]
        order = [(over_core, whole), (over_near, rest), (over_rep, whole)]
        order += [(over_far, rest), (over_near, whole), (over_far, whole)]
        for stage, members in order:
            for u in members:
                stage(u)
    else:
        terms, merged, from_near, from_far, held, sends_k, recvs_k, fetched = sems[8:]
        pairs = terms.shape[0]

        def fetch(p):
            return pltpu.make_async_copy(pair_ref.at[p], held.at[p % 2], fetched.at[p % 2])

        def hop(p, which):
            if which == 0:
                return remote(
                    terms.at[p, :, :, 1 - core], merged.at[p], sends_k, recvs_k, 3 * p, sibling
                )
            if which == 1:
                return remote(
                    merged.at[p, :, 1 - low], from_near.at[p], sends_k, recvs_k, 3 * p + 1, near
                )
            return remote(
                merged.at[p, 1 - high, low], from_far.at[p], sends_k, recvs_k, 3 * p + 2, far
            )

        def merge_core(p):
            arrived(merged.at[p], sends_k, recvs_k, 3 * p)
            for h in range(2):
                for w in range(2):
                    both = [merged[p, h, w], terms[p, h, w, core]]
                    merged[p, h, w] = summed(both, BF16)
            hop(p, 1).start()

        def merge_near(p):
            arrived(from_near.at[p], sends_k, recvs_k, 3 * p + 1)
            for h in range(2):
                merged[p, h, low] = summed([merged[p, h, low], from_near[p, h]], BF16)
            hop(p, 2).start()

        def merge_far(p):
            arrived(from_far.at[p], sends_k, recvs_k, 3 * p + 2)
            cols = pl.ds(pl.multiple_of(p * PAIR, PAIR), PAIR)
            both = summed([merged[p, high, low], from_far[p]], BF16)
            grad_key_ref[:, cols] = both[:, :PAIR]
            grad_value_ref[:, cols] = both[:, PAIR:]

        def compute(p):
            fetch(p).wait()

            @pl.when(p < pairs - 1)
            def _():
                fetch(p + 1).start()

            cols = pl.ds(pl.multiple_of(p * PAIR, PAIR), PAIR)
            slot = p % 2
            query_part, key_part, value_part = pair_grads(
                query_ref[:, cols], grad_ref[:, cols], held[slot, :, :PAIR], held[slot, :, PAIR:]
            )
            grad_query_ref[:, cols] = query_part
            shape = terms.shape[1:5] + (PAIR,)
            terms[p, :, :, :, :, :PAIR] = key_part.reshape(shape)
            terms[p, :, :, :, :, PAIR:] = value_part.reshape(shape)
            hop(p, 0).start()

        fetch(0).start()

        def step_all(t, carry):
            for lag, merge in ((1, merge_core), (2, merge_near), (3, merge_far)):

                @pl.when((t >= lag) & (t < pairs + lag))
                def _(lag=lag, merge=merge):
                    merge(t - lag)

            @pl.when(t < pairs)
            def _():
                compute(t)

            for i in range(steps):

                @pl.when(t == i)
                def _(i=i):
                    advance(i)

            return carry

        lax.fori_loop(0, max(pairs + 3, steps), step_all, 0)
        for p in range(pairs):
            for which in range(3):
                hop(p, which).wait_send()
    for u, (a, start, width) in enumerate(units):
        if kind_of[u] != REST:
            for k in range(1, reps):
                block = mid[u].at[(rep + reps - k) % reps]
                arrived(block, sends_g, recvs_g, u * (reps - 1) + k - 1)
            outs[a][:, :, start : start + width] = mid[u][...].astype(F32)
    for u, (a, start, width) in enumerate(units):
        cols = pl.ds(start, width)
        if kind_of[u] != DEPTH:
            left(ins[a].at[:, :, 1 - core, :, :, cols], sends_c, recvs_c, u)
        if kind_of[u] != REST:
            left(own[u].at[:, 1 - low], sends_z, recvs_z, 2 * u)
            left(own[u].at[1 - high, low], sends_z, recvs_z, 2 * u + 1)
        for k in range(1, reps):
            index = u * (reps - 1) + k - 1
            if kind_of[u] != DEPTH:
                left(first[u].at[:, :, (rep + k) % reps], sends_r, recvs_r, index)
            if kind_of[u] != REST:
                left(mid[u].at[rep], sends_g, recvs_g, index)


def split_rows(part):
    reps = lax.axis_size("rep")
    rows, width = part.shape
    return part.reshape(2, 2, 2, reps, rows // (8 * reps), width)


def reduce_many(blocks, pieces, kinds, identity, query=None, grad=None, pairs=None):
    reps = lax.axis_size("rep")
    count = len(blocks)
    units = [
        (at, low, size)
        for at, block in enumerate(blocks)
        for low, size in cut(block.shape[-1], pieces[at])
    ]
    dma = pltpu.SemaphoreType.DMA
    vmem = pl.BlockSpec(memory_space=pltpu.VMEM)

    def buffers(without, *lead):
        shapes = []
        for at, _, size in units:
            tile = (blocks[at].shape[-2], size)
            if kinds[at] == without:
                shapes.append(pltpu.VMEM((8, 128), BF16))
            else:
                shapes.append(pltpu.VMEM(lead + tile, blocks[at].dtype))
        return shapes

    total = len(units)
    out_shape = [
        jax.ShapeDtypeStruct((2, 2) + block.shape[4:], block.dtype)
        if kind == REST
        else jax.ShapeDtypeStruct((reps,) + block.shape[-2:], F32)
        for block, kind in zip(blocks, kinds)
    ]
    operands = list(blocks)
    in_specs = [vmem] * count
    more = []
    if pairs is not None:
        tokens, width = query.shape
        number = width // PAIR
        block = (tokens, 2 * PAIR)
        operands += [query, grad, pairs]
        in_specs += [vmem] * 2 + [pl.BlockSpec(memory_space=pl.ANY)]
        out_shape += [jax.ShapeDtypeStruct((tokens, width), BF16)] * 3
        more = [
            pltpu.VMEM((number, 2, 2, 2) + block, BF16),
            pltpu.VMEM((number, 2, 2) + block, BF16),
            pltpu.VMEM((number, 2) + block, BF16),
            pltpu.VMEM((number,) + block, BF16),
            pltpu.VMEM((2,) + pairs.shape[1:], BF16),
            dma((3 * number,)),
            dma((3 * number,)),
            dma((2,)),
        ]
    sums = pl.pallas_call(
        functools.partial(reduce_kernel, units, tuple(kinds), reps, pairs is not None),
        out_shape=out_shape,
        in_specs=in_specs,
        out_specs=[vmem] * len(out_shape),
        scratch_shapes=buffers(DEPTH, 2, 2, reps)
        + buffers(DEPTH, reps - 1, 2, 2)
        + buffers(REST, 2)
        + buffers(REST)
        + buffers(REST, 2, 2)
        + buffers(REST, reps)
        + [dma((total,))] * 2
        + [dma((total * (reps - 1),))] * 2
        + [dma((total * 2,))] * 2
        + [dma((total * (reps - 1),))] * 2
        + more,
        compiler_params=pltpu.CompilerParams(
            collective_id=identity, has_side_effects=True, vmem_limit_bytes=60 * 1024 * 1024
        ),
    )(*operands)
    totals = [
        total if kind == REST else total.reshape(-1, total.shape[2])
        for total, kind in zip(sums, kinds)
    ]
    return totals + list(sums[count:])


def blocked(shard):
    return shard.reshape(lax.axis_size("rep"), -1, shard.shape[1])


def divides(rows):
    reps = lax.axis_size("rep")
    return lax.axis_size("cp") == 8 and reps == 4 and rows % (8 * reps) == 0


def on_device(
    tokens,
    query_weight,
    query_bias,
    key_weight,
    value_weight,
    value_bias,
    output_weight,
    output_bias,
    first_gain,
    first_shift,
    up_weight,
    up_bias,
    down_weight,
    down_bias,
    second_gain,
    second_shift,
    cotangent,
):
    row_count = tokens.shape[1]
    width = tokens.shape[2]
    local_tokens = tokens[0]
    fast = divides(query_weight.shape[0])
    reps = lax.axis_size("rep")
    small = (
        query_bias,
        value_bias,
        output_bias,
        first_gain,
        first_shift,
        up_bias,
        down_bias,
        second_gain,
        second_shift,
    )
    if fast:
        rows = []
        for vector in small:
            lines = -(-vector.shape[0] // 128)
            rows.append(
                jnp.pad(vector.astype(F32), (0, 128 * lines - vector.shape[0])).reshape(lines, 128)
            )
        packed = jnp.concatenate(rows, axis=0)
        packed = jnp.pad(packed, ((0, -packed.shape[0] % (8 * reps)), (0, 0))).astype(BF16)
        shards = (key_weight, value_weight, query_weight, packed)
        shards += (output_weight, up_weight, down_weight)
        w_key, w_value, w_query, gathered, *begun = gather_many(
            [blocked(shard) for shard in shards],
            (1, 1, 1, 1, 1, 2, 2),
            (FULL,) * 4 + (DEPTH,) * 3,
            1,
        )
        w_key, w_value, w_query = [w.reshape(-1, width) for w in (w_key, w_value, w_query)]
        gathered = gathered.reshape(-1, packed.shape[0], 128)
    else:
        w_query, w_key, w_value = [
            gather_all(shard) for shard in (query_weight, key_weight, value_weight)
        ]
        gathered = lax.all_gather(jnp.concatenate(small)[None], "cp", axis=0, tiled=True)
    vectors = []
    at = 0
    for vector in small:
        size = vector.shape[0]
        if fast:
            lines = -(-size // 128)
            part = gathered[:, at : at + lines].reshape(-1, 128 * lines)[:, :size]
            at += lines
        else:
            part = gathered[:, at : at + size]
            at += size
        vectors.append(part.reshape(-1).astype(F32))
    b_query, b_value, b_output, gain_one, shift_one, b_up, b_down, gain_two, shift_two = vectors
    key_rows = matmul(local_tokens, w_key).astype(BF16)
    value_rows = (matmul(local_tokens, w_value) + b_value).astype(BF16)
    chunk = width // CHUNKS
    query_rows = (matmul(local_tokens, w_query) + b_query).astype(BF16)
    query_scaled = query_rows * jnp.asarray(1.0 / math.sqrt(HD), BF16)
    if fast:
        w_output, w_up, w_down, context_low, pairs = gather_many(
            begun,
            (1, 2, 2),
            (REST,) * 3,
            2,
            query_scaled,
            key_rows,
            value_rows,
        )
        w_output, w_down = w_output.reshape(-1, width), w_down.reshape(-1, width)
        w_up = w_up.reshape(-1, up_weight.shape[1])
        pairs = pairs.reshape(pairs.shape[0], -1, 2 * PAIR)
    else:
        w_output, w_up, w_down = [
            gather_all(shard) for shard in (output_weight, up_weight, down_weight)
        ]
        pair_rows = mixed(key_rows, value_rows)
        queries = [query_scaled[:, chunk * i : chunk * (i + 1)] for i in range(CHUNKS)]
        pairs = [
            lax.all_gather(
                pair_rows[:, 2 * chunk * i : 2 * chunk * (i + 1)], "cp", axis=0, tiled=True
            )
            for i in range(CHUNKS)
        ]
        context_low = jnp.concatenate(
            [attend(query, pair) for query, pair in zip(queries, pairs)], axis=1
        )
    attn_out = matmul(context_low, w_output) + b_output
    resid_first = local_tokens.astype(F32) + attn_out
    first_norm, pull_first = jax.vjp(normalize, resid_first, gain_one, shift_one)
    first_low = first_norm.astype(BF16)
    inner_act = matmul(first_low, w_up) + b_up
    hidden, pull_gelu = jax.vjp(gelu_exact, inner_act)
    hidden_low = hidden.astype(BF16)
    resid_second = first_norm + (matmul(hidden_low, w_down) + b_down)
    layer_out, pull_second = jax.vjp(normalize, resid_second, gain_two, shift_two)

    grad_resid2, grad_gain2, grad_shift2 = pull_second(cotangent[0])
    grad_outer = grad_resid2.astype(BF16)
    grad_down_bias = column_sum(grad_outer)
    part_down = over_rows(hidden_low, grad_outer).astype(BF16)
    grad_inner = pull_gelu(against(grad_outer, w_down))[0].astype(BF16)
    grad_up_bias = column_sum(grad_inner)
    part_up = over_rows(first_low, grad_inner).astype(BF16)
    grad_first = grad_resid2 + against(grad_inner, w_up)
    grad_resid1, grad_gain1, grad_shift1 = pull_first(grad_first)
    grad_attn = grad_resid1.astype(BF16)
    grad_output_bias = column_sum(grad_attn)
    part_output = over_rows(context_low, grad_attn).astype(BF16)
    grad_context = against(grad_attn, w_output).astype(BF16)

    if fast:
        (
            *begun,
            grad_query_low,
            grad_key_low,
            grad_value_low,
        ) = reduce_many(
            [split_rows(part) for part in (part_down, part_up, part_output)],
            (2, 2, 1),
            (REST,) * 3,
            3,
            query_scaled,
            grad_context,
            pairs,
        )
    else:
        grad_queries = []
        grad_pairs = []
        for i in range(CHUNKS):
            grad_query, grad_terms = attend_back(
                queries[i], grad_context[:, chunk * i : chunk * (i + 1)], pairs[i]
            )
            grad_queries.append(grad_query)
            grad_pairs.append(
                lax.psum_scatter(grad_terms, "cp", scatter_dimension=0, tiled=True)
            )
        grad_query_low = jnp.concatenate(grad_queries, axis=1)
        grad_key_low, grad_value_low = unmixed(jnp.concatenate(grad_pairs, axis=1))
    part_query = over_rows(local_tokens, grad_query_low).astype(BF16)
    part_key = over_rows(local_tokens, grad_key_low).astype(BF16)
    part_value = over_rows(local_tokens, grad_value_low).astype(BF16)
    grad_tokens = (
        grad_resid1
        + against(grad_query_low, w_query)
        + against(grad_key_low, w_key)
        + against(grad_value_low, w_value)
    )

    small_grads = (
        column_sum(grad_query_low),
        column_sum(grad_value_low),
        grad_output_bias,
        grad_gain1,
        grad_shift1,
        grad_up_bias,
        grad_down_bias,
        grad_gain2,
        grad_shift2,
    )
    owners = lax.axis_size("cp")
    total_sq = jnp.broadcast_to(jnp.sum(grad_tokens * grad_tokens), (owners, 1))
    flat = jnp.concatenate(
        [vector.reshape(owners, -1) for vector in small_grads] + [total_sq], axis=1
    )
    if fast:
        flat = jnp.pad(flat, ((0, 0), (0, -flat.shape[1] % (8 * 128 * reps))))
        blocks = [split_rows(part) for part in (part_query, part_key, part_value)]
        full_query, full_key, full_value, sums, full_down, full_up, full_output = reduce_many(
            blocks + [flat.reshape(2, 2, 2, reps, -1, 128)] + begun,
            (1,) * 7,
            (FULL,) * 4 + (DEPTH,) * 3,
            4,
        )
        sums = sums.reshape(-1)
    else:
        parts = (part_down, part_up, part_output, part_query, part_key, part_value)
        shards = [scatter_all(part) for part in parts]
        full_down, full_up, full_output, full_query, full_key, full_value = [
            part.astype(F32) for part in lax.psum(tuple(shards), "rep")
        ]
        sums = lax.psum(flat, ("rep", "cp"))
        sums = lax.dynamic_slice_in_dim(sums, lax.axis_index("cp"), 1, 0)[0]
    reduced = []
    at = 0
    for shard in small:
        reduced.append(sums[at : at + shard.shape[0]])
        at += shard.shape[0]
    entries = lax.axis_size("rep") * owners * row_count * width
    rms_values = jnp.sqrt(sums[at : at + 1] / entries)

    return (
        layer_out[None],
        grad_tokens[None],
        full_query,
        reduced[0],
        full_key,
        full_value,
        reduced[1],
        full_output,
        reduced[2],
        reduced[3],
        reduced[4],
        full_up,
        reduced[5],
        full_down,
        reduced[6],
        reduced[7],
        reduced[8],
        rms_values,
    )


def solution(mesh):
    rows = P("cp", None)
    vector = P("cp")
    whole = P("rep", "cp", None)
    params = (
        rows,
        vector,
        rows,
        rows,
        vector,
        rows,
        vector,
        vector,
        vector,
        rows,
        vector,
        rows,
        vector,
        vector,
        vector,
    )
    return jax.shard_map(
        on_device,
        mesh=mesh,
        in_specs=(whole,) + params + (whole,),
        out_specs=(whole, whole) + params + (P(),),
        check_vma=False,
    )
```

```python
import functools
import math

import jax
import jax.numpy as jnp
from jax import lax
from jax.experimental import pallas as pl
from jax.experimental.pallas import tpu as pltpu
from jax.sharding import PartitionSpec as P

HD = 64
PAIR = 2 * HD
CHUNKS = 3
AHEAD = 2
FULL, DEPTH, REST = range(3)
EPSILON = 1e-12
BF16 = jnp.bfloat16
F32 = jnp.float32
MESH = pl.DeviceIdType.MESH


def normalize(values, norm_gain, norm_shift):
    center = values - jnp.mean(values, axis=-1, keepdims=True)
    spread = jnp.mean(center * center, axis=-1, keepdims=True)
    return center * lax.rsqrt(spread + EPSILON) * norm_gain + norm_shift


def gelu_exact(values):
    return 0.5 * values * (1.0 + lax.erf(values * (1.0 / math.sqrt(2.0))))


def matmul(left, right):
    return jnp.dot(left, right, preferred_element_type=F32)


def over_rows(left, right):
    return lax.dot_general(left, right, (((0,), (0,)), ((), ())), preferred_element_type=F32)


def against(left, right):
    return lax.dot_general(left, right, (((1,), (1,)), ((), ())), preferred_element_type=F32)


def column_sum(values):
    return jnp.sum(values.astype(F32), axis=0)


def head_mask(shape, head):
    lane = lax.broadcasted_iota(jnp.int32, shape, 1)
    return (lane >= head * HD) & (lane < (head + 1) * HD)


def pair_context(query, keys, values):
    total = None
    for head in range(2):
        mask = head_mask(query.shape, head)
        scores = against(jnp.where(mask, query, jnp.zeros_like(query)), keys)
        top = jnp.max(scores, axis=-1, keepdims=True)
        weight = jnp.exp(scores - top)
        inverse = 1.0 / jnp.sum(weight, axis=-1, keepdims=True)
        part = matmul((weight * inverse).astype(BF16), values)
        total = part if head == 0 else jnp.where(mask, part, total)
    return total.astype(BF16)


def forward_kernel(query_ref, pair_ref, context_ref):
    context_ref[...] = pair_context(query_ref[...], pair_ref[:, :PAIR], pair_ref[:, PAIR:])


def pair_grads(query, grad, keys, values):
    zeros = jnp.zeros_like(query)
    key_part = value_part = query_part = None
    for head in range(2):
        mask = head_mask(query.shape, head)
        own_query = jnp.where(mask, query, zeros)
        own_grad = jnp.where(mask, grad, zeros)
        scores = against(keys, own_query)
        top = jnp.max(scores, axis=0, keepdims=True)
        weight = jnp.exp(scores - top)
        inverse = 1.0 / jnp.sum(weight, axis=0, keepdims=True)
        probs = weight * inverse
        grad_probs = against(values, own_grad)
        delta = jnp.sum(probs * grad_probs, axis=0, keepdims=True)
        grad_scores = (probs * (grad_probs - delta)).astype(BF16)
        new_value = matmul(probs.astype(BF16), own_grad)
        new_key = matmul(grad_scores, own_query)
        new_query = over_rows(keys, grad_scores)
        if head == 0:
            key_part, value_part, query_part = new_key, new_value, new_query
        else:
            key_part = key_part + new_key
            value_part = value_part + new_value
            row = lax.broadcasted_iota(jnp.int32, new_query.shape, 0)
            query_part = jnp.where(row < HD, query_part, new_query)
    query_part = (query_part.T * (1.0 / math.sqrt(HD))).astype(BF16)
    return query_part, key_part.astype(BF16), value_part.astype(BF16)


def backward_kernel(query_ref, grad_ref, pair_ref, grad_query_ref, grad_pair_ref):
    grad_query_ref[...], grad_pair_ref[:, :PAIR], grad_pair_ref[:, PAIR:] = pair_grads(
        query_ref[...], grad_ref[...], pair_ref[:, :PAIR], pair_ref[:, PAIR:]
    )


def column_block(rows, width):
    return pl.BlockSpec((rows, width), lambda i: (0, i))


def attend(query, pairs):
    rows, width = query.shape
    keys = pairs.shape[0]
    return pl.pallas_call(
        forward_kernel,
        grid=(width // PAIR,),
        in_specs=[column_block(rows, PAIR), column_block(keys, 2 * PAIR)],
        out_specs=column_block(rows, PAIR),
        out_shape=jax.ShapeDtypeStruct((rows, width), BF16),
    )(query, pairs)


def attend_back(query, grad, pairs):
    rows, width = query.shape
    keys = pairs.shape[0]
    return pl.pallas_call(
        backward_kernel,
        grid=(width // PAIR,),
        in_specs=[
            column_block(rows, PAIR),
            column_block(rows, PAIR),
            column_block(keys, 2 * PAIR),
        ],
        out_specs=(column_block(rows, PAIR), column_block(keys, 2 * PAIR)),
        out_shape=(
            jax.ShapeDtypeStruct((rows, width), BF16),
            jax.ShapeDtypeStruct((keys, 2 * width), BF16),
        ),
    )(query, grad, pairs)


def mixed(left, right):
    parts = []
    for low in range(0, left.shape[1], PAIR):
        parts += [left[:, low : low + PAIR], right[:, low : low + PAIR]]
    return jnp.concatenate(parts, axis=1)


def unmixed(both):
    starts = range(0, both.shape[1], 2 * PAIR)
    return (
        jnp.concatenate([both[:, low : low + PAIR] for low in starts], axis=1),
        jnp.concatenate([both[:, low + PAIR : low + 2 * PAIR] for low in starts], axis=1),
    )


def gather_all(shard):
    return lax.all_gather(shard, "cp", axis=0, tiled=True)


def scatter_all(values):
    return lax.psum_scatter(values.astype(BF16), "cp", scatter_dimension=0, tiled=True)


def places():
    rep = lax.axis_index("rep")
    cp = lax.axis_index("cp")
    return rep, cp // 4, (cp // 2) % 2, cp % 2


def place_of(high, low, core):
    return 4 * high + 2 * low + core


def enter(reps):
    rep, high, low, core = places()
    barrier = pltpu.get_barrier_semaphore()
    peers = [
        (rep, place_of(high, low, 1 - core)),
        (rep, place_of(high, 1 - low, core)),
        (rep, place_of(1 - high, low, core)),
    ]
    peers += [((rep + k) % reps, place_of(high, low, core)) for k in range(1, reps)]
    for peer in peers:
        pl.semaphore_signal(barrier, inc=1, device_id=peer, device_id_type=MESH)
    pl.semaphore_wait(barrier, len(peers))


def remote(src, dst, sends, recvs, at, peer):
    return pltpu.make_async_remote_copy(
        src_ref=src,
        dst_ref=dst,
        send_sem=sends.at[at],
        recv_sem=recvs.at[at],
        device_id=peer,
        device_id_type=MESH,
    )


def gather_kernel(units, kinds, reps, pairs, *refs):
    count = len(kinds)
    ins = refs[:count]
    at = count
    if pairs:
        query_ref, key_ref, value_ref = refs[at : at + 3]
        at += 3
    outs = refs[at : at + count]
    at += count
    if pairs:
        context_ref, pair_ref = refs[at : at + 2]
        at += 2
    sends_z, recvs_z, sends_r, recvs_r, sends_c, recvs_c, local = refs[at : at + 7]
    rep, high, low, core = places()
    me = (rep, place_of(high, low, core))
    sibling = (rep, place_of(high, low, 1 - core))
    far = (rep, place_of(1 - high, low, core))
    near = (rep, place_of(high, 1 - low, core))
    enter(reps)
    copies = []

    def send(src, dst, sends, recvs, at, peer):
        remote(src, dst, sends, recvs, at, peer).start()

    def left(block, sends, recvs, at):
        remote(block, block, sends, recvs, at, me).wait_send()

    def arrived(block, sends, recvs, at):
        remote(block, block, sends, recvs, at, me).wait_recv()

    origins = (
        (high, low),
        (high, 1 - low),
        (1 - high, low),
        (1 - high, 1 - low),
    )

    def block_of(u, which, side, quarter):
        at, start, size = units[u]
        from_high, from_low = origins[which]
        return outs[at].at[from_high, from_low, side, quarter, :, pl.ds(start, size)]

    def held(p, which, side):
        from_high, from_low = origins[which]
        return pair_ref.at[p, from_high, from_low, side]

    if pairs:
        sends_k, recvs_k, sends_s, recvs_s = refs[at + 7 :]

    def offer(p):
        own = held(p, 0, core)
        send(own, own, sends_k, recvs_k, 3 * p + 1, far)
        send(own, own, sends_k, recvs_k, 3 * p, near)
        send(own, own, sends_s, recvs_s, 4 * p, sibling)

    total = len(units)
    kind_of = [kinds[at] for at, _, _ in units]

    def begin(u):
        at, start, size = units[u]
        block = ins[at].at[rep, :, pl.ds(start, size)]
        send(block, block_of(u, 0, core, rep), sends_z, recvs_z, 3 * u + 1, far)
        send(block, block_of(u, 0, core, rep), sends_z, recvs_z, 3 * u, near)

    def own_whole(u):
        at, start, size = units[u]
        if kind_of[u] == REST:
            return block_of(u, 0, core, slice(None))
        return ins[at].at[:, :, pl.ds(start, size)]

    for u in range(total):
        if kind_of[u] == FULL:
            begin(u)
    for u in range(total):
        if kind_of[u] != DEPTH:
            send(
                own_whole(u), block_of(u, 0, core, slice(None)), sends_c, recvs_c, 4 * u, sibling
            )
    for at in range(count):
        if kinds[at] != REST:
            copy = pltpu.make_async_copy(ins[at], outs[at].at[high, low, core], local.at[at])
            copy.start()
            copies.append(copy)

    for p in range(pairs):
        cols = pl.ds(PAIR * p, PAIR)
        pair_ref[p, high, low, core, :, :PAIR] = key_ref[:, cols]
        pair_ref[p, high, low, core, :, PAIR:] = value_ref[:, cols]
        if p < AHEAD:
            offer(p)

    def spread(u, which):
        block = block_of(u, which, core, rep)
        if kind_of[u] != REST:
            arrived(block, sends_z, recvs_z, 3 * u + which - 1)
            if which == 2:
                send(block, block, sends_z, recvs_z, 3 * u + 2, near)
        if kind_of[u] == DEPTH:
            return
        for j in range(1, reps):
            index = (3 * u + which - 1) * (reps - 1) + j - 1
            peer = ((rep + j) % reps, me[1])
            send(block, block, sends_r, recvs_r, index, peer)

    def pass_on(u, which):
        if kind_of[u] == DEPTH:
            return
        for j in range(1, reps):
            index = (3 * u + which - 1) * (reps - 1) + j - 1
            block = block_of(u, which, core, (rep + reps - j) % reps)
            arrived(block, sends_r, recvs_r, index)
        whole = block_of(u, which, core, slice(None))
        send(whole, whole, sends_c, recvs_c, 4 * u + which, sibling)

    lead = kind_of.count(FULL)

    def advance(step):
        if step < total:
            spread(step, 1)
            spread(step, 2)
            if step < lead:
                for u in range(lead, total):
                    if (u - lead) * lead // (total - lead) == step:
                        begin(u)
        if 1 <= step < total + 1:
            spread(step - 1, 3)
        if 2 <= step:
            for which in range(1, 4):
                pass_on(step - 2, which)

    def take(p, which):
        block = held(p, which, core)
        arrived(block, sends_k, recvs_k, 3 * p + which - 1)
        if which == 2:
            send(block, block, sends_k, recvs_k, 3 * p + 2, near)
        send(block, block, sends_s, recvs_s, 4 * p + which, sibling)

    def compute(p):
        for which in range(4):
            arrived(held(p, which, 1 - core), sends_s, recvs_s, 4 * p + which)
        cols = pl.ds(pl.multiple_of(p * PAIR, PAIR), PAIR)
        shape = (-1, PAIR)
        context_ref[:, cols] = pair_context(
            query_ref[:, cols],
            pair_ref[p, :, :, :, :, :PAIR].reshape(shape),
            pair_ref[p, :, :, :, :, PAIR:].reshape(shape),
        )

    steps = total + 2
    if pairs:
        for u in range(total):
            for which in range(1, 4):
                spread(u, which)

    def finish(step):
        if 0 < step <= total:
            for which in range(1, 4):
                pass_on(step - 1, which)

    if not pairs:
        for step in range(steps):
            advance(step)
    else:

        def step_all(t, carry):
            @pl.when(t < pairs)
            def _():
                take(t, 1)
                take(t, 2)

            @pl.when(t < pairs - AHEAD)
            def _():
                offer(t + AHEAD)

            @pl.when((t >= 1) & (t < pairs + 1))
            def _():
                take(t - 1, 3)

            for i in range(steps):

                @pl.when(t == i)
                def _(i=i):
                    finish(i)

            @pl.when((t >= 2) & (t < pairs + 2))
            def _():
                compute(t - 2)

            return carry

        lax.fori_loop(0, max(pairs + 2, steps), step_all, 0)
    for u in range(total):
        if kind_of[u] != DEPTH:
            for which in range(4):
                block = block_of(u, which, 1 - core, slice(None))
                arrived(block, sends_c, recvs_c, 4 * u + which)
    for copy in copies:
        copy.wait()
    for u, (at, start, size) in enumerate(units):
        if kind_of[u] != REST:
            block = ins[at].at[rep, :, pl.ds(start, size)]
            left(block, sends_z, recvs_z, 3 * u)
            left(block, sends_z, recvs_z, 3 * u + 1)
            left(block_of(u, 2, core, rep), sends_z, recvs_z, 3 * u + 2)
        if kind_of[u] != DEPTH:
            left(own_whole(u), sends_c, recvs_c, 4 * u)
            for which in range(1, 4):
                left(block_of(u, which, core, slice(None)), sends_c, recvs_c, 4 * u + which)
                for j in range(1, reps):
                    index = (3 * u + which - 1) * (reps - 1) + j - 1
                    left(block_of(u, which, core, rep), sends_r, recvs_r, index)
    for p in range(pairs):
        for at, which in enumerate((0, 0, 2)):
            left(held(p, which, core), sends_k, recvs_k, 3 * p + at)
        for which in range(4):
            left(held(p, which, core), sends_s, recvs_s, 4 * p + which)


def cut(width, pieces):
    size = width // pieces
    if size % 128:
        return [(0, width)]
    return [(size * i, size) for i in range(pieces)]


def gather_many(shards, pieces, kinds, identity, query=None, keys=None, values=None):
    reps = lax.axis_size("rep")
    count = len(shards)
    units = [
        (at, low, size)
        for at, shard in enumerate(shards)
        for low, size in cut(shard.shape[-1], pieces[at])
    ]
    total = len(units)
    hops = 3 * total * (reps - 1)
    dma = pltpu.SemaphoreType.DMA
    vmem = pl.BlockSpec(memory_space=pltpu.VMEM)
    out_shape = [
        jax.ShapeDtypeStruct(
            shard.shape if kind == REST else (2, 2, 2) + shard.shape, shard.dtype
        )
        for shard, kind in zip(shards, kinds)
    ]
    operands = list(shards)
    spaces = []
    more = []
    pairs = 0
    if query is not None:
        pairs = query.shape[1] // PAIR
        operands += [query, keys, values]
        spaces = [vmem] * 3
        out_shape += [
            jax.ShapeDtypeStruct(query.shape, BF16),
            jax.ShapeDtypeStruct((pairs, 2, 2, 2, keys.shape[0], 2 * PAIR), BF16),
        ]
        more = [dma((3 * pairs,))] * 2 + [dma((4 * pairs,))] * 2
    return pl.pallas_call(
        functools.partial(gather_kernel, units, tuple(kinds), reps, pairs),
        input_output_aliases={at: at for at in range(count) if kinds[at] == REST},
        out_shape=out_shape,
        in_specs=[
            pl.BlockSpec(memory_space=pl.ANY if kind == REST else pltpu.VMEM) for kind in kinds
        ]
        + spaces,
        out_specs=[pl.BlockSpec(memory_space=pl.ANY)] * count + spaces[:2],
        scratch_shapes=[dma((3 * total,))] * 2
        + [dma((hops,))] * 2
        + [dma((4 * total,))] * 2
        + [dma((count,))]
        + more,
        compiler_params=pltpu.CompilerParams(
            collective_id=identity, has_side_effects=True, vmem_limit_bytes=60 * 1024 * 1024
        ),
    )(*operands)


def summed(parts, kind):
    total = parts[0].astype(F32)
    for part in parts[1:]:
        total = total + part.astype(F32)
    return total.astype(kind)


def reduce_kernel(units, kinds, reps, fused, *refs):
    count = len(kinds)
    ins = refs[:count]
    at = count
    if fused:
        query_ref, grad_ref, pair_ref = refs[at : at + 3]
        at += 3
    outs = refs[at : at + count]
    at += count
    if fused:
        grad_query_ref, grad_key_ref, grad_value_ref = refs[at : at + 3]
        at += 3
    size = len(units)
    first, second, third, fourth, own, mid, final = [
        refs[at + i * size : at + (i + 1) * size] for i in range(7)
    ]
    written = refs[at + 7 * size]
    sems = refs[at + 7 * size + 1 :]

    def write(u):
        a, start, width = units[u]
        block = outs[a].at[:, :, pl.ds(start, width)]
        return pltpu.make_async_copy(final[u], block, written.at[u])

    kind_of = [kinds[a] for a, _, _ in units]
    sends_c, recvs_c, sends_r, recvs_r, sends_z, recvs_z, sends_g, recvs_g = sems[:8]
    rep, high, low, core = places()
    me = (rep, place_of(high, low, core))
    sibling = (rep, place_of(high, low, 1 - core))
    far = (rep, place_of(1 - high, low, core))
    near = (rep, place_of(high, 1 - low, core))
    enter(reps)
    def send(src, dst, sends, recvs, at, peer):
        remote(src, dst, sends, recvs, at, peer).start()

    def left(block, sends, recvs, at):
        remote(block, block, sends, recvs, at, me).wait_send()

    def arrived(block, sends, recvs, at):
        remote(block, block, sends, recvs, at, me).wait_recv()

    for u, (a, start, width) in enumerate(units):
        if kind_of[u] == DEPTH:
            own[u][...] = ins[a][:, :, :, start : start + width]
            send(own[u].at[:, 1 - low], third[u], sends_z, recvs_z, 2 * u, near)
            continue
        block = ins[a].at[:, :, 1 - core, :, :, pl.ds(start, width)]
        send(block, first[u], sends_c, recvs_c, u, sibling)

    def over_core(u):
        a, start, width = units[u]
        if kind_of[u] == DEPTH:
            return
        arrived(first[u], sends_c, recvs_c, u)

        def step(i, carry):
            h, w, q = i // (2 * reps), (i // reps) % 2, i % reps
            mine = ins[a][h, w, core, q, :, start : start + width]
            first[u][h, w, q] = summed([first[u][h, w, q], mine], first[u].dtype)
            return carry

        lax.fori_loop(0, 4 * reps, step, 0)
        for k in range(1, reps):
            target = (rep + k) % reps
            send(
                first[u].at[:, :, target],
                second[u].at[k - 1],
                sends_r,
                recvs_r,
                u * (reps - 1) + k - 1,
                (target, me[1]),
            )

    def over_rep(u):
        a, start, width = units[u]
        if kind_of[u] == DEPTH:
            return
        for k in range(1, reps):
            arrived(second[u].at[k - 1], sends_r, recvs_r, u * (reps - 1) + k - 1)

        def step(i, carry):
            h, w = i // 2, i % 2
            parts = [first[u][h, w, rep]] + [second[u][k, h, w] for k in range(reps - 1)]
            total = summed(parts, first[u].dtype)
            if kind_of[u] == REST:
                outs[a][h, w, :, start : start + width] = total
            else:
                own[u][h, w] = total
            return carry

        lax.fori_loop(0, 4, step, 0)
        if kind_of[u] == FULL:
            send(own[u].at[:, 1 - low], third[u], sends_z, recvs_z, 2 * u, near)

    def over_near(u):
        if kind_of[u] == REST:
            return
        arrived(third[u], sends_z, recvs_z, 2 * u)
        for h in range(2):
            own[u][h, low] = summed([own[u][h, low], third[u][h]], own[u].dtype)
        send(own[u].at[1 - high, low], fourth[u], sends_z, recvs_z, 2 * u + 1, far)

    def over_far(u):
        if kind_of[u] == REST:
            return
        arrived(fourth[u], sends_z, recvs_z, 2 * u + 1)
        mid[u][rep] = summed([own[u][high, low], fourth[u][...]], mid[u].dtype)
        block = mid[u].at[rep]
        for k in range(1, reps):
            peer = ((rep + k) % reps, me[1])
            send(block, block, sends_g, recvs_g, u * (reps - 1) + k - 1, peer)

    if not fused:
        whole = [u for u in range(size) if kind_of[u] != DEPTH]
        rest = [u for u in range(size) if kind_of[u] == DEPTH]
        order = [(over_core, whole), (over_near, rest), (over_rep, whole)]
        order += [(over_far, rest), (over_near, whole), (over_far, whole)]
        for stage, members in order:
            for u in members:
                stage(u)
    else:
        terms, merged, from_near, from_far, held, sends_k, recvs_k, fetched = sems[8:]
        pairs = terms.shape[0]

        def advance(step):
            for u in range(size):
                if step == u // 2:
                    over_core(u)
                if step == pairs - 1 + u // 2:
                    over_rep(u)

        steps = pairs + size // 2 + 1

        def fetch(p):
            return pltpu.make_async_copy(pair_ref.at[p], held.at[p % 2], fetched.at[p % 2])

        def hop(p, which):
            if which == 0:
                return remote(
                    terms.at[p, :, :, 1 - core], merged.at[p], sends_k, recvs_k, 3 * p, sibling
                )
            if which == 1:
                return remote(
                    merged.at[p, :, 1 - low], from_near.at[p], sends_k, recvs_k, 3 * p + 1, near
                )
            return remote(
                merged.at[p, 1 - high, low], from_far.at[p], sends_k, recvs_k, 3 * p + 2, far
            )

        def merge_core(p):
            arrived(merged.at[p], sends_k, recvs_k, 3 * p)
            for h in range(2):
                for w in range(2):
                    both = [merged[p, h, w], terms[p, h, w, core]]
                    merged[p, h, w] = summed(both, BF16)
            hop(p, 1).start()

        def merge_near(p):
            arrived(from_near.at[p], sends_k, recvs_k, 3 * p + 1)
            for h in range(2):
                merged[p, h, low] = summed([merged[p, h, low], from_near[p, h]], BF16)
            hop(p, 2).start()

        def merge_far(p):
            arrived(from_far.at[p], sends_k, recvs_k, 3 * p + 2)
            cols = pl.ds(pl.multiple_of(p * PAIR, PAIR), PAIR)
            both = summed([merged[p, high, low], from_far[p]], BF16)
            grad_key_ref[:, cols] = both[:, :PAIR]
            grad_value_ref[:, cols] = both[:, PAIR:]

        def compute(p):
            fetch(p).wait()

            @pl.when(p < pairs - 1)
            def _():
                fetch(p + 1).start()

            cols = pl.ds(pl.multiple_of(p * PAIR, PAIR), PAIR)
            slot = p % 2
            query_part, key_part, value_part = pair_grads(
                query_ref[:, cols], grad_ref[:, cols], held[slot, :, :PAIR], held[slot, :, PAIR:]
            )
            grad_query_ref[:, cols] = query_part
            shape = terms.shape[1:5] + (PAIR,)
            terms[p, :, :, :, :, :PAIR] = key_part.reshape(shape)
            terms[p, :, :, :, :, PAIR:] = value_part.reshape(shape)
            hop(p, 0).start()

        fetch(0).start()

        def step_all(t, carry):
            for lag, merge in ((1, merge_core), (2, merge_near), (3, merge_far)):

                @pl.when((t >= lag) & (t < pairs + lag))
                def _(lag=lag, merge=merge):
                    merge(t - lag)

            @pl.when(t < pairs)
            def _():
                compute(t)

            for i in range(steps):

                @pl.when(t == i)
                def _(i=i):
                    advance(i)

            return carry

        lax.fori_loop(0, max(pairs + 3, steps), step_all, 0)
        for p in range(pairs):
            for which in range(3):
                hop(p, which).wait_send()
    for u, (a, start, width) in enumerate(units):
        if kind_of[u] != REST:
            for k in range(1, reps):
                block = mid[u].at[(rep + reps - k) % reps]
                arrived(block, sends_g, recvs_g, u * (reps - 1) + k - 1)
            final[u][...] = mid[u][...].astype(F32)
            write(u).start()
    for u in range(size):
        if kind_of[u] != REST:
            write(u).wait()
    for u, (a, start, width) in enumerate(units):
        cols = pl.ds(start, width)
        if kind_of[u] != DEPTH:
            left(ins[a].at[:, :, 1 - core, :, :, cols], sends_c, recvs_c, u)
        if kind_of[u] != REST:
            left(own[u].at[:, 1 - low], sends_z, recvs_z, 2 * u)
            left(own[u].at[1 - high, low], sends_z, recvs_z, 2 * u + 1)
        for k in range(1, reps):
            index = u * (reps - 1) + k - 1
            if kind_of[u] != DEPTH:
                left(first[u].at[:, :, (rep + k) % reps], sends_r, recvs_r, index)
            if kind_of[u] != REST:
                left(mid[u].at[rep], sends_g, recvs_g, index)


def split_rows(part):
    reps = lax.axis_size("rep")
    rows, width = part.shape
    return part.reshape(2, 2, 2, reps, rows // (8 * reps), width)


def reduce_many(blocks, pieces, kinds, identity, query=None, grad=None, pairs=None):
    reps = lax.axis_size("rep")
    count = len(blocks)
    units = [
        (at, low, size)
        for at, block in enumerate(blocks)
        for low, size in cut(block.shape[-1], pieces[at])
    ]
    dma = pltpu.SemaphoreType.DMA
    vmem = pl.BlockSpec(memory_space=pltpu.VMEM)

    def buffers(without, *lead, kind=None):
        shapes = []
        for at, _, size in units:
            tile = (blocks[at].shape[-2], size)
            if kinds[at] == without:
                shapes.append(pltpu.VMEM((8, 128), BF16))
            else:
                shapes.append(pltpu.VMEM(lead + tile, kind or blocks[at].dtype))
        return shapes

    total = len(units)
    out_shape = [
        jax.ShapeDtypeStruct((2, 2) + block.shape[4:], block.dtype)
        if kind == REST
        else jax.ShapeDtypeStruct((reps,) + block.shape[-2:], F32)
        for block, kind in zip(blocks, kinds)
    ]
    operands = list(blocks)
    in_specs = [vmem] * count
    more = []
    if pairs is not None:
        tokens, width = query.shape
        number = width // PAIR
        block = (tokens, 2 * PAIR)
        operands += [query, grad, pairs]
        in_specs += [vmem] * 2 + [pl.BlockSpec(memory_space=pl.ANY)]
        out_shape += [jax.ShapeDtypeStruct((tokens, width), BF16)] * 3
        more = [
            pltpu.VMEM((number, 2, 2, 2) + block, BF16),
            pltpu.VMEM((number, 2, 2) + block, BF16),
            pltpu.VMEM((number, 2) + block, BF16),
            pltpu.VMEM((number,) + block, BF16),
            pltpu.VMEM((2,) + pairs.shape[1:], BF16),
            dma((3 * number,)),
            dma((3 * number,)),
            dma((2,)),
        ]
    sums = pl.pallas_call(
        functools.partial(reduce_kernel, units, tuple(kinds), reps, pairs is not None),
        out_shape=out_shape,
        in_specs=in_specs,
        out_specs=[
            vmem if kind == REST else pl.BlockSpec(memory_space=pltpu.HBM) for kind in kinds
        ]
        + [vmem] * (len(out_shape) - count),
        scratch_shapes=buffers(DEPTH, 2, 2, reps)
        + buffers(DEPTH, reps - 1, 2, 2)
        + buffers(REST, 2)
        + buffers(REST)
        + buffers(REST, 2, 2)
        + buffers(REST, reps)
        + buffers(REST, reps, kind=F32)
        + [dma((total,))]
        + [dma((total,))] * 2
        + [dma((total * (reps - 1),))] * 2
        + [dma((total * 2,))] * 2
        + [dma((total * (reps - 1),))] * 2
        + more,
        compiler_params=pltpu.CompilerParams(
            collective_id=identity, has_side_effects=True, vmem_limit_bytes=60 * 1024 * 1024
        ),
    )(*operands)
    totals = [
        total if kind == REST else total.reshape(-1, total.shape[2])
        for total, kind in zip(sums, kinds)
    ]
    return totals + list(sums[count:])


def blocked(shard):
    return shard.reshape(lax.axis_size("rep"), -1, shard.shape[1])


def divides(rows):
    reps = lax.axis_size("rep")
    return lax.axis_size("cp") == 8 and reps == 4 and rows % (8 * reps) == 0


def on_device(
    tokens,
    query_weight,
    query_bias,
    key_weight,
    value_weight,
    value_bias,
    output_weight,
    output_bias,
    first_gain,
    first_shift,
    up_weight,
    up_bias,
    down_weight,
    down_bias,
    second_gain,
    second_shift,
    cotangent,
):
    row_count = tokens.shape[1]
    width = tokens.shape[2]
    local_tokens = tokens[0]
    fast = divides(query_weight.shape[0])
    reps = lax.axis_size("rep")
    small = (
        query_bias,
        value_bias,
        output_bias,
        first_gain,
        first_shift,
        up_bias,
        down_bias,
        second_gain,
        second_shift,
    )
    if fast:
        rows = []
        for vector in small:
            lines = -(-vector.shape[0] // 128)
            rows.append(
                jnp.pad(vector.astype(F32), (0, 128 * lines - vector.shape[0])).reshape(lines, 128)
            )
        packed = jnp.concatenate(rows, axis=0)
        packed = jnp.pad(packed, ((0, -packed.shape[0] % (8 * reps)), (0, 0))).astype(BF16)
        shards = (key_weight, value_weight, query_weight, packed)
        shards += (output_weight, up_weight, down_weight)
        w_key, w_value, w_query, gathered, *begun = gather_many(
            [blocked(shard) for shard in shards],
            (1, 1, 1, 1, 1, 2, 2),
            (FULL,) * 4 + (DEPTH,) * 3,
            1,
        )
        w_key, w_value, w_query = [w.reshape(-1, width) for w in (w_key, w_value, w_query)]
        gathered = gathered.reshape(-1, packed.shape[0], 128)
    else:
        w_query, w_key, w_value = [
            gather_all(shard) for shard in (query_weight, key_weight, value_weight)
        ]
        gathered = lax.all_gather(jnp.concatenate(small)[None], "cp", axis=0, tiled=True)
    vectors = []
    at = 0
    for vector in small:
        size = vector.shape[0]
        if fast:
            lines = -(-size // 128)
            part = gathered[:, at : at + lines].reshape(-1, 128 * lines)[:, :size]
            at += lines
        else:
            part = gathered[:, at : at + size]
            at += size
        vectors.append(part.reshape(-1).astype(F32))
    b_query, b_value, b_output, gain_one, shift_one, b_up, b_down, gain_two, shift_two = vectors
    key_rows = matmul(local_tokens, w_key).astype(BF16)
    value_rows = (matmul(local_tokens, w_value) + b_value).astype(BF16)
    chunk = width // CHUNKS
    query_rows = (matmul(local_tokens, w_query) + b_query).astype(BF16)
    query_scaled = query_rows * jnp.asarray(1.0 / math.sqrt(HD), BF16)
    if fast:
        w_output, w_up, w_down, context_low, pairs = gather_many(
            begun,
            (1, 2, 2),
            (REST,) * 3,
            2,
            query_scaled,
            key_rows,
            value_rows,
        )
        w_output, w_down = w_output.reshape(-1, width), w_down.reshape(-1, width)
        w_up = w_up.reshape(-1, up_weight.shape[1])
        pairs = pairs.reshape(pairs.shape[0], -1, 2 * PAIR)
    else:
        w_output, w_up, w_down = [
            gather_all(shard) for shard in (output_weight, up_weight, down_weight)
        ]
        pair_rows = mixed(key_rows, value_rows)
        queries = [query_scaled[:, chunk * i : chunk * (i + 1)] for i in range(CHUNKS)]
        pairs = [
            lax.all_gather(
                pair_rows[:, 2 * chunk * i : 2 * chunk * (i + 1)], "cp", axis=0, tiled=True
            )
            for i in range(CHUNKS)
        ]
        context_low = jnp.concatenate(
            [attend(query, pair) for query, pair in zip(queries, pairs)], axis=1
        )
    attn_out = matmul(context_low, w_output) + b_output
    resid_first = local_tokens.astype(F32) + attn_out
    first_norm, pull_first = jax.vjp(normalize, resid_first, gain_one, shift_one)
    first_low = first_norm.astype(BF16)
    inner_act = matmul(first_low, w_up) + b_up
    hidden, pull_gelu = jax.vjp(gelu_exact, inner_act)
    hidden_low = hidden.astype(BF16)
    resid_second = first_norm + (matmul(hidden_low, w_down) + b_down)
    layer_out, pull_second = jax.vjp(normalize, resid_second, gain_two, shift_two)

    grad_resid2, grad_gain2, grad_shift2 = pull_second(cotangent[0])
    grad_outer = grad_resid2.astype(BF16)
    grad_down_bias = column_sum(grad_outer)
    part_down = over_rows(hidden_low, grad_outer).astype(BF16)
    grad_inner = pull_gelu(against(grad_outer, w_down))[0].astype(BF16)
    grad_up_bias = column_sum(grad_inner)
    part_up = over_rows(first_low, grad_inner).astype(BF16)
    grad_first = grad_resid2 + against(grad_inner, w_up)
    grad_resid1, grad_gain1, grad_shift1 = pull_first(grad_first)
    grad_attn = grad_resid1.astype(BF16)
    grad_output_bias = column_sum(grad_attn)
    part_output = over_rows(context_low, grad_attn).astype(BF16)
    grad_context = against(grad_attn, w_output).astype(BF16)

    if fast:
        (
            *begun,
            grad_query_low,
            grad_key_low,
            grad_value_low,
        ) = reduce_many(
            [split_rows(part) for part in (part_down, part_up, part_output)],
            (2, 2, 1),
            (REST,) * 3,
            3,
            query_scaled,
            grad_context,
            pairs,
        )
    else:
        grad_queries = []
        grad_pairs = []
        for i in range(CHUNKS):
            grad_query, grad_terms = attend_back(
                queries[i], grad_context[:, chunk * i : chunk * (i + 1)], pairs[i]
            )
            grad_queries.append(grad_query)
            grad_pairs.append(
                lax.psum_scatter(grad_terms, "cp", scatter_dimension=0, tiled=True)
            )
        grad_query_low = jnp.concatenate(grad_queries, axis=1)
        grad_key_low, grad_value_low = unmixed(jnp.concatenate(grad_pairs, axis=1))
    part_query = over_rows(local_tokens, grad_query_low).astype(BF16)
    part_key = over_rows(local_tokens, grad_key_low).astype(BF16)
    part_value = over_rows(local_tokens, grad_value_low).astype(BF16)
    grad_tokens = (
        grad_resid1
        + against(grad_query_low, w_query)
        + against(grad_key_low, w_key)
        + against(grad_value_low, w_value)
    )

    small_grads = (
        column_sum(grad_query_low),
        column_sum(grad_value_low),
        grad_output_bias,
        grad_gain1,
        grad_shift1,
        grad_up_bias,
        grad_down_bias,
        grad_gain2,
        grad_shift2,
    )
    owners = lax.axis_size("cp")
    total_sq = jnp.broadcast_to(jnp.sum(grad_tokens * grad_tokens), (owners, 1))
    flat = jnp.concatenate(
        [vector.reshape(owners, -1) for vector in small_grads] + [total_sq], axis=1
    )
    if fast:
        flat = jnp.pad(flat, ((0, 0), (0, -flat.shape[1] % (8 * 128 * reps))))
        blocks = [split_rows(part) for part in (part_query, part_key, part_value)]
        full_query, full_key, full_value, sums, full_down, full_up, full_output = reduce_many(
            blocks + [flat.reshape(2, 2, 2, reps, -1, 128)] + begun,
            (1,) * 7,
            (FULL,) * 4 + (DEPTH,) * 3,
            4,
        )
        sums = sums.reshape(-1)
    else:
        parts = (part_down, part_up, part_output, part_query, part_key, part_value)
        shards = [scatter_all(part) for part in parts]
        full_down, full_up, full_output, full_query, full_key, full_value = [
            part.astype(F32) for part in lax.psum(tuple(shards), "rep")
        ]
        sums = lax.psum(flat, ("rep", "cp"))
        sums = lax.dynamic_slice_in_dim(sums, lax.axis_index("cp"), 1, 0)[0]
    reduced = []
    at = 0
    for shard in small:
        reduced.append(sums[at : at + shard.shape[0]])
        at += shard.shape[0]
    entries = lax.axis_size("rep") * owners * row_count * width
    rms_values = jnp.sqrt(sums[at : at + 1] / entries)

    return (
        layer_out[None],
        grad_tokens[None],
        full_query,
        reduced[0],
        full_key,
        full_value,
        reduced[1],
        full_output,
        reduced[2],
        reduced[3],
        reduced[4],
        full_up,
        reduced[5],
        full_down,
        reduced[6],
        reduced[7],
        reduced[8],
        rms_values,
    )


def solution(mesh):
    rows = P("cp", None)
    vector = P("cp")
    whole = P("rep", "cp", None)
    params = (
        rows,
        vector,
        rows,
        rows,
        vector,
        rows,
        vector,
        vector,
        vector,
        rows,
        vector,
        rows,
        vector,
        vector,
        vector,
    )
    return jax.shard_map(
        on_device,
        mesh=mesh,
        in_specs=(whole,) + params + (whole,),
        out_specs=(whole, whole) + params + (P(),),
        check_vma=False,
    )
```

```python
import functools
import math

import jax
import jax.numpy as jnp
from jax import lax
from jax.experimental import pallas as pl
from jax.experimental.pallas import tpu as pltpu
from jax.sharding import PartitionSpec as P

HD = 64
PAIR = 2 * HD
CHUNKS = 3
AHEAD = 3
FULL, DEPTH, REST = range(3)
EPSILON = 1e-12
BF16 = jnp.bfloat16
F32 = jnp.float32
MESH = pl.DeviceIdType.MESH


def normalize(values, norm_gain, norm_shift):
    center = values - jnp.mean(values, axis=-1, keepdims=True)
    spread = jnp.mean(center * center, axis=-1, keepdims=True)
    return center * lax.rsqrt(spread + EPSILON) * norm_gain + norm_shift


def gelu_exact(values):
    return 0.5 * values * (1.0 + lax.erf(values * (1.0 / math.sqrt(2.0))))


def matmul(left, right):
    return jnp.dot(left, right, preferred_element_type=F32)


def over_rows(left, right):
    return lax.dot_general(left, right, (((0,), (0,)), ((), ())), preferred_element_type=F32)


def against(left, right):
    return lax.dot_general(left, right, (((1,), (1,)), ((), ())), preferred_element_type=F32)


def column_sum(values):
    return jnp.sum(values.astype(F32), axis=0)


def head_mask(shape, head):
    lane = lax.broadcasted_iota(jnp.int32, shape, 1)
    return (lane >= head * HD) & (lane < (head + 1) * HD)


def pair_context(query, keys, values):
    total = None
    for head in range(2):
        mask = head_mask(query.shape, head)
        scores = against(jnp.where(mask, query, jnp.zeros_like(query)), keys)
        top = jnp.max(scores, axis=-1, keepdims=True)
        weight = jnp.exp(scores - top)
        inverse = 1.0 / jnp.sum(weight, axis=-1, keepdims=True)
        part = matmul((weight * inverse).astype(BF16), values)
        total = part if head == 0 else jnp.where(mask, part, total)
    return total.astype(BF16)


def forward_kernel(query_ref, pair_ref, context_ref):
    context_ref[...] = pair_context(query_ref[...], pair_ref[:, :PAIR], pair_ref[:, PAIR:])


def pair_grads(query, grad, keys, values):
    zeros = jnp.zeros_like(query)
    key_part = value_part = query_part = None
    for head in range(2):
        mask = head_mask(query.shape, head)
        own_query = jnp.where(mask, query, zeros)
        own_grad = jnp.where(mask, grad, zeros)
        scores = against(keys, own_query)
        top = jnp.max(scores, axis=0, keepdims=True)
        weight = jnp.exp(scores - top)
        inverse = 1.0 / jnp.sum(weight, axis=0, keepdims=True)
        probs = weight * inverse
        grad_probs = against(values, own_grad)
        delta = jnp.sum(probs * grad_probs, axis=0, keepdims=True)
        grad_scores = (probs * (grad_probs - delta)).astype(BF16)
        new_value = matmul(probs.astype(BF16), own_grad)
        new_key = matmul(grad_scores, own_query)
        new_query = over_rows(keys, grad_scores)
        if head == 0:
            key_part, value_part, query_part = new_key, new_value, new_query
        else:
            key_part = key_part + new_key
            value_part = value_part + new_value
            row = lax.broadcasted_iota(jnp.int32, new_query.shape, 0)
            query_part = jnp.where(row < HD, query_part, new_query)
    query_part = (query_part.T * (1.0 / math.sqrt(HD))).astype(BF16)
    return query_part, key_part.astype(BF16), value_part.astype(BF16)


def backward_kernel(query_ref, grad_ref, pair_ref, grad_query_ref, grad_pair_ref):
    grad_query_ref[...], grad_pair_ref[:, :PAIR], grad_pair_ref[:, PAIR:] = pair_grads(
        query_ref[...], grad_ref[...], pair_ref[:, :PAIR], pair_ref[:, PAIR:]
    )


def column_block(rows, width):
    return pl.BlockSpec((rows, width), lambda i: (0, i))


def attend(query, pairs):
    rows, width = query.shape
    keys = pairs.shape[0]
    return pl.pallas_call(
        forward_kernel,
        grid=(width // PAIR,),
        in_specs=[column_block(rows, PAIR), column_block(keys, 2 * PAIR)],
        out_specs=column_block(rows, PAIR),
        out_shape=jax.ShapeDtypeStruct((rows, width), BF16),
    )(query, pairs)


def attend_back(query, grad, pairs):
    rows, width = query.shape
    keys = pairs.shape[0]
    return pl.pallas_call(
        backward_kernel,
        grid=(width // PAIR,),
        in_specs=[
            column_block(rows, PAIR),
            column_block(rows, PAIR),
            column_block(keys, 2 * PAIR),
        ],
        out_specs=(column_block(rows, PAIR), column_block(keys, 2 * PAIR)),
        out_shape=(
            jax.ShapeDtypeStruct((rows, width), BF16),
            jax.ShapeDtypeStruct((keys, 2 * width), BF16),
        ),
    )(query, grad, pairs)


def mixed(left, right):
    parts = []
    for low in range(0, left.shape[1], PAIR):
        parts += [left[:, low : low + PAIR], right[:, low : low + PAIR]]
    return jnp.concatenate(parts, axis=1)


def unmixed(both):
    starts = range(0, both.shape[1], 2 * PAIR)
    return (
        jnp.concatenate([both[:, low : low + PAIR] for low in starts], axis=1),
        jnp.concatenate([both[:, low + PAIR : low + 2 * PAIR] for low in starts], axis=1),
    )


def gather_all(shard):
    return lax.all_gather(shard, "cp", axis=0, tiled=True)


def scatter_all(values):
    return lax.psum_scatter(values.astype(BF16), "cp", scatter_dimension=0, tiled=True)


def places():
    rep = lax.axis_index("rep")
    cp = lax.axis_index("cp")
    return rep, cp // 4, (cp // 2) % 2, cp % 2


def place_of(high, low, core):
    return 4 * high + 2 * low + core


def enter(reps):
    rep, high, low, core = places()
    barrier = pltpu.get_barrier_semaphore()
    peers = [
        (rep, place_of(high, low, 1 - core)),
        (rep, place_of(high, 1 - low, core)),
        (rep, place_of(1 - high, low, core)),
    ]
    peers += [((rep + k) % reps, place_of(high, low, core)) for k in range(1, reps)]
    for peer in peers:
        pl.semaphore_signal(barrier, inc=1, device_id=peer, device_id_type=MESH)
    pl.semaphore_wait(barrier, len(peers))


def remote(src, dst, sends, recvs, at, peer):
    return pltpu.make_async_remote_copy(
        src_ref=src,
        dst_ref=dst,
        send_sem=sends.at[at],
        recv_sem=recvs.at[at],
        device_id=peer,
        device_id_type=MESH,
    )


def gather_kernel(units, kinds, reps, pairs, *refs):
    count = len(kinds)
    ins = refs[:count]
    at = count
    if pairs:
        query_ref, key_ref, value_ref = refs[at : at + 3]
        at += 3
    outs = refs[at : at + count]
    at += count
    if pairs:
        context_ref, pair_ref = refs[at : at + 2]
        at += 2
    sends_z, recvs_z, sends_r, recvs_r, sends_c, recvs_c, local = refs[at : at + 7]
    rep, high, low, core = places()
    me = (rep, place_of(high, low, core))
    sibling = (rep, place_of(high, low, 1 - core))
    far = (rep, place_of(1 - high, low, core))
    near = (rep, place_of(high, 1 - low, core))
    enter(reps)
    copies = []

    def send(src, dst, sends, recvs, at, peer):
        remote(src, dst, sends, recvs, at, peer).start()

    def left(block, sends, recvs, at):
        remote(block, block, sends, recvs, at, me).wait_send()

    def arrived(block, sends, recvs, at):
        remote(block, block, sends, recvs, at, me).wait_recv()

    origins = (
        (high, low),
        (high, 1 - low),
        (1 - high, low),
        (1 - high, 1 - low),
    )

    def block_of(u, which, side, quarter):
        at, start, size = units[u]
        from_high, from_low = origins[which]
        return outs[at].at[from_high, from_low, side, quarter, :, pl.ds(start, size)]

    def held(p, which, side):
        from_high, from_low = origins[which]
        return pair_ref.at[p, from_high, from_low, side]

    if pairs:
        sends_k, recvs_k, sends_s, recvs_s = refs[at + 7 :]

    def offer(p):
        own = held(p, 0, core)
        send(own, own, sends_k, recvs_k, 3 * p + 1, far)
        send(own, own, sends_k, recvs_k, 3 * p, near)
        send(own, own, sends_s, recvs_s, 4 * p, sibling)

    total = len(units)
    kind_of = [kinds[at] for at, _, _ in units]

    def begin(u):
        at, start, size = units[u]
        block = ins[at].at[rep, :, pl.ds(start, size)]
        send(block, block_of(u, 0, core, rep), sends_z, recvs_z, 3 * u + 1, far)
        send(block, block_of(u, 0, core, rep), sends_z, recvs_z, 3 * u, near)

    def own_whole(u):
        at, start, size = units[u]
        if kind_of[u] == REST:
            return block_of(u, 0, core, slice(None))
        return ins[at].at[:, :, pl.ds(start, size)]

    for u in range(total):
        if kind_of[u] == FULL:
            begin(u)
    for u in range(total):
        if kind_of[u] != DEPTH:
            send(
                own_whole(u), block_of(u, 0, core, slice(None)), sends_c, recvs_c, 4 * u, sibling
            )
    for at in range(count):
        if kinds[at] != REST:
            copy = pltpu.make_async_copy(ins[at], outs[at].at[high, low, core], local.at[at])
            copy.start()
            copies.append(copy)

    for p in range(pairs):
        cols = pl.ds(PAIR * p, PAIR)
        pair_ref[p, high, low, core, :, :PAIR] = key_ref[:, cols]
        pair_ref[p, high, low, core, :, PAIR:] = value_ref[:, cols]
        if p < AHEAD:
            offer(p)

    def spread(u, which):
        block = block_of(u, which, core, rep)
        if kind_of[u] != REST:
            arrived(block, sends_z, recvs_z, 3 * u + which - 1)
            if which == 2:
                send(block, block, sends_z, recvs_z, 3 * u + 2, near)
        if kind_of[u] == DEPTH:
            return
        for j in range(1, reps):
            index = (3 * u + which - 1) * (reps - 1) + j - 1
            peer = ((rep + j) % reps, me[1])
            send(block, block, sends_r, recvs_r, index, peer)

    def pass_on(u, which):
        if kind_of[u] == DEPTH:
            return
        for j in range(1, reps):
            index = (3 * u + which - 1) * (reps - 1) + j - 1
            block = block_of(u, which, core, (rep + reps - j) % reps)
            arrived(block, sends_r, recvs_r, index)
        whole = block_of(u, which, core, slice(None))
        send(whole, whole, sends_c, recvs_c, 4 * u + which, sibling)

    lead = kind_of.count(FULL)

    def advance(step):
        if step < total:
            spread(step, 1)
            spread(step, 2)
            if step < lead:
                for u in range(lead, total):
                    if (u - lead) * lead // (total - lead) == step:
                        begin(u)
        if 1 <= step < total + 1:
            spread(step - 1, 3)
        if 2 <= step:
            for which in range(1, 4):
                pass_on(step - 2, which)

    def take(p, which):
        block = held(p, which, core)
        arrived(block, sends_k, recvs_k, 3 * p + which - 1)
        if which == 2:
            send(block, block, sends_k, recvs_k, 3 * p + 2, near)
        send(block, block, sends_s, recvs_s, 4 * p + which, sibling)

    def compute(p):
        for which in range(4):
            arrived(held(p, which, 1 - core), sends_s, recvs_s, 4 * p + which)
        cols = pl.ds(pl.multiple_of(p * PAIR, PAIR), PAIR)
        shape = (-1, PAIR)
        context_ref[:, cols] = pair_context(
            query_ref[:, cols],
            pair_ref[p, :, :, :, :, :PAIR].reshape(shape),
            pair_ref[p, :, :, :, :, PAIR:].reshape(shape),
        )

    steps = total + 2
    if pairs:
        for u in range(total):
            for which in range(1, 4):
                spread(u, which)

    def finish(step):
        if 0 < step <= total:
            for which in range(1, 4):
                pass_on(step - 1, which)

    if not pairs:
        for step in range(steps):
            advance(step)
    else:

        def step_all(t, carry):
            @pl.when(t < pairs)
            def _():
                take(t, 1)
                take(t, 2)

            @pl.when(t < pairs - AHEAD)
            def _():
                offer(t + AHEAD)

            @pl.when((t >= 1) & (t < pairs + 1))
            def _():
                take(t - 1, 3)

            for i in range(steps):

                @pl.when(t == i)
                def _(i=i):
                    finish(i)

            @pl.when((t >= 2) & (t < pairs + 2))
            def _():
                compute(t - 2)

            return carry

        lax.fori_loop(0, max(pairs + 2, steps), step_all, 0)
    for u in range(total):
        if kind_of[u] != DEPTH:
            for which in range(4):
                block = block_of(u, which, 1 - core, slice(None))
                arrived(block, sends_c, recvs_c, 4 * u + which)
    for copy in copies:
        copy.wait()
    for u, (at, start, size) in enumerate(units):
        if kind_of[u] != REST:
            block = ins[at].at[rep, :, pl.ds(start, size)]
            left(block, sends_z, recvs_z, 3 * u)
            left(block, sends_z, recvs_z, 3 * u + 1)
            left(block_of(u, 2, core, rep), sends_z, recvs_z, 3 * u + 2)
        if kind_of[u] != DEPTH:
            left(own_whole(u), sends_c, recvs_c, 4 * u)
            for which in range(1, 4):
                left(block_of(u, which, core, slice(None)), sends_c, recvs_c, 4 * u + which)
                for j in range(1, reps):
                    index = (3 * u + which - 1) * (reps - 1) + j - 1
                    left(block_of(u, which, core, rep), sends_r, recvs_r, index)
    for p in range(pairs):
        for at, which in enumerate((0, 0, 2)):
            left(held(p, which, core), sends_k, recvs_k, 3 * p + at)
        for which in range(4):
            left(held(p, which, core), sends_s, recvs_s, 4 * p + which)


def cut(width, pieces):
    size = width // pieces
    if size % 128:
        return [(0, width)]
    return [(size * i, size) for i in range(pieces)]


def gather_many(shards, pieces, kinds, identity, query=None, keys=None, values=None):
    reps = lax.axis_size("rep")
    count = len(shards)
    units = [
        (at, low, size)
        for at, shard in enumerate(shards)
        for low, size in cut(shard.shape[-1], pieces[at])
    ]
    total = len(units)
    hops = 3 * total * (reps - 1)
    dma = pltpu.SemaphoreType.DMA
    vmem = pl.BlockSpec(memory_space=pltpu.VMEM)
    out_shape = [
        jax.ShapeDtypeStruct(
            shard.shape if kind == REST else (2, 2, 2) + shard.shape, shard.dtype
        )
        for shard, kind in zip(shards, kinds)
    ]
    operands = list(shards)
    spaces = []
    more = []
    pairs = 0
    if query is not None:
        pairs = query.shape[1] // PAIR
        operands += [query, keys, values]
        spaces = [vmem] * 3
        out_shape += [
            jax.ShapeDtypeStruct(query.shape, BF16),
            jax.ShapeDtypeStruct((pairs, 2, 2, 2, keys.shape[0], 2 * PAIR), BF16),
        ]
        more = [dma((3 * pairs,))] * 2 + [dma((4 * pairs,))] * 2
    return pl.pallas_call(
        functools.partial(gather_kernel, units, tuple(kinds), reps, pairs),
        input_output_aliases={at: at for at in range(count) if kinds[at] == REST},
        out_shape=out_shape,
        in_specs=[
            pl.BlockSpec(memory_space=pl.ANY if kind == REST else pltpu.VMEM) for kind in kinds
        ]
        + spaces,
        out_specs=[pl.BlockSpec(memory_space=pl.ANY)] * count + spaces[:2],
        scratch_shapes=[dma((3 * total,))] * 2
        + [dma((hops,))] * 2
        + [dma((4 * total,))] * 2
        + [dma((count,))]
        + more,
        compiler_params=pltpu.CompilerParams(
            collective_id=identity, has_side_effects=True, vmem_limit_bytes=60 * 1024 * 1024
        ),
    )(*operands)


def summed(parts, kind):
    total = parts[0].astype(F32)
    for part in parts[1:]:
        total = total + part.astype(F32)
    return total.astype(kind)


def reduce_kernel(units, kinds, reps, fused, *refs):
    count = len(kinds)
    ins = refs[:count]
    at = count
    if fused:
        query_ref, grad_ref, pair_ref = refs[at : at + 3]
        at += 3
    outs = refs[at : at + count]
    at += count
    if fused:
        grad_query_ref, grad_key_ref, grad_value_ref = refs[at : at + 3]
        at += 3
    size = len(units)
    first, second, third, fourth, own, mid, final = [
        refs[at + i * size : at + (i + 1) * size] for i in range(7)
    ]
    written = refs[at + 7 * size]
    sems = refs[at + 7 * size + 1 :]

    def write(u):
        a, start, width = units[u]
        block = outs[a].at[:, :, pl.ds(start, width)]
        return pltpu.make_async_copy(final[u], block, written.at[u])

    kind_of = [kinds[a] for a, _, _ in units]
    sends_c, recvs_c, sends_r, recvs_r, sends_z, recvs_z, sends_g, recvs_g = sems[:8]
    rep, high, low, core = places()
    me = (rep, place_of(high, low, core))
    sibling = (rep, place_of(high, low, 1 - core))
    far = (rep, place_of(1 - high, low, core))
    near = (rep, place_of(high, 1 - low, core))
    enter(reps)
    def send(src, dst, sends, recvs, at, peer):
        remote(src, dst, sends, recvs, at, peer).start()

    def left(block, sends, recvs, at):
        remote(block, block, sends, recvs, at, me).wait_send()

    def arrived(block, sends, recvs, at):
        remote(block, block, sends, recvs, at, me).wait_recv()

    for u, (a, start, width) in enumerate(units):
        if kind_of[u] == DEPTH:
            own[u][...] = ins[a][:, :, :, start : start + width]
            send(own[u].at[:, 1 - low], third[u], sends_z, recvs_z, 2 * u, near)
            continue
        block = ins[a].at[:, :, 1 - core, :, :, pl.ds(start, width)]
        send(block, first[u], sends_c, recvs_c, u, sibling)

    def over_core(u):
        a, start, width = units[u]
        if kind_of[u] == DEPTH:
            return
        arrived(first[u], sends_c, recvs_c, u)

        def step(i, carry):
            h, w, q = i // (2 * reps), (i // reps) % 2, i % reps
            mine = ins[a][h, w, core, q, :, start : start + width]
            first[u][h, w, q] = summed([first[u][h, w, q], mine], first[u].dtype)
            return carry

        lax.fori_loop(0, 4 * reps, step, 0)
        for k in range(1, reps):
            target = (rep + k) % reps
            send(
                first[u].at[:, :, target],
                second[u].at[k - 1],
                sends_r,
                recvs_r,
                u * (reps - 1) + k - 1,
                (target, me[1]),
            )

    def over_rep(u):
        a, start, width = units[u]
        if kind_of[u] == DEPTH:
            return
        for k in range(1, reps):
            arrived(second[u].at[k - 1], sends_r, recvs_r, u * (reps - 1) + k - 1)

        def step(i, carry):
            h, w = i // 2, i % 2
            parts = [first[u][h, w, rep]] + [second[u][k, h, w] for k in range(reps - 1)]
            total = summed(parts, first[u].dtype)
            if kind_of[u] == REST:
                outs[a][h, w, :, start : start + width] = total
            else:
                own[u][h, w] = total
            return carry

        lax.fori_loop(0, 4, step, 0)
        if kind_of[u] == FULL:
            send(own[u].at[:, 1 - low], third[u], sends_z, recvs_z, 2 * u, near)

    def over_near(u):
        if kind_of[u] == REST:
            return
        arrived(third[u], sends_z, recvs_z, 2 * u)
        for h in range(2):
            own[u][h, low] = summed([own[u][h, low], third[u][h]], own[u].dtype)
        send(own[u].at[1 - high, low], fourth[u], sends_z, recvs_z, 2 * u + 1, far)

    def over_far(u):
        if kind_of[u] == REST:
            return
        arrived(fourth[u], sends_z, recvs_z, 2 * u + 1)
        mid[u][rep] = summed([own[u][high, low], fourth[u][...]], mid[u].dtype)
        block = mid[u].at[rep]
        for k in range(1, reps):
            peer = ((rep + k) % reps, me[1])
            send(block, block, sends_g, recvs_g, u * (reps - 1) + k - 1, peer)

    if not fused:
        whole = [u for u in range(size) if kind_of[u] != DEPTH]
        rest = [u for u in range(size) if kind_of[u] == DEPTH]
        order = [(over_core, whole), (over_near, rest), (over_rep, whole)]
        order += [(over_far, rest), (over_near, whole), (over_far, whole)]
        for stage, members in order:
            for u in members:
                stage(u)
    else:
        terms, merged, from_near, from_far, held, sends_k, recvs_k, fetched = sems[8:]
        pairs = terms.shape[0]

        def advance(step):
            for u in range(size):
                if step == u // 2:
                    over_core(u)
                if step == pairs - 1 + u // 2:
                    over_rep(u)

        steps = pairs + size // 2 + 1

        def fetch(p):
            return pltpu.make_async_copy(pair_ref.at[p], held.at[p % 2], fetched.at[p % 2])

        def hop(p, which):
            if which == 0:
                return remote(
                    terms.at[p, :, :, 1 - core], merged.at[p], sends_k, recvs_k, 3 * p, sibling
                )
            if which == 1:
                return remote(
                    merged.at[p, :, 1 - low], from_near.at[p], sends_k, recvs_k, 3 * p + 1, near
                )
            return remote(
                merged.at[p, 1 - high, low], from_far.at[p], sends_k, recvs_k, 3 * p + 2, far
            )

        def merge_core(p):
            arrived(merged.at[p], sends_k, recvs_k, 3 * p)
            for h in range(2):
                for w in range(2):
                    both = [merged[p, h, w], terms[p, h, w, core]]
                    merged[p, h, w] = summed(both, BF16)
            hop(p, 1).start()

        def merge_near(p):
            arrived(from_near.at[p], sends_k, recvs_k, 3 * p + 1)
            for h in range(2):
                merged[p, h, low] = summed([merged[p, h, low], from_near[p, h]], BF16)
            hop(p, 2).start()

        def merge_far(p):
            arrived(from_far.at[p], sends_k, recvs_k, 3 * p + 2)
            cols = pl.ds(pl.multiple_of(p * PAIR, PAIR), PAIR)
            both = summed([merged[p, high, low], from_far[p]], BF16)
            grad_key_ref[:, cols] = both[:, :PAIR]
            grad_value_ref[:, cols] = both[:, PAIR:]

        def compute(p):
            fetch(p).wait()

            @pl.when(p < pairs - 1)
            def _():
                fetch(p + 1).start()

            cols = pl.ds(pl.multiple_of(p * PAIR, PAIR), PAIR)
            slot = p % 2
            query_part, key_part, value_part = pair_grads(
                query_ref[:, cols], grad_ref[:, cols], held[slot, :, :PAIR], held[slot, :, PAIR:]
            )
            grad_query_ref[:, cols] = query_part
            shape = terms.shape[1:5] + (PAIR,)
            terms[p, :, :, :, :, :PAIR] = key_part.reshape(shape)
            terms[p, :, :, :, :, PAIR:] = value_part.reshape(shape)
            hop(p, 0).start()

        fetch(0).start()

        def step_all(t, carry):
            for lag, merge in ((1, merge_core), (2, merge_near), (3, merge_far)):

                @pl.when((t >= lag) & (t < pairs + lag))
                def _(lag=lag, merge=merge):
                    merge(t - lag)

            @pl.when(t < pairs)
            def _():
                compute(t)

            for i in range(steps):

                @pl.when(t == i)
                def _(i=i):
                    advance(i)

            return carry

        lax.fori_loop(0, max(pairs + 3, steps), step_all, 0)
        for p in range(pairs):
            for which in range(3):
                hop(p, which).wait_send()
    for u, (a, start, width) in enumerate(units):
        if kind_of[u] != REST:
            for k in range(1, reps):
                block = mid[u].at[(rep + reps - k) % reps]
                arrived(block, sends_g, recvs_g, u * (reps - 1) + k - 1)
            final[u][...] = mid[u][...].astype(F32)
            write(u).start()
    for u in range(size):
        if kind_of[u] != REST:
            write(u).wait()
    for u, (a, start, width) in enumerate(units):
        cols = pl.ds(start, width)
        if kind_of[u] != DEPTH:
            left(ins[a].at[:, :, 1 - core, :, :, cols], sends_c, recvs_c, u)
        if kind_of[u] != REST:
            left(own[u].at[:, 1 - low], sends_z, recvs_z, 2 * u)
            left(own[u].at[1 - high, low], sends_z, recvs_z, 2 * u + 1)
        for k in range(1, reps):
            index = u * (reps - 1) + k - 1
            if kind_of[u] != DEPTH:
                left(first[u].at[:, :, (rep + k) % reps], sends_r, recvs_r, index)
            if kind_of[u] != REST:
                left(mid[u].at[rep], sends_g, recvs_g, index)


def split_rows(part):
    reps = lax.axis_size("rep")
    rows, width = part.shape
    return part.reshape(2, 2, 2, reps, rows // (8 * reps), width)


def reduce_many(blocks, pieces, kinds, identity, query=None, grad=None, pairs=None):
    reps = lax.axis_size("rep")
    count = len(blocks)
    units = [
        (at, low, size)
        for at, block in enumerate(blocks)
        for low, size in cut(block.shape[-1], pieces[at])
    ]
    dma = pltpu.SemaphoreType.DMA
    vmem = pl.BlockSpec(memory_space=pltpu.VMEM)

    def buffers(without, *lead, kind=None):
        shapes = []
        for at, _, size in units:
            tile = (blocks[at].shape[-2], size)
            if kinds[at] == without:
                shapes.append(pltpu.VMEM((8, 128), BF16))
            else:
                shapes.append(pltpu.VMEM(lead + tile, kind or blocks[at].dtype))
        return shapes

    total = len(units)
    out_shape = [
        jax.ShapeDtypeStruct((2, 2) + block.shape[4:], block.dtype)
        if kind == REST
        else jax.ShapeDtypeStruct((reps,) + block.shape[-2:], F32)
        for block, kind in zip(blocks, kinds)
    ]
    operands = list(blocks)
    in_specs = [vmem] * count
    more = []
    if pairs is not None:
        tokens, width = query.shape
        number = width // PAIR
        block = (tokens, 2 * PAIR)
        operands += [query, grad, pairs]
        in_specs += [vmem] * 2 + [pl.BlockSpec(memory_space=pl.ANY)]
        out_shape += [jax.ShapeDtypeStruct((tokens, width), BF16)] * 3
        more = [
            pltpu.VMEM((number, 2, 2, 2) + block, BF16),
            pltpu.VMEM((number, 2, 2) + block, BF16),
            pltpu.VMEM((number, 2) + block, BF16),
            pltpu.VMEM((number,) + block, BF16),
            pltpu.VMEM((2,) + pairs.shape[1:], BF16),
            dma((3 * number,)),
            dma((3 * number,)),
            dma((2,)),
        ]
    sums = pl.pallas_call(
        functools.partial(reduce_kernel, units, tuple(kinds), reps, pairs is not None),
        out_shape=out_shape,
        in_specs=in_specs,
        out_specs=[
            vmem if kind == REST else pl.BlockSpec(memory_space=pltpu.HBM) for kind in kinds
        ]
        + [vmem] * (len(out_shape) - count),
        scratch_shapes=buffers(DEPTH, 2, 2, reps)
        + buffers(DEPTH, reps - 1, 2, 2)
        + buffers(REST, 2)
        + buffers(REST)
        + buffers(REST, 2, 2)
        + buffers(REST, reps)
        + buffers(REST, reps, kind=F32)
        + [dma((total,))]
        + [dma((total,))] * 2
        + [dma((total * (reps - 1),))] * 2
        + [dma((total * 2,))] * 2
        + [dma((total * (reps - 1),))] * 2
        + more,
        compiler_params=pltpu.CompilerParams(
            collective_id=identity, has_side_effects=True, vmem_limit_bytes=60 * 1024 * 1024
        ),
    )(*operands)
    totals = [
        total if kind == REST else total.reshape(-1, total.shape[2])
        for total, kind in zip(sums, kinds)
    ]
    return totals + list(sums[count:])


def blocked(shard):
    return shard.reshape(lax.axis_size("rep"), -1, shard.shape[1])


def divides(rows):
    reps = lax.axis_size("rep")
    return lax.axis_size("cp") == 8 and reps == 4 and rows % (8 * reps) == 0


def on_device(
    tokens,
    query_weight,
    query_bias,
    key_weight,
    value_weight,
    value_bias,
    output_weight,
    output_bias,
    first_gain,
    first_shift,
    up_weight,
    up_bias,
    down_weight,
    down_bias,
    second_gain,
    second_shift,
    cotangent,
):
    row_count = tokens.shape[1]
    width = tokens.shape[2]
    local_tokens = tokens[0]
    fast = divides(query_weight.shape[0])
    reps = lax.axis_size("rep")
    small = (
        query_bias,
        value_bias,
        output_bias,
        first_gain,
        first_shift,
        up_bias,
        down_bias,
        second_gain,
        second_shift,
    )
    if fast:
        rows = []
        for vector in small:
            lines = -(-vector.shape[0] // 128)
            rows.append(
                jnp.pad(vector.astype(F32), (0, 128 * lines - vector.shape[0])).reshape(lines, 128)
            )
        packed = jnp.concatenate(rows, axis=0)
        packed = jnp.pad(packed, ((0, -packed.shape[0] % (8 * reps)), (0, 0))).astype(BF16)
        shards = (key_weight, value_weight, query_weight, packed)
        shards += (output_weight, up_weight, down_weight)
        w_key, w_value, w_query, gathered, *begun = gather_many(
            [blocked(shard) for shard in shards],
            (1, 1, 1, 1, 1, 2, 2),
            (FULL,) * 4 + (DEPTH,) * 3,
            1,
        )
        w_key, w_value, w_query = [w.reshape(-1, width) for w in (w_key, w_value, w_query)]
        gathered = gathered.reshape(-1, packed.shape[0], 128)
    else:
        w_query, w_key, w_value = [
            gather_all(shard) for shard in (query_weight, key_weight, value_weight)
        ]
        gathered = lax.all_gather(jnp.concatenate(small)[None], "cp", axis=0, tiled=True)
    vectors = []
    at = 0
    for vector in small:
        size = vector.shape[0]
        if fast:
            lines = -(-size // 128)
            part = gathered[:, at : at + lines].reshape(-1, 128 * lines)[:, :size]
            at += lines
        else:
            part = gathered[:, at : at + size]
            at += size
        vectors.append(part.reshape(-1).astype(F32))
    b_query, b_value, b_output, gain_one, shift_one, b_up, b_down, gain_two, shift_two = vectors
    key_rows = matmul(local_tokens, w_key).astype(BF16)
    value_rows = (matmul(local_tokens, w_value) + b_value).astype(BF16)
    chunk = width // CHUNKS
    query_rows = (matmul(local_tokens, w_query) + b_query).astype(BF16)
    query_scaled = query_rows * jnp.asarray(1.0 / math.sqrt(HD), BF16)
    if fast:
        w_output, w_up, w_down, context_low, pairs = gather_many(
            begun,
            (1, 2, 2),
            (REST,) * 3,
            2,
            query_scaled,
            key_rows,
            value_rows,
        )
        w_output, w_down = w_output.reshape(-1, width), w_down.reshape(-1, width)
        w_up = w_up.reshape(-1, up_weight.shape[1])
        pairs = pairs.reshape(pairs.shape[0], -1, 2 * PAIR)
    else:
        w_output, w_up, w_down = [
            gather_all(shard) for shard in (output_weight, up_weight, down_weight)
        ]
        pair_rows = mixed(key_rows, value_rows)
        queries = [query_scaled[:, chunk * i : chunk * (i + 1)] for i in range(CHUNKS)]
        pairs = [
            lax.all_gather(
                pair_rows[:, 2 * chunk * i : 2 * chunk * (i + 1)], "cp", axis=0, tiled=True
            )
            for i in range(CHUNKS)
        ]
        context_low = jnp.concatenate(
            [attend(query, pair) for query, pair in zip(queries, pairs)], axis=1
        )
    attn_out = matmul(context_low, w_output) + b_output
    resid_first = local_tokens.astype(F32) + attn_out
    first_norm, pull_first = jax.vjp(normalize, resid_first, gain_one, shift_one)
    first_low = first_norm.astype(BF16)
    inner_act = matmul(first_low, w_up) + b_up
    hidden, pull_gelu = jax.vjp(gelu_exact, inner_act)
    hidden_low = hidden.astype(BF16)
    resid_second = first_norm + (matmul(hidden_low, w_down) + b_down)
    layer_out, pull_second = jax.vjp(normalize, resid_second, gain_two, shift_two)

    grad_resid2, grad_gain2, grad_shift2 = pull_second(cotangent[0])
    grad_outer = grad_resid2.astype(BF16)
    grad_down_bias = column_sum(grad_outer)
    part_down = over_rows(hidden_low, grad_outer).astype(BF16)
    grad_inner = pull_gelu(against(grad_outer, w_down))[0].astype(BF16)
    grad_up_bias = column_sum(grad_inner)
    part_up = over_rows(first_low, grad_inner).astype(BF16)
    grad_first = grad_resid2 + against(grad_inner, w_up)
    grad_resid1, grad_gain1, grad_shift1 = pull_first(grad_first)
    grad_attn = grad_resid1.astype(BF16)
    grad_output_bias = column_sum(grad_attn)
    part_output = over_rows(context_low, grad_attn).astype(BF16)
    grad_context = against(grad_attn, w_output).astype(BF16)

    if fast:
        (
            *begun,
            grad_query_low,
            grad_key_low,
            grad_value_low,
        ) = reduce_many(
            [split_rows(part) for part in (part_down, part_up, part_output)],
            (2, 2, 1),
            (REST,) * 3,
            3,
            query_scaled,
            grad_context,
            pairs,
        )
    else:
        grad_queries = []
        grad_pairs = []
        for i in range(CHUNKS):
            grad_query, grad_terms = attend_back(
                queries[i], grad_context[:, chunk * i : chunk * (i + 1)], pairs[i]
            )
            grad_queries.append(grad_query)
            grad_pairs.append(
                lax.psum_scatter(grad_terms, "cp", scatter_dimension=0, tiled=True)
            )
        grad_query_low = jnp.concatenate(grad_queries, axis=1)
        grad_key_low, grad_value_low = unmixed(jnp.concatenate(grad_pairs, axis=1))
    part_query = over_rows(local_tokens, grad_query_low).astype(BF16)
    part_key = over_rows(local_tokens, grad_key_low).astype(BF16)
    part_value = over_rows(local_tokens, grad_value_low).astype(BF16)
    grad_tokens = (
        grad_resid1
        + against(grad_query_low, w_query)
        + against(grad_key_low, w_key)
        + against(grad_value_low, w_value)
    )

    small_grads = (
        column_sum(grad_query_low),
        column_sum(grad_value_low),
        grad_output_bias,
        grad_gain1,
        grad_shift1,
        grad_up_bias,
        grad_down_bias,
        grad_gain2,
        grad_shift2,
    )
    owners = lax.axis_size("cp")
    total_sq = jnp.broadcast_to(jnp.sum(grad_tokens * grad_tokens), (owners, 1))
    flat = jnp.concatenate(
        [vector.reshape(owners, -1) for vector in small_grads] + [total_sq], axis=1
    )
    if fast:
        flat = jnp.pad(flat, ((0, 0), (0, -flat.shape[1] % (8 * 128 * reps))))
        blocks = [split_rows(part) for part in (part_query, part_key, part_value)]
        full_query, full_key, full_value, sums, full_down, full_up, full_output = reduce_many(
            blocks + [flat.reshape(2, 2, 2, reps, -1, 128)] + begun,
            (1,) * 7,
            (FULL,) * 4 + (DEPTH,) * 3,
            4,
        )
        sums = sums.reshape(-1)
    else:
        parts = (part_down, part_up, part_output, part_query, part_key, part_value)
        shards = [scatter_all(part) for part in parts]
        full_down, full_up, full_output, full_query, full_key, full_value = [
            part.astype(F32) for part in lax.psum(tuple(shards), "rep")
        ]
        sums = lax.psum(flat, ("rep", "cp"))
        sums = lax.dynamic_slice_in_dim(sums, lax.axis_index("cp"), 1, 0)[0]
    reduced = []
    at = 0
    for shard in small:
        reduced.append(sums[at : at + shard.shape[0]])
        at += shard.shape[0]
    entries = lax.axis_size("rep") * owners * row_count * width
    rms_values = jnp.sqrt(sums[at : at + 1] / entries)

    return (
        layer_out[None],
        grad_tokens[None],
        full_query,
        reduced[0],
        full_key,
        full_value,
        reduced[1],
        full_output,
        reduced[2],
        reduced[3],
        reduced[4],
        full_up,
        reduced[5],
        full_down,
        reduced[6],
        reduced[7],
        reduced[8],
        rms_values,
    )


def solution(mesh):
    rows = P("cp", None)
    vector = P("cp")
    whole = P("rep", "cp", None)
    params = (
        rows,
        vector,
        rows,
        rows,
        vector,
        rows,
        vector,
        vector,
        vector,
        rows,
        vector,
        rows,
        vector,
        vector,
        vector,
    )
    return jax.shard_map(
        on_device,
        mesh=mesh,
        in_specs=(whole,) + params + (whole,),
        out_specs=(whole, whole) + params + (P(),),
        check_vma=False,
    )
```
